32 devices in a mesh: grp: 2 (over y), vec: 4 (over z), walk: 2 (over x), orb: 2 (over core).
Axes of the slice: x: 2, y: 2, z: 4, core: 2. Of those that a mesh axis runs over, the one named last changes fastest.
Arguments:
- walkers: bfloat16 [32, 512, 128], P(('grp', 'walk'), 'orb'), parts along dimension 0, may hold values from -3 to 3
- inv_intersection: bfloat16 [32, 128, 128], P(('grp', 'walk')), parts along dimension 0, may hold values from -0.5 to 0.5
- trial: bfloat16 [512, 128], replicated, may hold values from -0.25 to 0.25
- vectors: bfloat16 [32, 512, 512], P('vec', 'orb')
- aux_field: float32 [32, 32], P(('grp', 'walk'), 'vec'), parts along dimension 0, may hold values from -5 to 5
- log_weight: float32 [32], P(('grp', 'walk')), parts along dimension 0, may hold values from -4 to 4
- copy_list: int32 [32], P(('grp', 'walk')), parts along dimension 0, may hold values from 0 to 15
Outputs:
- walkers_out: bfloat16 [32, 512, 128], P(('grp', 'walk'), 'orb'), parts along dimension 0
- weights_out: float32 [32], P(('grp', 'walk')), parts along dimension 0
The draws below stay inside these ranges and needn't reach their ends.
There are 2 independent parts, one for each index of `grp`. The reference program is written for one: setup_inputs(seed, part) draws one part's arguments, and reference() takes and returns one part's arrays. A program takes and returns all parts, laid end to end along the dimension named above; an argument that names none is the same for every part. Nothing has to cross between parts.
Inputs may be any that keep to these rules, and one draw needn't show every extreme that they name: `copy_list`: the walker, within the same ensemble, whose copy fills the slot.
All inputs are finite; a program needn't handle non-finite values.
Results may differ from the reference program's by a relative error of at most 0.008.
Values may be sent and summed in bfloat16 or wider, within the bound.
A program may use at most 64 MiB of HBM per device.

```python
import math
import jax
import jax.numpy as jnp
import numpy as np
from jax import lax

N = 512
E = 128
ORDER = 6
CHOL = 32
WALKERS = 16


def draw_vectors(key, part):
    base = jax.random.normal(key, (CHOL, N, N), jnp.float32)
    spread = 5.0 / math.sqrt(N * CHOL)
    sym = (base + jnp.swapaxes(base, 1, 2)) * (spread / math.sqrt(2.0))
    return sym.astype(jnp.bfloat16)


def set_ends(drawn, key, smallest, top_value):
    dims = drawn.shape
    index_at = [jax.random.randint(jax.random.fold_in(key, axis), (), 0, dims[axis]) for axis in range(len(dims))]
    drawn = drawn.at[tuple(index_at)].set(smallest)
    longest = dims.index(max(dims))
    index_at[longest] = (index_at[longest] + 1) % dims[longest]
    return drawn.at[tuple(index_at)].set(top_value)


def steps_of(own_key, shape, shards, smallest, high):
    level, own = 1.0, jax.random.fold_in(own_key, 6)
    for position, parts in shards:
        heights = jnp.exp(jax.random.uniform(jax.random.fold_in(own, position), (parts,), jnp.float32, smallest / len(shards), high / len(shards)))
        level = level * jnp.repeat(heights, shape[position] // parts).reshape([-1 if axis == position else 1 for axis in range(len(shape))])
    return level


def rank_bounds(count, slope):
    loads = [(1 << 20) // math.isqrt(grade ** slope) + 1 for grade in range(1, count + 1)]
    width = 1 + sum(loads) // (1 << 30)
    return np.cumsum(np.array([max(1, weight // width) for weight in loads]))


def ranked_ids(own_key, shape, count, slope):
    table = rank_bounds(count, slope)
    pick = jax.random.randint(jax.random.fold_in(own_key, 1), shape, 0, int(table[count - 1]))
    rank = jnp.searchsorted(jnp.asarray(table, jnp.int32), pick, side="right")
    return jax.random.permutation(jax.random.fold_in(own_key, 2), count)[rank].astype(jnp.int32)


def gaussian(own_key, extent, scale, reach, pieces=(), kind=jnp.bfloat16):
    factor_of = steps_of(own_key, extent, pieces, -0.22, 0.18) if pieces else 1.0
    array = jax.random.normal(own_key, extent, jnp.float32) * scale * factor_of
    return jnp.minimum(jnp.maximum(array, -reach), reach).astype(kind)


def setup_inputs(seed: int = 0, part: int = 0) -> dict:
    streams_of = jax.random.split(jax.random.key(seed), 8)
    own_keys = jax.random.split(jax.random.fold_in(streams_of[7], part), 8)
    return {
        "walkers": gaussian(own_keys[0], (WALKERS, N, E), 0.5, 3.0, ((0, 2), (1, 2))),
        "inv_intersection": gaussian(own_keys[1], (WALKERS, E, E), E ** -0.5, 0.5, ((0, 2),)),
        "trial": gaussian(streams_of[2], (N, E), N ** -0.5, 0.25),
        "vectors": draw_vectors(jax.random.fold_in(streams_of[7], 71), part),
        "aux_field": gaussian(own_keys[4], (WALKERS, CHOL), 1.0, 5.0, ((0, 2), (1, 4)), jnp.float32),
        "log_weight": gaussian(own_keys[5], (WALKERS,), 1.0, 4.0, ((0, 2),), jnp.float32),
        "copy_list": set_ends(ranked_ids(own_keys[6], (WALKERS,), WALKERS, 2), jax.random.fold_in(own_keys[6], 3), 0, WALKERS - 1).astype(jnp.int32),
    }


step_root = math.sqrt(0.08)

def reference(walkers, inv_intersection, trial, vectors, aux_field, log_weight, copy_list):
    high = lax.Precision.HIGHEST
    green = jnp.einsum('wne,wef->wnf', walkers.astype(jnp.float32), inv_intersection.astype(jnp.float32), precision=high).astype(jnp.bfloat16)
    mixed = jnp.einsum('gnm,me->gne', vectors.astype(jnp.float32), trial.astype(jnp.float32), precision=high).astype(jnp.bfloat16)
    bias = jnp.einsum('wne,gne->wg', green.astype(jnp.float32), mixed.astype(jnp.float32), precision=high)
    shift = -step_root * bias
    field = aux_field - shift
    new_log = log_weight + lax.optimization_barrier(jnp.sum(aux_field * shift - 0.5 * shift * shift, axis=1))
    weighted = (field * step_root).astype(jnp.bfloat16)
    operator = jnp.einsum('wg,gnm->wnm', weighted.astype(jnp.float32), vectors.astype(jnp.float32), precision=high).astype(jnp.bfloat16)
    operand = operator.astype(jnp.float32)
    term = walkers
    total = walkers.astype(jnp.float32)
    for degree in range(1, ORDER + 1):
        product = jnp.einsum('wnm,wme->wne', operand, term.astype(jnp.float32), precision=high)
        term = (product / degree).astype(jnp.bfloat16)
        total = total + term.astype(jnp.float32)
    propagated = total.astype(jnp.bfloat16)
    return (propagated[copy_list], new_log[copy_list])
```

```python
import functools
import math

import jax
import jax.numpy as jnp
from jax import lax
from jax.experimental import pallas as pl
from jax.experimental.pallas import tpu as pltpu
from jax.sharding import PartitionSpec as P

ORDER = 6
BLOCKS = 4
SKEW = 5
PARTS = 2
REACH = 3
MESH = pl.DeviceIdType.MESH
F32 = jnp.float32
BF16 = jnp.bfloat16

step_root = math.sqrt(0.08)


def remote(src, dst, send, recv, where):
    return pltpu.make_async_remote_copy(
        src_ref=src, dst_ref=dst, send_sem=send, recv_sem=recv, device_id=where, device_id_type=MESH
    )


def kernel(
    depth, width,
    walkers_in, inverse_in, trial_in, vectors_in, aux_in, log_in, copies_in,
    out, out_log,
    walkers, inverse, trial, vectors, aux, log_weight, copies,
    green, mixed, strips, level, bias_all, facts, picked, partial, leaving, arrived, given, crossed,
    extra_in, extra_out, edge, staged, pool, full, term, result, gathered,
    load_sems, copies_send, copies_recv, facts_send, facts_recv, bias_send, bias_recv,
    chain_send, chain_recv, cross_recv, swap_send, swap_recv, extra_send, extra_recv, edge_sems,
    stage_send, pool_recv, own_send, next_send, slot_recv, write_sems,
):
    z = lax.axis_index("vec")
    x = lax.axis_index("walk")
    o = lax.axis_index("orb")
    last = depth - 1
    local, rows, electrons = walkers.shape
    count, _, orbitals = vectors.shape
    half = local // 2
    block = orbitals // 4
    span = 2 * block // count
    wide = count * span
    chunks = half * BLOCKS
    mine = half // 2
    lanes = extra_in.shape[2]
    hops = range(1, width)

    barrier = pltpu.get_barrier_semaphore()

    def greet(where):
        pl.semaphore_signal(barrier, inc=1, device_id=where, device_id_type=MESH)

    greet({"orb": 1 - o})
    for hop in hops:
        for core in range(2):
            greet({"walk": lax.rem(x + hop, width), "orb": core})

    @pl.when(z > 0)
    def _():
        for core in range(2):
            greet({"vec": z - 1, "orb": core})

    @pl.when(z < last)
    def _():
        for core in range(2):
            greet({"vec": z + 1, "orb": core})

    pairs = (
        (copies_in, copies.at[x]), (log_in, log_weight), (walkers_in, walkers), (inverse_in, inverse), (trial_in, trial),
        (vectors_in, vectors), (aux_in, aux),
    )
    loads = [pltpu.make_async_copy(src, dst, load_sems.at[n]) for n, (src, dst) in enumerate(pairs)]
    for load in loads:
        load.start()

    loads[2].wait()
    loads[3].wait()
    for w in range(local):
        green[w] = jnp.dot(walkers[w], inverse[w], preferred_element_type=F32).astype(BF16)
    loads[4].wait()
    loads[5].wait()
    for g in range(count):
        mixed[g] = jnp.dot(vectors[g], trial[...], preferred_element_type=F32).astype(BF16)
    gram = jnp.zeros((local * span, wide), F32)
    for j in range(rows // span):
        left = green[:, j * span:(j + 1) * span, :].reshape(local * span, electrons)
        right = mixed[:, j * span:(j + 1) * span, :].reshape(wide, electrons)
        gram = gram + lax.dot_general(left, right, (((1,), (1,)), ((), ())), preferred_element_type=F32)
    row_id = lax.broadcasted_iota(jnp.int32, (local * span, wide), 0)
    col_id = lax.broadcasted_iota(jnp.int32, (local * span, wide), 1)
    same = row_id % span == col_id % span
    folded = jnp.sum(jnp.where(same, gram, 0.0).reshape(local, span, wide), axis=1)
    wide_row = lax.broadcasted_iota(jnp.int32, (wide, wide), 0)
    wide_col = lax.broadcasted_iota(jnp.int32, (wide, wide), 1)
    groups = jnp.where(wide_row // span == wide_col // span, 1.0, 0.0).astype(F32)
    bias_all[o, x] = jnp.dot(folded, groups, precision=lax.Precision.HIGHEST, preferred_element_type=F32)

    loads[6].wait()
    loads[0].wait()
    loads[1].wait()
    pick_row = lax.broadcasted_iota(jnp.int32, (count, wide), 0)
    pick_col = lax.broadcasted_iota(jnp.int32, (count, wide), 1)
    pick = jnp.where(pick_row == pick_col // span, 1.0, 0.0).astype(F32)
    facts[x, 0:local, :] = jnp.dot(aux[...], pick, precision=lax.Precision.HIGHEST, preferred_element_type=F32)
    walker_id = lax.broadcasted_iota(jnp.int32, (local, wide), 0)
    weights = jnp.zeros((local, wide), F32)
    for w in range(local):
        weights = jnp.where(walker_id == w, log_weight[w], weights)
    facts[x, local:2 * local, :] = weights

    sides = jnp.where(z > 0, 2, 0) + jnp.where(z < last, 2, 0)
    pl.semaphore_wait(barrier, 1 + 2 * (width - 1) + sides)

    bias_peers = [{"walk": lax.rem(x + hop, width), "orb": core} for hop in hops for core in range(2)] + [{"orb": 1 - o}]
    bias_copies = [
        remote(bias_all.at[o, x], bias_all.at[o, x], bias_send.at[n], bias_recv.at[o, x], where)
        for n, where in enumerate(bias_peers)
    ]
    for copy in bias_copies:
        copy.start()

    def facts_copy(hop, owner):
        return remote(
            facts.at[owner], facts.at[owner], facts_send.at[hop], facts_recv.at[owner], {"walk": lax.rem(x + hop, width)}
        )

    def copies_copy(hop, owner):
        return remote(
            copies.at[owner], copies.at[owner], copies_send.at[hop], copies_recv.at[owner],
            {"walk": lax.rem(x + hop, width)},
        )

    for hop in hops:
        copies_copy(hop, x).start()
        facts_copy(hop, x).start()

    chunk_row = lax.broadcasted_iota(jnp.int32, (count, span, block), 1)
    chunk_col = lax.broadcasted_iota(jnp.int32, (count, span, block), 2)
    crossing = jnp.zeros((count, span, block), F32)

    def columns(n):
        return pl.ds(pl.multiple_of(n * block, block), block)

    for j in range(block // span):
        here = slice(j * span, (j + 1) * span)
        below = slice(block + j * span, block + (j + 1) * span)
        first = vectors[:, here, columns(2 * o)].astype(F32)
        second = vectors[:, below, columns(1 + 2 * o)].astype(F32)
        crossing = crossing + jnp.where(chunk_row + j * span == chunk_col, second, 0.0)
        joined = jnp.where(chunk_row + j * span <= chunk_col, first, second).astype(BF16)
        strips[j, :, 0:block] = joined.reshape(wide, block)
        strips[j, :, block:2 * block] = vectors[:, here, block:2 * block].reshape(wide, block)
        strips[j, :, 2 * block:3 * block] = vectors[:, here, columns(2 + o)].reshape(wide, block)
        strips[j, :, 3 * block:] = vectors[:, below, columns(3 * (1 - o))].reshape(wide, block)
    level[...] = crossing.reshape(wide, block).astype(BF16)

    for hop in hops:
        other = lax.rem(x + hop, width)
        facts_copy(hop, other).wait_recv()
        for core in range(2):
            remote(
                bias_all.at[core, other], bias_all.at[core, other], bias_send.at[0], bias_recv.at[core, other], {"walk": other}
            ).wait_recv()
    remote(bias_all.at[1 - o, x], bias_all.at[1 - o, x], bias_send.at[0], bias_recv.at[1 - o, x], {"orb": 1 - o}).wait_recv()

    for s in range(local):
        source = copies[x, s]
        column = source // local
        at = source % local
        row = pl.ds(at, 1)
        picked[0, s:s + 1, :] = bias_all[0, column, row, :] + bias_all[1, column, row, :]
        picked[1, s:s + 1, :] = facts[column, row, :]
        picked[2, s:s + 1, :] = facts[column, pl.ds(local + at, 1), :]

    bias = picked[0]
    drawn = picked[1]
    shift = -step_root * bias
    field = drawn - shift
    factor = jnp.sum(drawn * shift - 0.5 * shift * shift, axis=1, keepdims=True) * (1.0 / span)
    factor = jnp.broadcast_to(factor, (local, lanes))
    weighted = (field * step_root).astype(BF16)
    spread = jnp.broadcast_to(weighted.astype(F32)[:, None, :], (local, span, wide)).reshape(local * span, wide)
    kron = jnp.where(same, spread, 0.0).astype(BF16)

    for j in range(block // span):
        summed = jnp.dot(kron, strips[j], preferred_element_type=F32)
        for n in range(BLOCKS):
            partial[:, n, j * span:(j + 1) * span, :] = summed[:, n * block:(n + 1) * block].reshape(local, span, block)
    edge_part = jnp.dot(weighted, level[...], preferred_element_type=F32)

    to_next = [z - 1, z + 1]
    upstream = [last - z, z]
    downstream = [z, last - z]
    at_end = (z == 0) | (z == last)
    end_side = jnp.where(z == 0, 0, 1)
    base = jnp.where(z == 0, 0, half)

    def chain_copy(side, c):
        return remote(
            leaving.at[side, c], arrived.at[side, c], chain_send.at[side, c], chain_recv.at[side, c],
            {"vec": to_next[side]},
        )

    def cross_copy(side, c):
        return remote(
            leaving.at[side, c], crossed.at[c], chain_send.at[side, c], cross_recv.at[c],
            {"vec": to_next[side], "orb": 1 - o},
        )

    def swap_copy(c):
        return remote(leaving.at[end_side, c], given.at[c], swap_send.at[c], swap_recv.at[c], {"orb": 1 - o})

    def extra_copy(side):
        return remote(
            extra_out.at[side], extra_in.at[side], extra_send.at[side], extra_recv.at[side], {"vec": to_next[side]}
        )

    def part_of(side, c):
        return partial[side * half + c // BLOCKS, c % BLOCKS]

    def chain_step(t, carry):
        for side in range(2):
            c = t - SKEW * upstream[side]
            head = upstream[side] == 0
            owner = downstream[side] == 0

            @pl.when((c >= 0) & (c < chunks) & jnp.logical_not(owner))
            def _():
                own = part_of(side, c)
                here = (c // BLOCKS) % 2 == o

                @pl.when(head)
                def _():
                    leaving[side, c] = own.astype(BF16)

                @pl.when(jnp.logical_not(head))
                def _():
                    chain_copy(side, c).wait_recv()
                    leaving[side, c] = (own + arrived[side, c].astype(F32)).astype(BF16)

                @pl.when((downstream[side] > 1) | here)
                def _():
                    chain_copy(side, c).start()

                @pl.when((downstream[side] == 1) & jnp.logical_not(here))
                def _():
                    cross_copy(side, c).start()

                @pl.when(c == 0)
                def _():
                    @pl.when(head)
                    def _():
                        extra_in[side] = jnp.zeros_like(extra_in[side])

                    @pl.when(jnp.logical_not(head))
                    def _():
                        extra_copy(side).wait_recv()

                    extra_out[side, 0:local, :] = extra_in[side, 0:local, :] + factor
                    extra_out[side, local:, :] = extra_in[side, local:, :] + edge_part
                    extra_copy(side).start()

        return carry

    lax.fori_loop(0, SKEW * (last - 1) + chunks, chain_step, jnp.int32(0))

    for hop in hops:
        copies_copy(hop, lax.rem(x + hop, width)).wait_recv()

    def stage_copy(hop, a):
        return remote(
            staged.at[hop, a], pool.at[x, a // 2, o], stage_send.at[hop, a], pool_recv.at[x, a // 2, o],
            {"walk": lax.rem(x + hop, width), "orb": a % 2},
        )

    def swap_core():
        return remote(edge.at[o], edge.at[o], edge_sems.at[0], edge_sems.at[1], {"orb": 1 - o})

    @pl.when(at_end)
    def _():
        for a in range(half):
            for hop in range(width):
                source = copies[lax.rem(x + hop, width), base + a]
                held = walkers[source % local]
                if hop > 0:
                    staged[hop, a] = held
                    stage_copy(hop, a).start()
                else:
                    @pl.when(a % 2 == o)
                    def _():
                        pool[x, a // 2, o] = held

                    @pl.when(a % 2 != o)
                    def _():
                        staged[hop, a] = held
                        stage_copy(hop, a).start()

        def give(c, carry):
            @pl.when((c // BLOCKS) % 2 != o)
            def _():
                leaving[end_side, c] = part_of(end_side, c).astype(BF16)
                swap_copy(c).start()

            return carry

        lax.fori_loop(0, chunks, give, jnp.int32(0))

        for side in range(2):
            @pl.when(end_side == side)
            def _():
                extra_copy(side).wait_recv()
        edge[o] = edge_part + extra_in[end_side, local:, :]
        swap_core().start()
        swap_core().wait_recv()

    share = rows // PARTS
    inward = jnp.where(z == 0, 1, last - 1)
    direct = [a == half - 1 and last <= REACH for a in range(half)]

    def place(w, part):
        return gathered.at[w, pl.ds(part * share, share)]

    def away_z(n):
        return jnp.where(z == 0, n, last - n)

    def spread_copies(a):
        w = base + a
        targets = []
        for n in (range(last, 0, -1) if direct[a] else (1,)):
            for core in (1 - a % 2, a % 2):
                targets.append((core, {"vec": away_z(n), "orb": core}))
        targets.append((1 - a % 2, {"orb": 1 - o}))
        return [
            remote(
                result.at[a // 2, core, pl.ds(part * share, share)], place(w, part),
                own_send.at[a // 2, n, part], slot_recv.at[w, part], where,
            )
            for n, (core, where) in enumerate(targets)
            for part in range(PARTS)
        ]

    def write_copy(w):
        return pltpu.make_async_copy(gathered.at[w], out.at[w], write_sems.at[w])

    upper = lax.broadcasted_iota(jnp.int32, (block, block), 0) < lax.broadcasted_iota(jnp.int32, (block, block), 1)
    level_mask = lax.broadcasted_iota(jnp.int32, (block, block), 0) == lax.broadcasted_iota(jnp.int32, (block, block), 1)

    def finish(a):
        w = base + a
        i = a // 2

        def put(r, c, value):
            full[columns(r), columns(c)] = value

        for n in range(BLOCKS):
            c = a * BLOCKS + n
            remote(
                leaving.at[end_side, c], arrived.at[end_side, c], chain_send.at[end_side, c], chain_recv.at[end_side, c],
                {"vec": inward},
            ).wait_recv()
            swap_copy(c).wait_recv()
            remote(
                leaving.at[end_side, c], crossed.at[c], chain_send.at[end_side, c], cross_recv.at[c],
                {"vec": inward, "orb": 1 - o},
            ).wait_recv()
            kept = part_of(end_side, c) + arrived[end_side, c].astype(F32)
            taken = given[c].astype(F32) + crossed[c].astype(F32)
            for core, value in ((o, kept), (1 - o, taken)):
                if n == 0:
                    flipped = value.T
                    line = edge[core, pl.ds(w, 1), :]
                    put(2 * core, 2 * core, jnp.where(upper | level_mask, value, flipped).astype(BF16))
                    low = jnp.where(level_mask, jnp.broadcast_to(line, (block, block)), jnp.where(upper, flipped, value))
                    put(2 * core + 1, 2 * core + 1, low.astype(BF16))
                else:
                    r, k = ((2 * core, 1), (2 * core, 2 + core), (2 * core + 1, 3 * (1 - core)))[n - 1]
                    value = value.astype(BF16)
                    put(r, k, value)
                    put(k, r, value.T)

        for hop in range(width):
            other = lax.rem(x + hop, width)
            for core in range(2):
                arrival = remote(
                    staged.at[0, 0], pool.at[other, i, core], stage_send.at[0, 0], pool_recv.at[other, i, core],
                    {"walk": other, "orb": core},
                )
                if hop > 0:
                    arrival.wait_recv()
                else:
                    @pl.when(core != o)
                    def _():
                        arrival.wait_recv()
        column = copies[x, w] // local
        for core in range(2):
            start = pool[0, i, core]
            for other in hops:
                start = jnp.where(column == other, pool[other, i, core], start)
            term[core * rows:(core + 1) * rows, :] = start
        running = term[...].astype(F32)
        for degree in range(1, ORDER + 1):
            fresh = (jnp.dot(full[...], term[...], preferred_element_type=F32) * (1.0 / degree)).astype(BF16)
            running = running + fresh.astype(F32)
            if degree < ORDER:
                term[...] = fresh
        result[i] = running.astype(BF16).reshape(2, rows, electrons)
        for copy in spread_copies(a):
            copy.start()
        gathered[w] = result[i, o]
        write_copy(w).start()

    for a in range(half):
        @pl.when(at_end & (a % 2 == o))
        def _():
            finish(a)

    new_log = picked[2][:, 0:lanes] + factor + extra_in[0, 0:local, :] + extra_in[1, 0:local, :]
    for s in range(local):
        out_log[s] = jnp.max(new_log[s:s + 1, :])

    def onward(w, part, hop_to):
        spot = place(w, part)
        return remote(spot, spot, next_send.at[w, part], slot_recv.at[w, part], {"vec": hop_to})

    near = jnp.where(z <= last - z, 0, 1)

    def route(side, a):
        w = side * half + a
        away = jnp.where(side == 0, z, last - z)
        hop_to = jnp.where(side == 0, z + 1, z - 1)
        return w, away, last - away, hop_to

    for a in range(half):
        for side in (near, 1 - near):
            w, away, end, hop_to = route(side, a)

            @pl.when((away > 0) | (o != a % 2))
            def _():
                for part in range(PARTS):
                    onward(w, part, hop_to).wait_recv()
                    if not direct[a]:
                        @pl.when((away > 0) & (end > 0))
                        def _():
                            onward(w, part, hop_to).start()
                write_copy(w).start()

    for w in range(local):
        write_copy(w).wait()

    for copy in bias_copies:
        copy.wait_send()
    for hop in hops:
        facts_copy(hop, x).wait_send()
        copies_copy(hop, x).wait_send()

    def drain(c, carry):
        for side in range(2):
            @pl.when(downstream[side] > 0)
            def _():
                chain_copy(side, c).wait_send()

        @pl.when(at_end & ((c // BLOCKS) % 2 != o))
        def _():
            swap_copy(c).wait_send()

        return carry

    lax.fori_loop(0, chunks, drain, jnp.int32(0))
    for side in range(2):
        @pl.when(downstream[side] > 0)
        def _():
            extra_copy(side).wait_send()

    @pl.when(at_end)
    def _():
        swap_core().wait_send()
        for a in range(half):
            for hop in range(width):
                if hop > 0:
                    stage_copy(hop, a).wait_send()
                else:
                    @pl.when(a % 2 != o)
                    def _():
                        stage_copy(hop, a).wait_send()

            @pl.when(a % 2 == o)
            def _():
                for copy in spread_copies(a):
                    copy.wait_send()

    for a in range(half):
        if not direct[a]:
            for side in range(2):
                w, away, end, hop_to = route(side, a)

                @pl.when((away > 0) & (end > 0))
                def _():
                    for part in range(PARTS):
                        onward(w, part, hop_to).wait_send()


def per_device(depth, width, walkers, inv_intersection, trial, vectors, aux_field, log_weight, copy_list):
    local, rows, electrons = walkers.shape
    count, _, orbitals = vectors.shape
    half = local // 2
    block = orbitals // 4
    span = 2 * block // count
    wide = count * span
    chunks = half * BLOCKS
    mine = half // 2
    lanes = 128
    reach = max(depth - 1, 1) if depth - 1 <= REACH else 1
    dma = pltpu.SemaphoreType.DMA
    anywhere = pl.BlockSpec(memory_space=pl.ANY)
    out, out_log = pl.pallas_call(
        functools.partial(kernel, depth, width),
        out_shape=(
            jax.ShapeDtypeStruct(walkers.shape, BF16),
            jax.ShapeDtypeStruct((local,), F32),
        ),
        in_specs=[anywhere] * 7,
        out_specs=(anywhere, pl.BlockSpec(memory_space=pltpu.SMEM)),
        scratch_shapes=[
            pltpu.VMEM(walkers.shape, BF16),
            pltpu.VMEM(inv_intersection.shape, BF16),
            pltpu.VMEM(trial.shape, BF16),
            pltpu.VMEM(vectors.shape, BF16),
            pltpu.VMEM(aux_field.shape, F32),
            pltpu.SMEM((local,), F32),
            pltpu.SMEM((width, local), jnp.int32),
            pltpu.VMEM((local, rows, electrons), BF16),
            pltpu.VMEM((count, rows, electrons), BF16),
            pltpu.VMEM((block // span, wide, BLOCKS * block), BF16),
            pltpu.VMEM((wide, block), BF16),
            pltpu.VMEM((2, width, local, wide), F32),
            pltpu.VMEM((width, 2 * local, wide), F32),
            pltpu.VMEM((3, local, wide), F32),
            pltpu.VMEM((local, BLOCKS, block, block), F32),
            pltpu.VMEM((2, chunks, block, block), BF16),
            pltpu.VMEM((2, chunks, block, block), BF16),
            pltpu.VMEM((chunks, block, block), BF16),
            pltpu.VMEM((chunks, block, block), BF16),
            pltpu.VMEM((2, 2 * local, lanes), F32),
            pltpu.VMEM((2, 2 * local, lanes), F32),
            pltpu.VMEM((2, local, lanes), F32),
            pltpu.VMEM((width, half, rows, electrons), BF16),
            pltpu.VMEM((width, mine, 2, rows, electrons), BF16),
            pltpu.VMEM((orbitals, orbitals), BF16),
            pltpu.VMEM((orbitals, electrons), BF16),
            pltpu.VMEM((mine, 2, rows, electrons), BF16),
            pltpu.VMEM((local, rows, electrons), BF16),
            dma((7,)),
            dma((width,)),
            dma((width,)),
            dma((width,)),
            dma((width,)),
            dma((2 * width,)),
            dma((2, width)),
            dma((2, chunks)),
            dma((2, chunks)),
            dma((chunks,)),
            dma((chunks,)),
            dma((chunks,)),
            dma((2,)),
            dma((2,)),
            dma((2,)),
            dma((width, half)),
            dma((width, mine, 2)),
            dma((mine, 2 * reach + 1, PARTS)),
            dma((local, PARTS)),
            dma((local, PARTS)),
            dma((local,)),
        ],
        compiler_params=pltpu.CompilerParams(collective_id=0, has_side_effects=True),
    )(walkers, inv_intersection, trial, vectors, aux_field, log_weight, copy_list)
    return out, out_log


def solution(mesh):
    depth, width = mesh.shape["vec"], mesh.shape["walk"]
    assert mesh.shape["orb"] == 2 and depth > 1
    return jax.shard_map(
        functools.partial(per_device, depth, width),
        mesh=mesh,
        in_specs=(
            P(("grp", "walk"), "orb", None),
            P(("grp", "walk"), None, None),
            P(),
            P("vec", "orb", None),
            P(("grp", "walk"), "vec"),
            P(("grp", "walk")),
            P(("grp", "walk")),
        ),
        out_specs=(P(("grp", "walk"), "orb", None), P(("grp", "walk"))),
        check_vma=False,
    )
```

```python
import functools
import math

import jax
import jax.numpy as jnp
from jax import lax
from jax.experimental import pallas as pl
from jax.experimental.pallas import tpu as pltpu
from jax.sharding import PartitionSpec as P

ORDER = 6
BLOCKS = 4
SKEW = 5
PARTS = 2
REACH = 3
MESH = pl.DeviceIdType.MESH
F32 = jnp.float32
BF16 = jnp.bfloat16

step_root = math.sqrt(0.08)


def remote(src, dst, send, recv, where):
    return pltpu.make_async_remote_copy(
        src_ref=src, dst_ref=dst, send_sem=send, recv_sem=recv, device_id=where, device_id_type=MESH
    )


def kernel(
    depth, width,
    walkers_in, inverse_in, trial_in, vectors_in, aux_in, log_in, copies_in,
    out, out_log,
    walkers, inverse, trial, vectors, aux, log_weight, copies,
    green, mixed, strips, level, bias_all, facts, picked, partial, leaving, arrived, given, crossed,
    extra_in, extra_out, edge, staged, pool, full, term, result, gathered,
    load_sems, copies_send, copies_recv, facts_send, facts_recv, bias_send, bias_recv,
    chain_send, chain_recv, cross_recv, swap_send, swap_recv, extra_send, extra_recv, edge_sems,
    stage_send, pool_recv, own_send, next_send, slot_recv, write_sems,
):
    z = lax.axis_index("vec")
    x = lax.axis_index("walk")
    o = lax.axis_index("orb")
    last = depth - 1
    local, rows, electrons = walkers.shape
    count, _, orbitals = vectors.shape
    half = local // 2
    block = orbitals // 4
    span = 2 * block // count
    wide = count * span
    chunks = half * BLOCKS
    mine = half // 2
    lanes = extra_in.shape[2]
    hops = range(1, width)

    barrier = pltpu.get_barrier_semaphore()

    def greet(where):
        pl.semaphore_signal(barrier, inc=1, device_id=where, device_id_type=MESH)

    greet({"orb": 1 - o})
    for hop in hops:
        for core in range(2):
            greet({"walk": lax.rem(x + hop, width), "orb": core})

    @pl.when(z > 0)
    def _():
        for core in range(2):
            greet({"vec": z - 1, "orb": core})

    @pl.when(z < last)
    def _():
        for core in range(2):
            greet({"vec": z + 1, "orb": core})

    pairs = (
        (copies_in, copies.at[x]), (log_in, log_weight), (walkers_in, walkers), (inverse_in, inverse), (trial_in, trial),
        (vectors_in, vectors), (aux_in, aux),
    )
    loads = [pltpu.make_async_copy(src, dst, load_sems.at[n]) for n, (src, dst) in enumerate(pairs)]
    for load in loads:
        load.start()

    loads[2].wait()
    loads[3].wait()
    for w in range(local):
        green[w] = jnp.dot(walkers[w], inverse[w], preferred_element_type=F32).astype(BF16)
    loads[4].wait()
    loads[5].wait()
    for g in range(count):
        mixed[g] = jnp.dot(vectors[g], trial[...], preferred_element_type=F32).astype(BF16)
    gram = jnp.zeros((local * span, wide), F32)
    for j in range(rows // span):
        left = green[:, j * span:(j + 1) * span, :].reshape(local * span, electrons)
        right = mixed[:, j * span:(j + 1) * span, :].reshape(wide, electrons)
        gram = gram + lax.dot_general(left, right, (((1,), (1,)), ((), ())), preferred_element_type=F32)
    row_id = lax.broadcasted_iota(jnp.int32, (local * span, wide), 0)
    col_id = lax.broadcasted_iota(jnp.int32, (local * span, wide), 1)
    same = row_id % span == col_id % span
    folded = jnp.sum(jnp.where(same, gram, 0.0).reshape(local, span, wide), axis=1)
    wide_row = lax.broadcasted_iota(jnp.int32, (wide, wide), 0)
    wide_col = lax.broadcasted_iota(jnp.int32, (wide, wide), 1)
    groups = jnp.where(wide_row // span == wide_col // span, 1.0, 0.0).astype(F32)
    bias_all[o, x] = jnp.dot(folded, groups, precision=lax.Precision.HIGHEST, preferred_element_type=F32)

    loads[6].wait()
    loads[0].wait()
    loads[1].wait()
    pick_row = lax.broadcasted_iota(jnp.int32, (count, wide), 0)
    pick_col = lax.broadcasted_iota(jnp.int32, (count, wide), 1)
    pick = jnp.where(pick_row == pick_col // span, 1.0, 0.0).astype(F32)
    facts[x, 0:local, :] = jnp.dot(aux[...], pick, precision=lax.Precision.HIGHEST, preferred_element_type=F32)
    walker_id = lax.broadcasted_iota(jnp.int32, (local, wide), 0)
    weights = jnp.zeros((local, wide), F32)
    for w in range(local):
        weights = jnp.where(walker_id == w, log_weight[w], weights)
    facts[x, local:2 * local, :] = weights

    sides = jnp.where(z > 0, 2, 0) + jnp.where(z < last, 2, 0)
    pl.semaphore_wait(barrier, 1 + 2 * (width - 1) + sides)

    bias_peers = [{"walk": lax.rem(x + hop, width), "orb": core} for hop in hops for core in range(2)] + [{"orb": 1 - o}]
    bias_copies = [
        remote(bias_all.at[o, x], bias_all.at[o, x], bias_send.at[n], bias_recv.at[o, x], where)
        for n, where in enumerate(bias_peers)
    ]
    for copy in bias_copies:
        copy.start()

    def facts_copy(hop, owner):
        return remote(
            facts.at[owner], facts.at[owner], facts_send.at[hop], facts_recv.at[owner], {"walk": lax.rem(x + hop, width)}
        )

    def copies_copy(hop, owner):
        return remote(
            copies.at[owner], copies.at[owner], copies_send.at[hop], copies_recv.at[owner],
            {"walk": lax.rem(x + hop, width)},
        )

    for hop in hops:
        copies_copy(hop, x).start()
        facts_copy(hop, x).start()

    chunk_row = lax.broadcasted_iota(jnp.int32, (count, span, block), 1)
    chunk_col = lax.broadcasted_iota(jnp.int32, (count, span, block), 2)
    crossing = jnp.zeros((count, span, block), F32)

    def columns(n):
        return pl.ds(pl.multiple_of(n * block, block), block)

    for j in range(block // span):
        here = slice(j * span, (j + 1) * span)
        below = slice(block + j * span, block + (j + 1) * span)
        first = vectors[:, here, columns(2 * o)].astype(F32)
        second = vectors[:, below, columns(1 + 2 * o)].astype(F32)
        crossing = crossing + jnp.where(chunk_row + j * span == chunk_col, second, 0.0)
        joined = jnp.where(chunk_row + j * span <= chunk_col, first, second).astype(BF16)
        strips[j, :, 0:block] = joined.reshape(wide, block)
        strips[j, :, block:2 * block] = vectors[:, here, block:2 * block].reshape(wide, block)
        strips[j, :, 2 * block:3 * block] = vectors[:, here, columns(2 + o)].reshape(wide, block)
        strips[j, :, 3 * block:] = vectors[:, below, columns(3 * (1 - o))].reshape(wide, block)
    level[...] = crossing.reshape(wide, block).astype(BF16)

    for hop in hops:
        other = lax.rem(x + hop, width)
        facts_copy(hop, other).wait_recv()
        for core in range(2):
            remote(
                bias_all.at[core, other], bias_all.at[core, other], bias_send.at[0], bias_recv.at[core, other], {"walk": other}
            ).wait_recv()
    remote(bias_all.at[1 - o, x], bias_all.at[1 - o, x], bias_send.at[0], bias_recv.at[1 - o, x], {"orb": 1 - o}).wait_recv()

    for s in range(local):
        source = copies[x, s]
        column = source // local
        at = source % local
        row = pl.ds(at, 1)
        picked[0, s:s + 1, :] = bias_all[0, column, row, :] + bias_all[1, column, row, :]
        picked[1, s:s + 1, :] = facts[column, row, :]
        picked[2, s:s + 1, :] = facts[column, pl.ds(local + at, 1), :]

    bias = picked[0]
    drawn = picked[1]
    shift = -step_root * bias
    field = drawn - shift
    factor = jnp.sum(drawn * shift - 0.5 * shift * shift, axis=1, keepdims=True) * (1.0 / span)
    factor = jnp.broadcast_to(factor, (local, lanes))
    weighted = (field * step_root).astype(BF16)
    spread = jnp.broadcast_to(weighted.astype(F32)[:, None, :], (local, span, wide)).reshape(local * span, wide)
    kron = jnp.where(same, spread, 0.0).astype(BF16)

    for j in range(block // span):
        summed = jnp.dot(kron, strips[j], preferred_element_type=F32)
        for n in range(BLOCKS):
            partial[:, n, j * span:(j + 1) * span, :] = summed[:, n * block:(n + 1) * block].reshape(local, span, block)
    edge_part = jnp.dot(weighted, level[...], preferred_element_type=F32)

    to_next = [z - 1, z + 1]
    upstream = [last - z, z]
    downstream = [z, last - z]
    at_end = (z == 0) | (z == last)
    end_side = jnp.where(z == 0, 0, 1)
    base = jnp.where(z == 0, 0, half)

    def chain_copy(side, c):
        return remote(
            leaving.at[side, c], arrived.at[side, c], chain_send.at[side, c], chain_recv.at[side, c],
            {"vec": to_next[side]},
        )

    def cross_copy(side, c):
        return remote(
            leaving.at[side, c], crossed.at[c], chain_send.at[side, c], cross_recv.at[c],
            {"vec": to_next[side], "orb": 1 - o},
        )

    def swap_copy(c):
        return remote(leaving.at[end_side, c], given.at[c], swap_send.at[c], swap_recv.at[c], {"orb": 1 - o})

    def extra_copy(side):
        return remote(
            extra_out.at[side], extra_in.at[side], extra_send.at[side], extra_recv.at[side], {"vec": to_next[side]}
        )

    def part_of(side, c):
        return partial[side * half + c // BLOCKS, c % BLOCKS]

    def chain_step(t, carry):
        for side in range(2):
            c = t - SKEW * upstream[side]
            head = upstream[side] == 0
            owner = downstream[side] == 0

            @pl.when((c >= 0) & (c < chunks) & jnp.logical_not(owner))
            def _():
                own = part_of(side, c)
                here = (c // BLOCKS) % 2 == o

                @pl.when(head)
                def _():
                    leaving[side, c] = own.astype(BF16)

                @pl.when(jnp.logical_not(head))
                def _():
                    chain_copy(side, c).wait_recv()
                    leaving[side, c] = (own + arrived[side, c].astype(F32)).astype(BF16)

                @pl.when((downstream[side] > 1) | here)
                def _():
                    chain_copy(side, c).start()

                @pl.when((downstream[side] == 1) & jnp.logical_not(here))
                def _():
                    cross_copy(side, c).start()

                @pl.when(c == 0)
                def _():
                    @pl.when(head)
                    def _():
                        extra_in[side] = jnp.zeros_like(extra_in[side])

                    @pl.when(jnp.logical_not(head))
                    def _():
                        extra_copy(side).wait_recv()

                    extra_out[side, 0:local, :] = extra_in[side, 0:local, :] + factor
                    extra_out[side, local:, :] = extra_in[side, local:, :] + edge_part
                    extra_copy(side).start()

        return carry

    lax.fori_loop(0, SKEW * (last - 1) + chunks, chain_step, jnp.int32(0))

    for hop in hops:
        copies_copy(hop, lax.rem(x + hop, width)).wait_recv()

    def stage_copy(hop, a):
        return remote(
            staged.at[hop, a], pool.at[x, a // 2, o], stage_send.at[hop, a], pool_recv.at[x, a // 2, o],
            {"walk": lax.rem(x + hop, width), "orb": a % 2},
        )

    def swap_core():
        return remote(edge.at[o], edge.at[o], edge_sems.at[0], edge_sems.at[1], {"orb": 1 - o})

    @pl.when(at_end)
    def _():
        for a in range(half):
            for hop in range(width):
                source = copies[lax.rem(x + hop, width), base + a]
                held = walkers[source % local]
                if hop > 0:
                    staged[hop, a] = held
                    stage_copy(hop, a).start()
                else:
                    @pl.when(a % 2 == o)
                    def _():
                        pool[x, a // 2, o] = held

                    @pl.when(a % 2 != o)
                    def _():
                        staged[hop, a] = held
                        stage_copy(hop, a).start()

        def give(c, carry):
            @pl.when((c // BLOCKS) % 2 != o)
            def _():
                leaving[end_side, c] = part_of(end_side, c).astype(BF16)
                swap_copy(c).start()

            return carry

        lax.fori_loop(0, chunks, give, jnp.int32(0))

        for side in range(2):
            @pl.when(end_side == side)
            def _():
                extra_copy(side).wait_recv()
        edge[o] = edge_part + extra_in[end_side, local:, :]
        swap_core().start()
        swap_core().wait_recv()

    share = rows // PARTS
    inward = jnp.where(z == 0, 1, last - 1)
    short = last <= REACH
    plans = [tuple(range(last if a == half - 1 else min(last, 2), 0, -1)) if short else (1,) for a in range(half)]

    def place(w, part):
        return gathered.at[w, pl.ds(part * share, share)]

    def away_z(n):
        return jnp.where(z == 0, n, last - n)

    def spread_copies(a):
        w = base + a
        targets = []
        for n in plans[a]:
            for core in (1 - a % 2, a % 2):
                targets.append((core, {"vec": away_z(n), "orb": core}))
        targets.append((1 - a % 2, {"orb": 1 - o}))
        return [
            remote(
                result.at[a // 2, core, pl.ds(part * share, share)], place(w, part),
                own_send.at[a // 2, n, part], slot_recv.at[w, part], where,
            )
            for n, (core, where) in enumerate(targets)
            for part in range(PARTS)
        ]

    def write_copy(w):
        return pltpu.make_async_copy(gathered.at[w], out.at[w], write_sems.at[w])

    upper = lax.broadcasted_iota(jnp.int32, (block, block), 0) < lax.broadcasted_iota(jnp.int32, (block, block), 1)
    level_mask = lax.broadcasted_iota(jnp.int32, (block, block), 0) == lax.broadcasted_iota(jnp.int32, (block, block), 1)

    def finish(a):
        w = base + a
        i = a // 2

        def put(r, c, value):
            full[columns(r), columns(c)] = value

        for n in range(BLOCKS):
            c = a * BLOCKS + n
            remote(
                leaving.at[end_side, c], arrived.at[end_side, c], chain_send.at[end_side, c], chain_recv.at[end_side, c],
                {"vec": inward},
            ).wait_recv()
            swap_copy(c).wait_recv()
            remote(
                leaving.at[end_side, c], crossed.at[c], chain_send.at[end_side, c], cross_recv.at[c],
                {"vec": inward, "orb": 1 - o},
            ).wait_recv()
            kept = part_of(end_side, c) + arrived[end_side, c].astype(F32)
            taken = given[c].astype(F32) + crossed[c].astype(F32)
            for core, value in ((o, kept), (1 - o, taken)):
                if n == 0:
                    flipped = value.T
                    line = edge[core, pl.ds(w, 1), :]
                    put(2 * core, 2 * core, jnp.where(upper | level_mask, value, flipped).astype(BF16))
                    low = jnp.where(level_mask, jnp.broadcast_to(line, (block, block)), jnp.where(upper, flipped, value))
                    put(2 * core + 1, 2 * core + 1, low.astype(BF16))
                else:
                    r, k = ((2 * core, 1), (2 * core, 2 + core), (2 * core + 1, 3 * (1 - core)))[n - 1]
                    value = value.astype(BF16)
                    put(r, k, value)
                    put(k, r, value.T)

        for hop in range(width):
            other = lax.rem(x + hop, width)
            for core in range(2):
                arrival = remote(
                    staged.at[0, 0], pool.at[other, i, core], stage_send.at[0, 0], pool_recv.at[other, i, core],
                    {"walk": other, "orb": core},
                )
                if hop > 0:
                    arrival.wait_recv()
                else:
                    @pl.when(core != o)
                    def _():
                        arrival.wait_recv()
        column = copies[x, w] // local
        for core in range(2):
            start = pool[0, i, core]
            for other in hops:
                start = jnp.where(column == other, pool[other, i, core], start)
            term[core * rows:(core + 1) * rows, :] = start
        running = term[...].astype(F32)
        for degree in range(1, ORDER + 1):
            fresh = (jnp.dot(full[...], term[...], preferred_element_type=F32) * (1.0 / degree)).astype(BF16)
            running = running + fresh.astype(F32)
            if degree < ORDER:
                term[...] = fresh
        result[i] = running.astype(BF16).reshape(2, rows, electrons)
        for copy in spread_copies(a):
            copy.start()
        gathered[w] = result[i, o]
        write_copy(w).start()

    for a in range(half):
        @pl.when(at_end & (a % 2 == o))
        def _():
            finish(a)

    new_log = picked[2][:, 0:lanes] + factor + extra_in[0, 0:local, :] + extra_in[1, 0:local, :]
    for s in range(local):
        out_log[s] = jnp.max(new_log[s:s + 1, :])

    def onward(w, part, hop_to):
        spot = place(w, part)
        return remote(spot, spot, next_send.at[w, part], slot_recv.at[w, part], {"vec": hop_to})

    near = jnp.where(z <= last - z, 0, 1)

    def route(side, a):
        w = side * half + a
        away = jnp.where(side == 0, z, last - z)
        hop_to = jnp.where(side == 0, z + 1, z - 1)
        return w, away, last - away, hop_to

    for a in range(half):
        for side in (near, 1 - near):
            w, away, end, hop_to = route(side, a)

            @pl.when((away > 0) | (o != a % 2))
            def _():
                for part in range(PARTS):
                    onward(w, part, hop_to).wait_recv()
                    if plans[a][0] < last:
                        @pl.when((away >= plans[a][0]) & (end > 0))
                        def _():
                            onward(w, part, hop_to).start()
                write_copy(w).start()

    for w in range(local):
        write_copy(w).wait()

    for copy in bias_copies:
        copy.wait_send()
    for hop in hops:
        facts_copy(hop, x).wait_send()
        copies_copy(hop, x).wait_send()

    def drain(c, carry):
        for side in range(2):
            @pl.when(downstream[side] > 0)
            def _():
                chain_copy(side, c).wait_send()

        @pl.when(at_end & ((c // BLOCKS) % 2 != o))
        def _():
            swap_copy(c).wait_send()

        return carry

    lax.fori_loop(0, chunks, drain, jnp.int32(0))
    for side in range(2):
        @pl.when(downstream[side] > 0)
        def _():
            extra_copy(side).wait_send()

    @pl.when(at_end)
    def _():
        swap_core().wait_send()
        for a in range(half):
            for hop in range(width):
                if hop > 0:
                    stage_copy(hop, a).wait_send()
                else:
                    @pl.when(a % 2 != o)
                    def _():
                        stage_copy(hop, a).wait_send()

            @pl.when(a % 2 == o)
            def _():
                for copy in spread_copies(a):
                    copy.wait_send()

    for a in range(half):
        if plans[a][0] < last:
            for side in range(2):
                w, away, end, hop_to = route(side, a)

                @pl.when((away >= plans[a][0]) & (end > 0))
                def _():
                    for part in range(PARTS):
                        onward(w, part, hop_to).wait_send()


def per_device(depth, width, walkers, inv_intersection, trial, vectors, aux_field, log_weight, copy_list):
    local, rows, electrons = walkers.shape
    count, _, orbitals = vectors.shape
    half = local // 2
    block = orbitals // 4
    span = 2 * block // count
    wide = count * span
    chunks = half * BLOCKS
    mine = half // 2
    lanes = 128
    reach = max(depth - 1, 1) if depth - 1 <= REACH else 1
    dma = pltpu.SemaphoreType.DMA
    anywhere = pl.BlockSpec(memory_space=pl.ANY)
    out, out_log = pl.pallas_call(
        functools.partial(kernel, depth, width),
        out_shape=(
            jax.ShapeDtypeStruct(walkers.shape, BF16),
            jax.ShapeDtypeStruct((local,), F32),
        ),
        in_specs=[anywhere] * 7,
        out_specs=(anywhere, pl.BlockSpec(memory_space=pltpu.SMEM)),
        scratch_shapes=[
            pltpu.VMEM(walkers.shape, BF16),
            pltpu.VMEM(inv_intersection.shape, BF16),
            pltpu.VMEM(trial.shape, BF16),
            pltpu.VMEM(vectors.shape, BF16),
            pltpu.VMEM(aux_field.shape, F32),
            pltpu.SMEM((local,), F32),
            pltpu.SMEM((width, local), jnp.int32),
            pltpu.VMEM((local, rows, electrons), BF16),
            pltpu.VMEM((count, rows, electrons), BF16),
            pltpu.VMEM((block // span, wide, BLOCKS * block), BF16),
            pltpu.VMEM((wide, block), BF16),
            pltpu.VMEM((2, width, local, wide), F32),
            pltpu.VMEM((width, 2 * local, wide), F32),
            pltpu.VMEM((3, local, wide), F32),
            pltpu.VMEM((local, BLOCKS, block, block), F32),
            pltpu.VMEM((2, chunks, block, block), BF16),
            pltpu.VMEM((2, chunks, block, block), BF16),
            pltpu.VMEM((chunks, block, block), BF16),
            pltpu.VMEM((chunks, block, block), BF16),
            pltpu.VMEM((2, 2 * local, lanes), F32),
            pltpu.VMEM((2, 2 * local, lanes), F32),
            pltpu.VMEM((2, local, lanes), F32),
            pltpu.VMEM((width, half, rows, electrons), BF16),
            pltpu.VMEM((width, mine, 2, rows, electrons), BF16),
            pltpu.VMEM((orbitals, orbitals), BF16),
            pltpu.VMEM((orbitals, electrons), BF16),
            pltpu.VMEM((mine, 2, rows, electrons), BF16),
            pltpu.VMEM((local, rows, electrons), BF16),
            dma((7,)),
            dma((width,)),
            dma((width,)),
            dma((width,)),
            dma((width,)),
            dma((2 * width,)),
            dma((2, width)),
            dma((2, chunks)),
            dma((2, chunks)),
            dma((chunks,)),
            dma((chunks,)),
            dma((chunks,)),
            dma((2,)),
            dma((2,)),
            dma((2,)),
            dma((width, half)),
            dma((width, mine, 2)),
            dma((mine, 2 * reach + 1, PARTS)),
            dma((local, PARTS)),
            dma((local, PARTS)),
            dma((local,)),
        ],
        compiler_params=pltpu.CompilerParams(collective_id=0, has_side_effects=True),
    )(walkers, inv_intersection, trial, vectors, aux_field, log_weight, copy_list)
    return out, out_log


def solution(mesh):
    depth, width = mesh.shape["vec"], mesh.shape["walk"]
    assert mesh.shape["orb"] == 2 and depth > 1
    return jax.shard_map(
        functools.partial(per_device, depth, width),
        mesh=mesh,
        in_specs=(
            P(("grp", "walk"), "orb", None),
            P(("grp", "walk"), None, None),
            P(),
            P("vec", "orb", None),
            P(("grp", "walk"), "vec"),
            P(("grp", "walk")),
            P(("grp", "walk")),
        ),
        out_specs=(P(("grp", "walk"), "orb", None), P(("grp", "walk"))),
        check_vma=False,
    )
```

```python
import functools
import math

import jax
import jax.numpy as jnp
from jax import lax
from jax.experimental import pallas as pl
from jax.experimental.pallas import tpu as pltpu
from jax.sharding import PartitionSpec as P

ORDER = 6
BLOCKS = 4
SUB = 2
SKEW = 10
PARTS = 2
REACH = 3
PLANS = ((2, -1, 1), (3, 2, 1), (2, 1), (2, 1))
MESH = pl.DeviceIdType.MESH
F32 = jnp.float32
BF16 = jnp.bfloat16

step_root = math.sqrt(0.08)


def remote(src, dst, send, recv, where):
    return pltpu.make_async_remote_copy(
        src_ref=src, dst_ref=dst, send_sem=send, recv_sem=recv, device_id=where, device_id_type=MESH
    )


def kernel(
    depth, width,
    walkers_in, inverse_in, trial_in, vectors_in, aux_in, log_in, copies_in,
    out, out_log,
    walkers, inverse, trial, vectors, aux, log_weight, copies,
    green, mixed, strips, level, bias_all, facts, picked, partial, leaving, arrived, given, crossed,
    back, extra_in, extra_out, edge, staged, pool, full, term, result, gathered,
    load_sems, copies_send, copies_recv, facts_send, facts_recv, bias_send, bias_recv,
    chain_send, chain_recv, cross_recv, back_recv, swap_send, swap_recv, extra_send, extra_recv, edge_sems,
    stage_send, pool_recv, own_send, next_send, slot_recv, write_sems,
):
    z = lax.axis_index("vec")
    x = lax.axis_index("walk")
    o = lax.axis_index("orb")
    last = depth - 1
    local, rows, electrons = walkers.shape
    count, _, orbitals = vectors.shape
    half = local // 2
    block = orbitals // 4
    span = 2 * block // count
    wide = count * span
    piece = block // SUB
    each = BLOCKS * SUB
    chunks = half * each
    mine = half // 2
    lanes = extra_in.shape[2]
    insets = [1 if a == half - 1 and last >= REACH else 0 for a in range(half)]
    hops = range(1, width)

    barrier = pltpu.get_barrier_semaphore()

    def greet(where):
        pl.semaphore_signal(barrier, inc=1, device_id=where, device_id_type=MESH)

    greet({"orb": 1 - o})
    for hop in hops:
        for core in range(2):
            greet({"walk": lax.rem(x + hop, width), "orb": core})

    @pl.when(z > 0)
    def _():
        for core in range(2):
            greet({"vec": z - 1, "orb": core})

    @pl.when(z < last)
    def _():
        for core in range(2):
            greet({"vec": z + 1, "orb": core})

    pairs = (
        (copies_in, copies.at[x]), (log_in, log_weight), (walkers_in, walkers), (inverse_in, inverse), (trial_in, trial),
        (vectors_in, vectors), (aux_in, aux),
    )
    loads = [pltpu.make_async_copy(src, dst, load_sems.at[n]) for n, (src, dst) in enumerate(pairs)]
    for load in loads:
        load.start()

    loads[2].wait()
    loads[3].wait()
    for w in range(local):
        green[w] = jnp.dot(walkers[w], inverse[w], preferred_element_type=F32).astype(BF16)
    loads[4].wait()
    loads[5].wait()
    for g in range(count):
        mixed[g] = jnp.dot(vectors[g], trial[...], preferred_element_type=F32).astype(BF16)
    gram = jnp.zeros((local * span, wide), F32)
    for j in range(rows // span):
        left = green[:, j * span:(j + 1) * span, :].reshape(local * span, electrons)
        right = mixed[:, j * span:(j + 1) * span, :].reshape(wide, electrons)
        gram = gram + lax.dot_general(left, right, (((1,), (1,)), ((), ())), preferred_element_type=F32)
    row_id = lax.broadcasted_iota(jnp.int32, (local * span, wide), 0)
    col_id = lax.broadcasted_iota(jnp.int32, (local * span, wide), 1)
    same = row_id % span == col_id % span
    folded = jnp.sum(jnp.where(same, gram, 0.0).reshape(local, span, wide), axis=1)
    wide_row = lax.broadcasted_iota(jnp.int32, (wide, wide), 0)
    wide_col = lax.broadcasted_iota(jnp.int32, (wide, wide), 1)
    groups = jnp.where(wide_row // span == wide_col // span, 1.0, 0.0).astype(F32)
    bias_all[o, x] = jnp.dot(folded, groups, precision=lax.Precision.HIGHEST, preferred_element_type=F32)

    loads[6].wait()
    loads[0].wait()
    loads[1].wait()
    pick_row = lax.broadcasted_iota(jnp.int32, (count, wide), 0)
    pick_col = lax.broadcasted_iota(jnp.int32, (count, wide), 1)
    pick = jnp.where(pick_row == pick_col // span, 1.0, 0.0).astype(F32)
    facts[x, 0:local, :] = jnp.dot(aux[...], pick, precision=lax.Precision.HIGHEST, preferred_element_type=F32)
    walker_id = lax.broadcasted_iota(jnp.int32, (local, wide), 0)
    weights = jnp.zeros((local, wide), F32)
    for w in range(local):
        weights = jnp.where(walker_id == w, log_weight[w], weights)
    facts[x, local:2 * local, :] = weights

    sides = jnp.where(z > 0, 2, 0) + jnp.where(z < last, 2, 0)
    pl.semaphore_wait(barrier, 1 + 2 * (width - 1) + sides)

    bias_peers = [{"walk": lax.rem(x + hop, width), "orb": core} for hop in hops for core in range(2)] + [{"orb": 1 - o}]
    bias_copies = [
        remote(bias_all.at[o, x], bias_all.at[o, x], bias_send.at[n], bias_recv.at[o, x], where)
        for n, where in enumerate(bias_peers)
    ]
    for copy in bias_copies:
        copy.start()

    def facts_copy(hop, owner):
        return remote(
            facts.at[owner], facts.at[owner], facts_send.at[hop], facts_recv.at[owner], {"walk": lax.rem(x + hop, width)}
        )

    def copies_copy(hop, owner):
        return remote(
            copies.at[owner], copies.at[owner], copies_send.at[hop], copies_recv.at[owner],
            {"walk": lax.rem(x + hop, width)},
        )

    for hop in hops:
        copies_copy(hop, x).start()
        facts_copy(hop, x).start()

    chunk_row = lax.broadcasted_iota(jnp.int32, (count, span, block), 1)
    chunk_col = lax.broadcasted_iota(jnp.int32, (count, span, block), 2)
    crossing = jnp.zeros((count, span, block), F32)

    def columns(n):
        return pl.ds(pl.multiple_of(n * block, block), block)

    for j in range(block // span):
        here = slice(j * span, (j + 1) * span)
        below = slice(block + j * span, block + (j + 1) * span)
        first = vectors[:, here, columns(2 * o)].astype(F32)
        second = vectors[:, below, columns(1 + 2 * o)].astype(F32)
        crossing = crossing + jnp.where(chunk_row + j * span == chunk_col, second, 0.0)
        joined = jnp.where(chunk_row + j * span <= chunk_col, first, second).astype(BF16)
        strips[j, :, 0:block] = joined.reshape(wide, block)
        strips[j, :, block:2 * block] = vectors[:, here, block:2 * block].reshape(wide, block)
        strips[j, :, 2 * block:3 * block] = vectors[:, here, columns(2 + o)].reshape(wide, block)
        strips[j, :, 3 * block:] = vectors[:, below, columns(3 * (1 - o))].reshape(wide, block)
    level[...] = crossing.reshape(wide, block).astype(BF16)

    for hop in hops:
        other = lax.rem(x + hop, width)
        facts_copy(hop, other).wait_recv()
        for core in range(2):
            remote(
                bias_all.at[core, other], bias_all.at[core, other], bias_send.at[0], bias_recv.at[core, other], {"walk": other}
            ).wait_recv()
    remote(bias_all.at[1 - o, x], bias_all.at[1 - o, x], bias_send.at[0], bias_recv.at[1 - o, x], {"orb": 1 - o}).wait_recv()

    for s in range(local):
        source = copies[x, s]
        column = source // local
        at = source % local
        row = pl.ds(at, 1)
        picked[0, s:s + 1, :] = bias_all[0, column, row, :] + bias_all[1, column, row, :]
        picked[1, s:s + 1, :] = facts[column, row, :]
        picked[2, s:s + 1, :] = facts[column, pl.ds(local + at, 1), :]

    bias = picked[0]
    drawn = picked[1]
    shift = -step_root * bias
    field = drawn - shift
    factor = jnp.sum(drawn * shift - 0.5 * shift * shift, axis=1, keepdims=True) * (1.0 / span)
    factor = jnp.broadcast_to(factor, (local, lanes))
    weighted = (field * step_root).astype(BF16)
    spread = jnp.broadcast_to(weighted.astype(F32)[:, None, :], (local, span, wide)).reshape(local * span, wide)
    kron = jnp.where(same, spread, 0.0).astype(BF16)

    for j in range(block // span):
        summed = jnp.dot(kron, strips[j], preferred_element_type=F32)
        for n in range(BLOCKS):
            partial[:, n, j * span:(j + 1) * span, :] = summed[:, n * block:(n + 1) * block].reshape(local, span, block)
    edge_part = jnp.dot(weighted, level[...], preferred_element_type=F32)

    to_next = [z - 1, z + 1]
    upstream = [last - z, z]
    downstream = [z, last - z]
    at_end = (z == 0) | (z == last)
    near = jnp.where(z <= last - z, 0, 1)
    base = near * half
    inward = jnp.where(near == 0, z + 1, z - 1)
    at_owner = [(z == n) | (z == last - n) for n in insets]

    def depth_of(c):
        return sum(jnp.where(c // each == a, n, 0) for a, n in enumerate(insets) if n) + jnp.int32(0)

    def chain_copy(side, c):
        return remote(
            leaving.at[side, c], arrived.at[side, c], chain_send.at[side, c], chain_recv.at[side, c],
            {"vec": to_next[side]},
        )

    def cross_copy(side, c):
        return remote(
            leaving.at[side, c], crossed.at[c], chain_send.at[side, c], cross_recv.at[c],
            {"vec": to_next[side], "orb": 1 - o},
        )

    def swap_copy(c):
        return remote(leaving.at[near, c], given.at[c], swap_send.at[c], swap_recv.at[c], {"orb": 1 - o})

    def extra_copy(side):
        return remote(
            extra_out.at[side], extra_in.at[side], extra_send.at[side], extra_recv.at[side], {"vec": to_next[side]}
        )

    def back_copy(c):
        return remote(
            leaving.at[near, c], back.at[o, c], chain_send.at[near, c], back_recv.at[o, c],
            {"vec": inward, "orb": (c // each) % 2},
        )

    def part_of(side, c):
        at = c % each
        return partial[side * half + c // each, at // SUB, pl.ds(pl.multiple_of((at % SUB) * piece, piece), piece), :]

    def chain_step(t, carry):
        for side in range(2):
            c = t - SKEW * upstream[side]
            head = upstream[side] == 0
            togo = downstream[side] - depth_of(c)

            @pl.when((c >= 0) & (c < chunks) & (togo > 0))
            def _():
                own = part_of(side, c)
                here = (c // each) % 2 == o

                @pl.when(head)
                def _():
                    leaving[side, c] = own.astype(BF16)

                @pl.when(jnp.logical_not(head))
                def _():
                    chain_copy(side, c).wait_recv()
                    leaving[side, c] = (own + arrived[side, c].astype(F32)).astype(BF16)

                @pl.when((togo > 1) | here)
                def _():
                    chain_copy(side, c).start()

                @pl.when((togo == 1) & jnp.logical_not(here))
                def _():
                    cross_copy(side, c).start()

                @pl.when(c == 0)
                def _():
                    @pl.when(head)
                    def _():
                        extra_in[side] = jnp.zeros_like(extra_in[side])

                    @pl.when(jnp.logical_not(head))
                    def _():
                        extra_copy(side).wait_recv()

                    extra_out[side, 0:local, :] = extra_in[side, 0:local, :] + factor
                    extra_out[side, local:, :] = extra_in[side, local:, :] + edge_part
                    extra_copy(side).start()

        return carry

    lax.fori_loop(0, SKEW * (last - 1) + chunks, chain_step, jnp.int32(0))

    for hop in hops:
        copies_copy(hop, lax.rem(x + hop, width)).wait_recv()

    def stage_copy(hop, a):
        return remote(
            staged.at[hop, a], pool.at[x, a // 2, o], stage_send.at[hop, a], pool_recv.at[x, a // 2, o],
            {"walk": lax.rem(x + hop, width), "orb": a % 2},
        )

    def swap_core():
        return remote(edge.at[o], edge.at[o], edge_sems.at[0], edge_sems.at[1], {"orb": 1 - o})

    for a in range(half):
        @pl.when(at_owner[a])
        def _():
            for hop in range(width):
                source = copies[lax.rem(x + hop, width), base + a]
                held = walkers[source % local]
                if hop > 0:
                    staged[hop, a] = held
                    stage_copy(hop, a).start()
                else:
                    @pl.when(a % 2 == o)
                    def _():
                        pool[x, a // 2, o] = held

                    @pl.when(a % 2 != o)
                    def _():
                        staged[hop, a] = held
                        stage_copy(hop, a).start()

            @pl.when(a % 2 != o)
            def _():
                def give(c, carry):
                    leaving[near, c] = part_of(near, c).astype(BF16)
                    swap_copy(c).start()
                    return carry

                lax.fori_loop(a * each, (a + 1) * each, give, jnp.int32(0))

        if insets[a]:
            @pl.when(at_end)
            def _():
                def back_step(c, carry):
                    leaving[near, c] = part_of(near, c).astype(BF16)
                    back_copy(c).start()
                    return carry

                lax.fori_loop(a * each, (a + 1) * each, back_step, jnp.int32(0))

    for side in range(2):
        @pl.when(at_end & (near == side))
        def _():
            extra_copy(side).wait_recv()

    owning = functools.reduce(jnp.logical_or, at_owner)

    @pl.when(owning)
    def _():
        edge[o] = edge_part + extra_in[0, local:, :] + extra_in[1, local:, :]
        swap_core().start()
        swap_core().wait_recv()

    share = rows // PARTS
    short = last <= REACH
    plans = [
        tuple(n for n in PLANS[min(half - a, len(PLANS)) - 1] if -insets[a] <= n <= last - insets[a])
        if short else (1,) + (-1,) * insets[a] for a in range(half)
    ]

    def passes(a, away):
        if not short:
            return (away > 0) & (away < last - insets[a])
        gaps = [away == n for n in range(1, last - insets[a]) if n + 1 not in plans[a]]
        return functools.reduce(jnp.logical_or, gaps, jnp.bool_(False))

    def place(w, part):
        return gathered.at[w, pl.ds(part * share, share)]

    def away_z(n):
        return jnp.where(near == 0, z + n, z - n)

    def spread_copies(a):
        w = base + a
        targets = []
        for n in plans[a]:
            for core in (1 - a % 2, a % 2):
                targets.append((core, {"vec": away_z(n), "orb": core}))
        targets.append((1 - a % 2, {"orb": 1 - o}))
        return [
            remote(
                result.at[a // 2, core, pl.ds(part * share, share)], place(w, part),
                own_send.at[a // 2, n, part], slot_recv.at[w, part], where,
            )
            for n, (core, where) in enumerate(targets)
            for part in range(PARTS)
        ]

    def write_copy(w):
        return pltpu.make_async_copy(gathered.at[w], out.at[w], write_sems.at[w])

    upper = lax.broadcasted_iota(jnp.int32, (block, block), 0) < lax.broadcasted_iota(jnp.int32, (block, block), 1)
    level_mask = lax.broadcasted_iota(jnp.int32, (block, block), 0) == lax.broadcasted_iota(jnp.int32, (block, block), 1)

    def finish(a):
        w = base + a
        i = a // 2

        def put(r, c, value):
            full[columns(r), columns(c)] = value

        for n in range(BLOCKS):
            first_c = a * each + n * SUB
            for c in range(first_c, first_c + SUB):
                remote(
                    leaving.at[near, c], arrived.at[near, c], chain_send.at[near, c], chain_recv.at[near, c], {"vec": inward}
                ).wait_recv()
                swap_copy(c).wait_recv()
                remote(
                    leaving.at[near, c], crossed.at[c], chain_send.at[near, c], cross_recv.at[c],
                    {"vec": inward, "orb": 1 - o},
                ).wait_recv()
                if insets[a]:
                    for core in range(2):
                        remote(
                            leaving.at[near, c], back.at[core, c], chain_send.at[near, c], back_recv.at[core, c],
                            {"vec": away_z(-1), "orb": core},
                        ).wait_recv()
            run = pl.ds(first_c, SUB)
            kept = partial[w, n] + arrived[near, run].reshape(block, block).astype(F32)
            taken = given[run].reshape(block, block).astype(F32) + crossed[run].reshape(block, block).astype(F32)
            if insets[a]:
                kept = kept + back[o, run].reshape(block, block).astype(F32)
                taken = taken + back[1 - o, run].reshape(block, block).astype(F32)
            for core, value in ((o, kept), (1 - o, taken)):
                if n == 0:
                    flipped = value.T
                    line = edge[core, pl.ds(w, 1), :]
                    put(2 * core, 2 * core, jnp.where(upper | level_mask, value, flipped).astype(BF16))
                    low = jnp.where(level_mask, jnp.broadcast_to(line, (block, block)), jnp.where(upper, flipped, value))
                    put(2 * core + 1, 2 * core + 1, low.astype(BF16))
                else:
                    r, k = ((2 * core, 1), (2 * core, 2 + core), (2 * core + 1, 3 * (1 - core)))[n - 1]
                    value = value.astype(BF16)
                    put(r, k, value)
                    put(k, r, value.T)

        for hop in range(width):
            other = lax.rem(x + hop, width)
            for core in range(2):
                arrival = remote(
                    staged.at[0, 0], pool.at[other, i, core], stage_send.at[0, 0], pool_recv.at[other, i, core],
                    {"walk": other, "orb": core},
                )
                if hop > 0:
                    arrival.wait_recv()
                else:
                    @pl.when(core != o)
                    def _():
                        arrival.wait_recv()
        column = copies[x, w] // local
        for core in range(2):
            start = pool[0, i, core]
            for other in hops:
                start = jnp.where(column == other, pool[other, i, core], start)
            term[core * rows:(core + 1) * rows, :] = start
        running = term[...].astype(F32)
        for degree in range(1, ORDER + 1):
            fresh = (jnp.dot(full[...], term[...], preferred_element_type=F32) * (1.0 / degree)).astype(BF16)
            running = running + fresh.astype(F32)
            if degree < ORDER:
                term[...] = fresh
        result[i] = running.astype(BF16).reshape(2, rows, electrons)
        for copy in spread_copies(a):
            copy.start()
        gathered[w] = result[i, o]
        write_copy(w).start()

    for a in range(half):
        @pl.when(at_owner[a] & (a % 2 == o))
        def _():
            finish(a)

    new_log = picked[2][:, 0:lanes] + factor + extra_in[0, 0:local, :] + extra_in[1, 0:local, :]
    for s in range(local):
        out_log[s] = jnp.max(new_log[s:s + 1, :])

    def onward(w, part, hop_to):
        spot = place(w, part)
        return remote(spot, spot, next_send.at[w, part], slot_recv.at[w, part], {"vec": hop_to})

    def route(side, a):
        w = side * half + a
        away = jnp.where(side == 0, z, last - z) - insets[a]
        hop_to = jnp.where(side == 0, z + 1, z - 1)
        return w, away, hop_to

    for a in range(half):
        for side in (near, 1 - near):
            w, away, hop_to = route(side, a)

            @pl.when((away != 0) | (o != a % 2))
            def _():
                for part in range(PARTS):
                    onward(w, part, hop_to).wait_recv()

                    @pl.when(passes(a, away))
                    def _():
                        onward(w, part, hop_to).start()
                write_copy(w).start()

    for w in range(local):
        write_copy(w).wait()

    for copy in bias_copies:
        copy.wait_send()
    for hop in hops:
        facts_copy(hop, x).wait_send()
        copies_copy(hop, x).wait_send()

    def drain(c, carry):
        for side in range(2):
            @pl.when(downstream[side] - depth_of(c) > 0)
            def _():
                chain_copy(side, c).wait_send()

        return carry

    lax.fori_loop(0, chunks, drain, jnp.int32(0))
    for side in range(2):
        @pl.when(downstream[side] > 0)
        def _():
            extra_copy(side).wait_send()

    @pl.when(owning)
    def _():
        swap_core().wait_send()

    for a in range(half):
        @pl.when(at_owner[a])
        def _():
            for hop in hops:
                stage_copy(hop, a).wait_send()

            @pl.when(a % 2 != o)
            def _():
                stage_copy(0, a).wait_send()

                def taken_back(c, carry):
                    swap_copy(c).wait_send()
                    return carry

                lax.fori_loop(a * each, (a + 1) * each, taken_back, jnp.int32(0))

            @pl.when(a % 2 == o)
            def _():
                for copy in spread_copies(a):
                    copy.wait_send()

        if insets[a]:
            @pl.when(at_end)
            def _():
                def back_done(c, carry):
                    back_copy(c).wait_send()
                    return carry

                lax.fori_loop(a * each, (a + 1) * each, back_done, jnp.int32(0))

    for a in range(half):
        for side in range(2):
            w, away, hop_to = route(side, a)

            @pl.when(passes(a, away))
            def _():
                for part in range(PARTS):
                    onward(w, part, hop_to).wait_send()


def per_device(depth, width, walkers, inv_intersection, trial, vectors, aux_field, log_weight, copy_list):
    local, rows, electrons = walkers.shape
    count, _, orbitals = vectors.shape
    half = local // 2
    block = orbitals // 4
    span = 2 * block // count
    wide = count * span
    piece = block // SUB
    chunks = half * BLOCKS * SUB
    mine = half // 2
    lanes = 128
    reach = max(max(depth - 1, 1) if depth - 1 <= REACH else 1, 2)
    dma = pltpu.SemaphoreType.DMA
    anywhere = pl.BlockSpec(memory_space=pl.ANY)
    out, out_log = pl.pallas_call(
        functools.partial(kernel, depth, width),
        out_shape=(
            jax.ShapeDtypeStruct(walkers.shape, BF16),
            jax.ShapeDtypeStruct((local,), F32),
        ),
        in_specs=[anywhere] * 7,
        out_specs=(anywhere, pl.BlockSpec(memory_space=pltpu.SMEM)),
        scratch_shapes=[
            pltpu.VMEM(walkers.shape, BF16),
            pltpu.VMEM(inv_intersection.shape, BF16),
            pltpu.VMEM(trial.shape, BF16),
            pltpu.VMEM(vectors.shape, BF16),
            pltpu.VMEM(aux_field.shape, F32),
            pltpu.SMEM((local,), F32),
            pltpu.SMEM((width, local), jnp.int32),
            pltpu.VMEM((local, rows, electrons), BF16),
            pltpu.VMEM((count, rows, electrons), BF16),
            pltpu.VMEM((block // span, wide, BLOCKS * block), BF16),
            pltpu.VMEM((wide, block), BF16),
            pltpu.VMEM((2, width, local, wide), F32),
            pltpu.VMEM((width, 2 * local, wide), F32),
            pltpu.VMEM((3, local, wide), F32),
            pltpu.VMEM((local, BLOCKS, block, block), F32),
            pltpu.VMEM((2, chunks, piece, block), BF16),
            pltpu.VMEM((2, chunks, piece, block), BF16),
            pltpu.VMEM((chunks, piece, block), BF16),
            pltpu.VMEM((chunks, piece, block), BF16),
            pltpu.VMEM((2, chunks, piece, block), BF16),
            pltpu.VMEM((2, 2 * local, lanes), F32),
            pltpu.VMEM((2, 2 * local, lanes), F32),
            pltpu.VMEM((2, local, lanes), F32),
            pltpu.VMEM((width, half, rows, electrons), BF16),
            pltpu.VMEM((width, mine, 2, rows, electrons), BF16),
            pltpu.VMEM((orbitals, orbitals), BF16),
            pltpu.VMEM((orbitals, electrons), BF16),
            pltpu.VMEM((mine, 2, rows, electrons), BF16),
            pltpu.VMEM((local, rows, electrons), BF16),
            dma((7,)),
            dma((width,)),
            dma((width,)),
            dma((width,)),
            dma((width,)),
            dma((2 * width,)),
            dma((2, width)),
            dma((2, chunks)),
            dma((2, chunks)),
            dma((chunks,)),
            dma((2, chunks)),
            dma((chunks,)),
            dma((chunks,)),
            dma((2,)),
            dma((2,)),
            dma((2,)),
            dma((width, half)),
            dma((width, mine, 2)),
            dma((mine, 2 * reach + 1, PARTS)),
            dma((local, PARTS)),
            dma((local, PARTS)),
            dma((local,)),
        ],
        compiler_params=pltpu.CompilerParams(collective_id=0, has_side_effects=True),
    )(walkers, inv_intersection, trial, vectors, aux_field, log_weight, copy_list)
    return out, out_log


def solution(mesh):
    depth, width = mesh.shape["vec"], mesh.shape["walk"]
    assert mesh.shape["orb"] == 2 and depth > 1
    return jax.shard_map(
        functools.partial(per_device, depth, width),
        mesh=mesh,
        in_specs=(
            P(("grp", "walk"), "orb", None),
            P(("grp", "walk"), None, None),
            P(),
            P("vec", "orb", None),
            P(("grp", "walk"), "vec"),
            P(("grp", "walk")),
            P(("grp", "walk")),
        ),
        out_specs=(P(("grp", "walk"), "orb", None), P(("grp", "walk"))),
        check_vma=False,
    )
```

```python
import functools
import math

import jax
import jax.numpy as jnp
from jax import lax
from jax.experimental import pallas as pl
from jax.experimental.pallas import tpu as pltpu
from jax.sharding import PartitionSpec as P

ORDER = 6
BLOCKS = 4
SUB = 1
SKEW = 5
PARTS = 2
REACH = 3
PLANS = ((2, -1, 1), (3, 2, 1), (2, 1), (2, 1))
MESH = pl.DeviceIdType.MESH
F32 = jnp.float32
BF16 = jnp.bfloat16

step_root = math.sqrt(0.08)


def remote(src, dst, send, recv, where):
    return pltpu.make_async_remote_copy(
        src_ref=src, dst_ref=dst, send_sem=send, recv_sem=recv, device_id=where, device_id_type=MESH
    )


def kernel(
    depth, width,
    walkers_in, inverse_in, trial_in, vectors_in, aux_in, log_in, copies_in,
    out, out_log,
    walkers, inverse, trial, vectors, aux, log_weight, copies,
    green, mixed, strips, level, bias_all, facts, picked, partial, leaving, arrived, given, crossed,
    back, extra_in, extra_out, edge, staged, pool, full, term, result,
    load_sems, copies_send, copies_recv, facts_send, facts_recv, bias_send, bias_recv,
    chain_send, chain_recv, cross_recv, back_recv, swap_send, swap_recv, extra_send, extra_recv, edge_sems,
    stage_send, pool_recv, own_send, next_send, slot_recv,
):
    gathered = out
    z = lax.axis_index("vec")
    x = lax.axis_index("walk")
    o = lax.axis_index("orb")
    last = depth - 1
    local, rows, electrons = walkers.shape
    count, _, orbitals = vectors.shape
    half = local // 2
    block = orbitals // 4
    span = 2 * block // count
    wide = count * span
    piece = block // SUB
    each = BLOCKS * SUB
    chunks = half * each
    mine = half // 2
    lanes = extra_in.shape[2]
    insets = [1 if a == half - 1 and last >= REACH else 0 for a in range(half)]
    hops = range(1, width)

    barrier = pltpu.get_barrier_semaphore()

    def greet(where):
        pl.semaphore_signal(barrier, inc=1, device_id=where, device_id_type=MESH)

    greet({"orb": 1 - o})
    for hop in hops:
        for core in range(2):
            greet({"walk": lax.rem(x + hop, width), "orb": core})

    @pl.when(z > 0)
    def _():
        for core in range(2):
            greet({"vec": z - 1, "orb": core})

    @pl.when(z < last)
    def _():
        for core in range(2):
            greet({"vec": z + 1, "orb": core})

    pairs = (
        (copies_in, copies.at[x]), (log_in, log_weight), (walkers_in, walkers), (inverse_in, inverse), (trial_in, trial),
        (vectors_in, vectors), (aux_in, aux),
    )
    loads = [pltpu.make_async_copy(src, dst, load_sems.at[n]) for n, (src, dst) in enumerate(pairs)]
    for load in loads:
        load.start()

    loads[2].wait()
    loads[3].wait()
    for w in range(local):
        green[w] = jnp.dot(walkers[w], inverse[w], preferred_element_type=F32).astype(BF16)
    loads[4].wait()
    loads[5].wait()
    for g in range(count):
        mixed[g] = jnp.dot(vectors[g], trial[...], preferred_element_type=F32).astype(BF16)
    gram = jnp.zeros((local * span, wide), F32)
    for j in range(rows // span):
        left = green[:, j * span:(j + 1) * span, :].reshape(local * span, electrons)
        right = mixed[:, j * span:(j + 1) * span, :].reshape(wide, electrons)
        gram = gram + lax.dot_general(left, right, (((1,), (1,)), ((), ())), preferred_element_type=F32)
    row_id = lax.broadcasted_iota(jnp.int32, (local * span, wide), 0)
    col_id = lax.broadcasted_iota(jnp.int32, (local * span, wide), 1)
    same = row_id % span == col_id % span
    folded = jnp.sum(jnp.where(same, gram, 0.0).reshape(local, span, wide), axis=1)
    wide_row = lax.broadcasted_iota(jnp.int32, (wide, wide), 0)
    wide_col = lax.broadcasted_iota(jnp.int32, (wide, wide), 1)
    groups = jnp.where(wide_row // span == wide_col // span, 1.0, 0.0).astype(F32)
    bias_all[o, x] = jnp.dot(folded, groups, precision=lax.Precision.HIGHEST, preferred_element_type=F32)

    loads[6].wait()
    loads[0].wait()
    loads[1].wait()
    pick_row = lax.broadcasted_iota(jnp.int32, (count, wide), 0)
    pick_col = lax.broadcasted_iota(jnp.int32, (count, wide), 1)
    pick = jnp.where(pick_row == pick_col // span, 1.0, 0.0).astype(F32)
    facts[x, 0:local, :] = jnp.dot(aux[...], pick, precision=lax.Precision.HIGHEST, preferred_element_type=F32)
    walker_id = lax.broadcasted_iota(jnp.int32, (local, wide), 0)
    weights = jnp.zeros((local, wide), F32)
    for w in range(local):
        weights = jnp.where(walker_id == w, log_weight[w], weights)
    facts[x, local:2 * local, :] = weights

    sides = jnp.where(z > 0, 2, 0) + jnp.where(z < last, 2, 0)
    pl.semaphore_wait(barrier, 1 + 2 * (width - 1) + sides)

    bias_peers = [{"walk": lax.rem(x + hop, width), "orb": core} for hop in hops for core in range(2)] + [{"orb": 1 - o}]
    bias_copies = [
        remote(bias_all.at[o, x], bias_all.at[o, x], bias_send.at[n], bias_recv.at[o, x], where)
        for n, where in enumerate(bias_peers)
    ]
    for copy in bias_copies:
        copy.start()

    def facts_copy(hop, owner):
        return remote(
            facts.at[owner], facts.at[owner], facts_send.at[hop], facts_recv.at[owner], {"walk": lax.rem(x + hop, width)}
        )

    def copies_copy(hop, owner):
        return remote(
            copies.at[owner], copies.at[owner], copies_send.at[hop], copies_recv.at[owner],
            {"walk": lax.rem(x + hop, width)},
        )

    for hop in hops:
        copies_copy(hop, x).start()
        facts_copy(hop, x).start()

    chunk_row = lax.broadcasted_iota(jnp.int32, (count, span, block), 1)
    chunk_col = lax.broadcasted_iota(jnp.int32, (count, span, block), 2)
    crossing = jnp.zeros((count, span, block), F32)

    def columns(n):
        return pl.ds(pl.multiple_of(n * block, block), block)

    for j in range(block // span):
        here = slice(j * span, (j + 1) * span)
        below = slice(block + j * span, block + (j + 1) * span)
        first = vectors[:, here, columns(2 * o)].astype(F32)
        second = vectors[:, below, columns(1 + 2 * o)].astype(F32)
        crossing = crossing + jnp.where(chunk_row + j * span == chunk_col, second, 0.0)
        joined = jnp.where(chunk_row + j * span <= chunk_col, first, second).astype(BF16)
        strips[j, :, 0:block] = joined.reshape(wide, block)
        strips[j, :, block:2 * block] = vectors[:, here, block:2 * block].reshape(wide, block)
        strips[j, :, 2 * block:3 * block] = vectors[:, here, columns(2 + o)].reshape(wide, block)
        strips[j, :, 3 * block:] = vectors[:, below, columns(3 * (1 - o))].reshape(wide, block)
    level[...] = crossing.reshape(wide, block).astype(BF16)

    for hop in hops:
        other = lax.rem(x + hop, width)
        facts_copy(hop, other).wait_recv()
        for core in range(2):
            remote(
                bias_all.at[core, other], bias_all.at[core, other], bias_send.at[0], bias_recv.at[core, other], {"walk": other}
            ).wait_recv()
    remote(bias_all.at[1 - o, x], bias_all.at[1 - o, x], bias_send.at[0], bias_recv.at[1 - o, x], {"orb": 1 - o}).wait_recv()

    for s in range(local):
        source = copies[x, s]
        column = source // local
        at = source % local
        row = pl.ds(at, 1)
        picked[0, s:s + 1, :] = bias_all[0, column, row, :] + bias_all[1, column, row, :]
        picked[1, s:s + 1, :] = facts[column, row, :]
        picked[2, s:s + 1, :] = facts[column, pl.ds(local + at, 1), :]

    bias = picked[0]
    drawn = picked[1]
    shift = -step_root * bias
    field = drawn - shift
    factor = jnp.sum(drawn * shift - 0.5 * shift * shift, axis=1, keepdims=True) * (1.0 / span)
    factor = jnp.broadcast_to(factor, (local, lanes))
    weighted = (field * step_root).astype(BF16)
    spread = jnp.broadcast_to(weighted.astype(F32)[:, None, :], (local, span, wide)).reshape(local * span, wide)
    kron = jnp.where(same, spread, 0.0).astype(BF16)

    for j in range(block // span):
        summed = jnp.dot(kron, strips[j], preferred_element_type=F32)
        for n in range(BLOCKS):
            partial[:, n, j * span:(j + 1) * span, :] = summed[:, n * block:(n + 1) * block].reshape(local, span, block)
    edge_part = jnp.dot(weighted, level[...], preferred_element_type=F32)

    to_next = [z - 1, z + 1]
    upstream = [last - z, z]
    downstream = [z, last - z]
    at_end = (z == 0) | (z == last)
    near = jnp.where(z <= last - z, 0, 1)
    base = near * half
    inward = jnp.where(near == 0, z + 1, z - 1)
    at_owner = [(z == n) | (z == last - n) for n in insets]

    def depth_of(c):
        return sum(jnp.where(c // each == a, n, 0) for a, n in enumerate(insets) if n) + jnp.int32(0)

    def chain_copy(side, c):
        return remote(
            leaving.at[side, c], arrived.at[side, c], chain_send.at[side, c], chain_recv.at[side, c],
            {"vec": to_next[side]},
        )

    def cross_copy(side, c):
        return remote(
            leaving.at[side, c], crossed.at[c], chain_send.at[side, c], cross_recv.at[c],
            {"vec": to_next[side], "orb": 1 - o},
        )

    def swap_copy(c):
        return remote(leaving.at[near, c], given.at[c], swap_send.at[c], swap_recv.at[c], {"orb": 1 - o})

    def extra_copy(side):
        return remote(
            extra_out.at[side], extra_in.at[side], extra_send.at[side], extra_recv.at[side], {"vec": to_next[side]}
        )

    def back_copy(c):
        return remote(
            leaving.at[near, c], back.at[o, c], chain_send.at[near, c], back_recv.at[o, c],
            {"vec": inward, "orb": (c // each) % 2},
        )

    def part_of(side, c):
        at = c % each
        return partial[side * half + c // each, at // SUB, pl.ds(pl.multiple_of((at % SUB) * piece, piece), piece), :]

    def chain_step(t, carry):
        for side in range(2):
            c = t - SKEW * upstream[side]
            head = upstream[side] == 0
            togo = downstream[side] - depth_of(c)

            @pl.when((c >= 0) & (c < chunks) & (togo > 0))
            def _():
                own = part_of(side, c)
                here = (c // each) % 2 == o

                @pl.when(head)
                def _():
                    leaving[side, c] = own.astype(BF16)

                @pl.when(jnp.logical_not(head))
                def _():
                    chain_copy(side, c).wait_recv()
                    leaving[side, c] = (own + arrived[side, c].astype(F32)).astype(BF16)

                @pl.when((togo > 1) | here)
                def _():
                    chain_copy(side, c).start()

                @pl.when((togo == 1) & jnp.logical_not(here))
                def _():
                    cross_copy(side, c).start()

                @pl.when(c == 0)
                def _():
                    @pl.when(head)
                    def _():
                        extra_in[side] = jnp.zeros_like(extra_in[side])

                    @pl.when(jnp.logical_not(head))
                    def _():
                        extra_copy(side).wait_recv()

                    extra_out[side, 0:local, :] = extra_in[side, 0:local, :] + factor
                    extra_out[side, local:, :] = extra_in[side, local:, :] + edge_part
                    extra_copy(side).start()

        return carry

    lax.fori_loop(0, SKEW * (last - 1) + chunks, chain_step, jnp.int32(0))

    for hop in hops:
        copies_copy(hop, lax.rem(x + hop, width)).wait_recv()

    def stage_copy(hop, a):
        return remote(
            staged.at[hop, a], pool.at[x, a // 2, o], stage_send.at[hop, a], pool_recv.at[x, a // 2, o],
            {"walk": lax.rem(x + hop, width), "orb": a % 2},
        )

    def swap_core():
        return remote(edge.at[o], edge.at[o], edge_sems.at[0], edge_sems.at[1], {"orb": 1 - o})

    for a in range(half):
        @pl.when(at_owner[a])
        def _():
            for hop in range(width):
                source = copies[lax.rem(x + hop, width), base + a]
                held = walkers[source % local]
                if hop > 0:
                    staged[hop, a] = held
                    stage_copy(hop, a).start()
                else:
                    @pl.when(a % 2 == o)
                    def _():
                        pool[x, a // 2, o] = held

                    @pl.when(a % 2 != o)
                    def _():
                        staged[hop, a] = held
                        stage_copy(hop, a).start()

            @pl.when(a % 2 != o)
            def _():
                def give(c, carry):
                    leaving[near, c] = part_of(near, c).astype(BF16)
                    swap_copy(c).start()
                    return carry

                lax.fori_loop(a * each, (a + 1) * each, give, jnp.int32(0))

        if insets[a]:
            @pl.when(at_end)
            def _():
                def back_step(c, carry):
                    leaving[near, c] = part_of(near, c).astype(BF16)
                    back_copy(c).start()
                    return carry

                lax.fori_loop(a * each, (a + 1) * each, back_step, jnp.int32(0))

    for side in range(2):
        @pl.when(at_end & (near == side))
        def _():
            extra_copy(side).wait_recv()

    owning = functools.reduce(jnp.logical_or, at_owner)

    @pl.when(owning)
    def _():
        edge[o] = edge_part + extra_in[0, local:, :] + extra_in[1, local:, :]
        swap_core().start()
        swap_core().wait_recv()

    share = rows // PARTS
    short = last <= REACH
    plans = [
        tuple(n for n in PLANS[min(half - a, len(PLANS)) - 1] if -insets[a] <= n <= last - insets[a])
        if short else (1,) + (-1,) * insets[a] for a in range(half)
    ]

    def passes(a, away):
        if not short:
            return (away > 0) & (away < last - insets[a])
        gaps = [away == n for n in range(1, last - insets[a]) if n + 1 not in plans[a]]
        return functools.reduce(jnp.logical_or, gaps, jnp.bool_(False))

    def place(w, part):
        return gathered.at[w, pl.ds(part * share, share)]

    def away_z(n):
        return jnp.where(near == 0, z + n, z - n)

    def spread_copies(a):
        w = base + a
        targets = []
        for n in plans[a]:
            for core in (1 - a % 2, a % 2):
                targets.append((core, {"vec": away_z(n), "orb": core}))
        targets.append((1 - a % 2, {"orb": 1 - o}))
        return [
            remote(
                result.at[a // 2, core, pl.ds(part * share, share)], place(w, part),
                own_send.at[a // 2, n, part], slot_recv.at[w, part], where,
            )
            for n, (core, where) in enumerate(targets)
            for part in range(PARTS)
        ]

    upper = lax.broadcasted_iota(jnp.int32, (block, block), 0) < lax.broadcasted_iota(jnp.int32, (block, block), 1)
    level_mask = lax.broadcasted_iota(jnp.int32, (block, block), 0) == lax.broadcasted_iota(jnp.int32, (block, block), 1)

    def finish(a):
        w = base + a
        i = a // 2

        def put(r, c, value):
            full[columns(r), columns(c)] = value

        for n in range(BLOCKS):
            first_c = a * each + n * SUB
            for c in range(first_c, first_c + SUB):
                remote(
                    leaving.at[near, c], arrived.at[near, c], chain_send.at[near, c], chain_recv.at[near, c], {"vec": inward}
                ).wait_recv()
                swap_copy(c).wait_recv()
                remote(
                    leaving.at[near, c], crossed.at[c], chain_send.at[near, c], cross_recv.at[c],
                    {"vec": inward, "orb": 1 - o},
                ).wait_recv()
                if insets[a]:
                    for core in range(2):
                        remote(
                            leaving.at[near, c], back.at[core, c], chain_send.at[near, c], back_recv.at[core, c],
                            {"vec": away_z(-1), "orb": core},
                        ).wait_recv()
            run = pl.ds(first_c, SUB)
            kept = partial[w, n] + arrived[near, run].reshape(block, block).astype(F32)
            taken = given[run].reshape(block, block).astype(F32) + crossed[run].reshape(block, block).astype(F32)
            if insets[a]:
                kept = kept + back[o, run].reshape(block, block).astype(F32)
                taken = taken + back[1 - o, run].reshape(block, block).astype(F32)
            for core, value in ((o, kept), (1 - o, taken)):
                if n == 0:
                    flipped = value.T
                    line = edge[core, pl.ds(w, 1), :]
                    put(2 * core, 2 * core, jnp.where(upper | level_mask, value, flipped).astype(BF16))
                    low = jnp.where(level_mask, jnp.broadcast_to(line, (block, block)), jnp.where(upper, flipped, value))
                    put(2 * core + 1, 2 * core + 1, low.astype(BF16))
                else:
                    r, k = ((2 * core, 1), (2 * core, 2 + core), (2 * core + 1, 3 * (1 - core)))[n - 1]
                    value = value.astype(BF16)
                    put(r, k, value)
                    put(k, r, value.T)

        for hop in range(width):
            other = lax.rem(x + hop, width)
            for core in range(2):
                arrival = remote(
                    staged.at[0, 0], pool.at[other, i, core], stage_send.at[0, 0], pool_recv.at[other, i, core],
                    {"walk": other, "orb": core},
                )
                if hop > 0:
                    arrival.wait_recv()
                else:
                    @pl.when(core != o)
                    def _():
                        arrival.wait_recv()
        column = copies[x, w] // local
        for core in range(2):
            start = pool[0, i, core]
            for other in hops:
                start = jnp.where(column == other, pool[other, i, core], start)
            term[core * rows:(core + 1) * rows, :] = start
        running = term[...].astype(F32)
        for degree in range(1, ORDER + 1):
            fresh = (jnp.dot(full[...], term[...], preferred_element_type=F32) * (1.0 / degree)).astype(BF16)
            running = running + fresh.astype(F32)
            if degree < ORDER:
                term[...] = fresh
        result[i] = running.astype(BF16).reshape(2, rows, electrons)
        for copy in spread_copies(a):
            copy.start()
        gathered[w] = result[i, o]

    for a in range(half):
        @pl.when(at_owner[a] & (a % 2 == o))
        def _():
            finish(a)

    new_log = picked[2][:, 0:lanes] + factor + extra_in[0, 0:local, :] + extra_in[1, 0:local, :]
    out_log[...] = new_log

    def onward(w, part, hop_to):
        spot = place(w, part)
        return remote(spot, spot, next_send.at[w, part], slot_recv.at[w, part], {"vec": hop_to})

    def route(side, a):
        w = side * half + a
        away = jnp.where(side == 0, z, last - z) - insets[a]
        hop_to = jnp.where(side == 0, z + 1, z - 1)
        return w, away, hop_to

    for a in range(half):
        for side in (near, 1 - near):
            w, away, hop_to = route(side, a)

            @pl.when((away != 0) | (o != a % 2))
            def _():
                for part in range(PARTS):
                    onward(w, part, hop_to).wait_recv()

                    @pl.when(passes(a, away))
                    def _():
                        onward(w, part, hop_to).start()


    for copy in bias_copies:
        copy.wait_send()
    for hop in hops:
        facts_copy(hop, x).wait_send()
        copies_copy(hop, x).wait_send()

    def drain(c, carry):
        for side in range(2):
            @pl.when(downstream[side] - depth_of(c) > 0)
            def _():
                chain_copy(side, c).wait_send()

        return carry

    lax.fori_loop(0, chunks, drain, jnp.int32(0))
    for side in range(2):
        @pl.when(downstream[side] > 0)
        def _():
            extra_copy(side).wait_send()

    @pl.when(owning)
    def _():
        swap_core().wait_send()

    for a in range(half):
        @pl.when(at_owner[a])
        def _():
            for hop in hops:
                stage_copy(hop, a).wait_send()

            @pl.when(a % 2 != o)
            def _():
                stage_copy(0, a).wait_send()

                def taken_back(c, carry):
                    swap_copy(c).wait_send()
                    return carry

                lax.fori_loop(a * each, (a + 1) * each, taken_back, jnp.int32(0))

            @pl.when(a % 2 == o)
            def _():
                for copy in spread_copies(a):
                    copy.wait_send()

        if insets[a]:
            @pl.when(at_end)
            def _():
                def back_done(c, carry):
                    back_copy(c).wait_send()
                    return carry

                lax.fori_loop(a * each, (a + 1) * each, back_done, jnp.int32(0))

    for a in range(half):
        for side in range(2):
            w, away, hop_to = route(side, a)

            @pl.when(passes(a, away))
            def _():
                for part in range(PARTS):
                    onward(w, part, hop_to).wait_send()


def per_device(depth, width, walkers, inv_intersection, trial, vectors, aux_field, log_weight, copy_list):
    local, rows, electrons = walkers.shape
    count, _, orbitals = vectors.shape
    half = local // 2
    block = orbitals // 4
    span = 2 * block // count
    wide = count * span
    piece = block // SUB
    chunks = half * BLOCKS * SUB
    mine = half // 2
    lanes = 128
    reach = max(max(depth - 1, 1) if depth - 1 <= REACH else 1, 2)
    dma = pltpu.SemaphoreType.DMA
    anywhere = pl.BlockSpec(memory_space=pl.ANY)
    out, out_log = pl.pallas_call(
        functools.partial(kernel, depth, width),
        out_shape=(
            pltpu.VMEM(walkers.shape, BF16),
            pltpu.VMEM((local, 128), F32),
        ),
        in_specs=[anywhere] * 7,
        out_specs=(pl.BlockSpec(memory_space=pltpu.VMEM), pl.BlockSpec(memory_space=pltpu.VMEM)),
        scratch_shapes=[
            pltpu.VMEM(walkers.shape, BF16),
            pltpu.VMEM(inv_intersection.shape, BF16),
            pltpu.VMEM(trial.shape, BF16),
            pltpu.VMEM(vectors.shape, BF16),
            pltpu.VMEM(aux_field.shape, F32),
            pltpu.SMEM((local,), F32),
            pltpu.SMEM((width, local), jnp.int32),
            pltpu.VMEM((local, rows, electrons), BF16),
            pltpu.VMEM((count, rows, electrons), BF16),
            pltpu.VMEM((block // span, wide, BLOCKS * block), BF16),
            pltpu.VMEM((wide, block), BF16),
            pltpu.VMEM((2, width, local, wide), F32),
            pltpu.VMEM((width, 2 * local, wide), F32),
            pltpu.VMEM((3, local, wide), F32),
            pltpu.VMEM((local, BLOCKS, block, block), F32),
            pltpu.VMEM((2, chunks, piece, block), BF16),
            pltpu.VMEM((2, chunks, piece, block), BF16),
            pltpu.VMEM((chunks, piece, block), BF16),
            pltpu.VMEM((chunks, piece, block), BF16),
            pltpu.VMEM((2, chunks, piece, block), BF16),
            pltpu.VMEM((2, 2 * local, lanes), F32),
            pltpu.VMEM((2, 2 * local, lanes), F32),
            pltpu.VMEM((2, local, lanes), F32),
            pltpu.VMEM((width, half, rows, electrons), BF16),
            pltpu.VMEM((width, mine, 2, rows, electrons), BF16),
            pltpu.VMEM((orbitals, orbitals), BF16),
            pltpu.VMEM((orbitals, electrons), BF16),
            pltpu.VMEM((mine, 2, rows, electrons), BF16),
            dma((7,)),
            dma((width,)),
            dma((width,)),
            dma((width,)),
            dma((width,)),
            dma((2 * width,)),
            dma((2, width)),
            dma((2, chunks)),
            dma((2, chunks)),
            dma((chunks,)),
            dma((2, chunks)),
            dma((chunks,)),
            dma((chunks,)),
            dma((2,)),
            dma((2,)),
            dma((2,)),
            dma((width, half)),
            dma((width, mine, 2)),
            dma((mine, 2 * reach + 1, PARTS)),
            dma((local, PARTS)),
            dma((local, PARTS)),
        ],
        compiler_params=pltpu.CompilerParams(collective_id=0, has_side_effects=True),
    )(walkers, inv_intersection, trial, vectors, aux_field, log_weight, copy_list)

    def settle(out_ref, log_ref, o1, o2, flat, sems):
        c1 = pltpu.make_async_copy(out_ref, o1, sems.at[0])
        c1.start()
        for s in range(local):
            flat[s] = jnp.max(log_ref[s:s + 1, :])
        c2 = pltpu.make_async_copy(flat, o2, sems.at[1])
        c2.start()
        c1.wait()
        c2.wait()

    return pl.pallas_call(
        settle,
        out_shape=(jax.ShapeDtypeStruct(walkers.shape, BF16), jax.ShapeDtypeStruct((local,), F32)),
        in_specs=[pl.BlockSpec(memory_space=pltpu.VMEM)] * 2,
        out_specs=(anywhere, anywhere),
        scratch_shapes=[pltpu.SMEM((local,), F32), dma((2,))],
    )(pltpu.with_memory_space_constraint(out, pltpu.VMEM), pltpu.with_memory_space_constraint(out_log, pltpu.VMEM))


def solution(mesh):
    depth, width = mesh.shape["vec"], mesh.shape["walk"]
    assert mesh.shape["orb"] == 2 and depth > 1
    return jax.shard_map(
        functools.partial(per_device, depth, width),
        mesh=mesh,
        in_specs=(
            P(("grp", "walk"), "orb", None),
            P(("grp", "walk"), None, None),
            P(),
            P("vec", "orb", None),
            P(("grp", "walk"), "vec"),
            P(("grp", "walk")),
            P(("grp", "walk")),
        ),
        out_specs=(P(("grp", "walk"), "orb", None), P(("grp", "walk"))),
        check_vma=False,
    )
```

```python
import functools
import math

import jax
import jax.numpy as jnp
from jax import lax
from jax.experimental import pallas as pl
from jax.experimental.pallas import tpu as pltpu
from jax.sharding import PartitionSpec as P

ORDER = 6
BLOCKS = 4
SUB = 1
SKEW = 4
PARTS = 1
LOADS = 4
REACH = 3
PLANS = ((2, -1, 1), (3, 2, 1), (3, 2, 1), (2, 1))
MESH = pl.DeviceIdType.MESH
F32 = jnp.float32
BF16 = jnp.bfloat16

step_root = math.sqrt(0.08)


def remote(src, dst, send, recv, where):
    return pltpu.make_async_remote_copy(
        src_ref=src, dst_ref=dst, send_sem=send, recv_sem=recv, device_id=where, device_id_type=MESH
    )


def kernel(
    depth, width,
    walkers_in, inverse_in, trial_in, vectors_in, aux_in, log_in, copies_in,
    out, out_log,
    walkers, inverse, trial, vectors, aux, log_weight, copies,
    green, mixed, strips, level, bias_all, facts, known, picked, partial, leaving, arrived, given, crossed,
    back, extra_in, extra_out, edge, staged, pool, full, term, result,
    load_sems, copies_send, copies_recv, facts_send, facts_recv, bias_send, bias_recv,
    chain_send, chain_recv, cross_recv, back_recv, swap_send, swap_recv, extra_send, extra_recv, edge_sems,
    stage_send, pool_recv, own_send, next_send, slot_recv,
):
    gathered = out
    z = lax.axis_index("vec")
    x = lax.axis_index("walk")
    o = lax.axis_index("orb")
    last = depth - 1
    local, rows, electrons = walkers.shape
    count, _, orbitals = vectors.shape
    half = local // 2
    block = orbitals // 4
    span = 2 * block // count
    wide = count * span
    piece = block // SUB
    each = BLOCKS * SUB
    chunks = half * each
    mine = half // 2
    lanes = extra_in.shape[2]
    insets = [1 if a == half - 1 and last >= REACH else 0 for a in range(half)]
    hops = range(1, width)

    barrier = pltpu.get_barrier_semaphore()

    def greet(where):
        pl.semaphore_signal(barrier, inc=1, device_id=where, device_id_type=MESH)

    greet({"orb": 1 - o})
    for hop in hops:
        for core in range(2):
            greet({"walk": lax.rem(x + hop, width), "orb": core})

    @pl.when(z > 0)
    def _():
        for core in range(2):
            greet({"vec": z - 1, "orb": core})

    @pl.when(z < last)
    def _():
        for core in range(2):
            greet({"vec": z + 1, "orb": core})

    batch = count // LOADS
    pairs = [
        (inverse_in, inverse), (walkers_in, walkers), (trial_in, trial), (copies_in, copies.at[x]), (log_in, log_weight),
        (aux_in, aux),
    ]
    for n in range(LOADS):
        group = pl.ds(n * batch, batch)
        pairs.append((vectors_in.at[group], vectors.at[group]))
    loads = [pltpu.make_async_copy(src, dst, load_sems.at[n]) for n, (src, dst) in enumerate(pairs)]
    for load in loads:
        load.start()

    loads[0].wait()
    loads[1].wait()
    for w in range(local):
        green[w] = jnp.dot(walkers[w], inverse[w], preferred_element_type=F32).astype(BF16)
    for n in range(2, 6):
        loads[n].wait()
    walker_id = lax.broadcasted_iota(jnp.int32, (local, lanes), 0)
    weights = jnp.zeros((local, lanes), F32)
    for w in range(local):
        weights = jnp.where(walker_id == w, log_weight[w], weights)
    facts[x] = weights
    facts[x, :, 0:count] = aux[...]
    for n in range(LOADS):
        loads[6 + n].wait()
        for g in range(n * batch, (n + 1) * batch):
            mixed[g] = jnp.dot(vectors[g], trial[...], preferred_element_type=F32).astype(BF16)
    gram = jnp.zeros((local * span, wide), F32)
    for j in range(rows // span):
        left = green[:, j * span:(j + 1) * span, :].reshape(local * span, electrons)
        right = mixed[:, j * span:(j + 1) * span, :].reshape(wide, electrons)
        gram = gram + lax.dot_general(left, right, (((1,), (1,)), ((), ())), preferred_element_type=F32)
    row_id = lax.broadcasted_iota(jnp.int32, (local * span, wide), 0)
    col_id = lax.broadcasted_iota(jnp.int32, (local * span, wide), 1)
    same = row_id % span == col_id % span
    folded = jnp.sum(jnp.where(same, gram, 0.0).reshape(local, span, wide), axis=1)
    lane_id = lax.broadcasted_iota(jnp.int32, (local, wide), 1)
    reach = 1
    while reach < span:
        low = lane_id % (2 * reach) < reach
        folded = folded + jnp.where(low, pltpu.roll(folded, wide - reach, 1), pltpu.roll(folded, reach, 1))
        reach *= 2
    bias_all[o, x] = folded

    sides = jnp.where(z > 0, 2, 0) + jnp.where(z < last, 2, 0)
    pl.semaphore_wait(barrier, 1 + 2 * (width - 1) + sides)

    bias_peers = [{"walk": lax.rem(x + hop, width), "orb": core} for hop in hops for core in range(2)] + [{"orb": 1 - o}]
    bias_copies = [
        remote(bias_all.at[o, x], bias_all.at[o, x], bias_send.at[n], bias_recv.at[o, x], where)
        for n, where in enumerate(bias_peers)
    ]
    def facts_copy(hop, owner):
        return remote(
            facts.at[owner], facts.at[owner], facts_send.at[hop], facts_recv.at[owner], {"walk": lax.rem(x + hop, width)}
        )

    def copies_copy(hop, owner):
        return remote(
            copies.at[owner], copies.at[owner], copies_send.at[hop], copies_recv.at[owner],
            {"walk": lax.rem(x + hop, width)},
        )

    for copy in bias_copies:
        copy.start()
    for hop in hops:
        facts_copy(hop, x).start()
        copies_copy(hop, x).start()

    chunk_row = lax.broadcasted_iota(jnp.int32, (count, span, block), 1)
    chunk_col = lax.broadcasted_iota(jnp.int32, (count, span, block), 2)
    crossing = jnp.zeros((count, span, block), F32)

    def columns(n):
        return pl.ds(pl.multiple_of(n * block, block), block)

    for j in range(block // span):
        here = slice(j * span, (j + 1) * span)
        below = slice(block + j * span, block + (j + 1) * span)
        first = vectors[:, here, columns(2 * o)].astype(F32)
        second = vectors[:, below, columns(1 + 2 * o)].astype(F32)
        crossing = crossing + jnp.where(chunk_row + j * span == chunk_col, second, 0.0)
        joined = jnp.where(chunk_row + j * span <= chunk_col, first, second).astype(BF16)
        strips[j, :, 0:block] = joined.reshape(wide, block)
        strips[j, :, block:2 * block] = vectors[:, here, block:2 * block].reshape(wide, block)
        strips[j, :, 2 * block:3 * block] = vectors[:, here, columns(2 + o)].reshape(wide, block)
        strips[j, :, 3 * block:] = vectors[:, below, columns(3 * (1 - o))].reshape(wide, block)
    level[...] = crossing.reshape(wide, block).astype(BF16)

    for hop in hops:
        facts_copy(hop, lax.rem(x + hop, width)).wait_recv()
    sources = [(copies[x, s] // local, pl.ds(copies[x, s] % local, 1)) for s in range(local)]
    for s, (column, row) in enumerate(sources):
        known[s:s + 1, :] = facts[column, row, :]
    pick_row = lax.broadcasted_iota(jnp.int32, (count, wide), 0)
    pick_col = lax.broadcasted_iota(jnp.int32, (count, wide), 1)
    pick = jnp.where(pick_row == pick_col // span, 1.0, 0.0).astype(F32)
    drawn = jnp.dot(known[:, 0:count], pick, precision=lax.Precision.HIGHEST, preferred_element_type=F32)
    old_log = jnp.broadcast_to(known[:, count:count + 1], (local, lanes))

    for hop in hops:
        other = lax.rem(x + hop, width)
        for core in range(2):
            remote(
                bias_all.at[core, other], bias_all.at[core, other], bias_send.at[0], bias_recv.at[core, other], {"walk": other}
            ).wait_recv()
    remote(bias_all.at[1 - o, x], bias_all.at[1 - o, x], bias_send.at[0], bias_recv.at[1 - o, x], {"orb": 1 - o}).wait_recv()

    for s, (column, row) in enumerate(sources):
        picked[s:s + 1, :] = bias_all[0, column, row, :] + bias_all[1, column, row, :]
    bias = picked[...]
    shift = -step_root * bias
    field = drawn - shift
    factor = jnp.sum(drawn * shift - 0.5 * shift * shift, axis=1, keepdims=True) * (1.0 / span)
    factor = jnp.broadcast_to(factor, (local, lanes))
    weighted = (field * step_root).astype(BF16)
    spread = jnp.broadcast_to(weighted.astype(F32)[:, None, :], (local, span, wide)).reshape(local * span, wide)
    kron = jnp.where(same, spread, 0.0).astype(BF16)

    for j in range(block // span):
        summed = jnp.dot(kron, strips[j], preferred_element_type=F32)
        for n in range(BLOCKS):
            partial[:, n, j * span:(j + 1) * span, :] = summed[:, n * block:(n + 1) * block].reshape(local, span, block)
    edge_part = jnp.dot(weighted, level[...], preferred_element_type=F32)

    to_next = [z - 1, z + 1]
    upstream = [last - z, z]
    downstream = [z, last - z]
    at_end = (z == 0) | (z == last)
    near = jnp.where(z <= last - z, 0, 1)
    base = near * half
    inward = jnp.where(near == 0, z + 1, z - 1)
    at_owner = [(z == n) | (z == last - n) for n in insets]

    def depth_of(c):
        return sum(jnp.where(c // each == a, n, 0) for a, n in enumerate(insets) if n) + jnp.int32(0)

    def chain_copy(side, c):
        return remote(
            leaving.at[side, c], arrived.at[side, c], chain_send.at[side, c], chain_recv.at[side, c],
            {"vec": to_next[side]},
        )

    def cross_copy(side, c):
        return remote(
            leaving.at[side, c], crossed.at[c], chain_send.at[side, c], cross_recv.at[c],
            {"vec": to_next[side], "orb": 1 - o},
        )

    def swap_copy(c):
        return remote(leaving.at[near, c], given.at[c], swap_send.at[c], swap_recv.at[c], {"orb": 1 - o})

    def extra_copy(side):
        return remote(
            extra_out.at[side], extra_in.at[side], extra_send.at[side], extra_recv.at[side], {"vec": to_next[side]}
        )

    def back_copy(c):
        return remote(
            leaving.at[near, c], back.at[o, c], chain_send.at[near, c], back_recv.at[o, c],
            {"vec": inward, "orb": (c // each) % 2},
        )

    def part_of(side, c):
        at = c % each
        return partial[side * half + c // each, at // SUB, pl.ds(pl.multiple_of((at % SUB) * piece, piece), piece), :]

    def chain_step(t, carry):
        for side in range(2):
            c = t - SKEW * upstream[side]
            head = upstream[side] == 0
            togo = downstream[side] - depth_of(c)

            @pl.when((c >= 0) & (c < chunks) & (togo > 0))
            def _():
                own = part_of(side, c)
                here = (c // each) % 2 == o

                @pl.when(head)
                def _():
                    leaving[side, c] = own.astype(BF16)

                @pl.when(jnp.logical_not(head))
                def _():
                    chain_copy(side, c).wait_recv()
                    leaving[side, c] = (own + arrived[side, c].astype(F32)).astype(BF16)

                @pl.when((togo > 1) | here)
                def _():
                    chain_copy(side, c).start()

                @pl.when((togo == 1) & jnp.logical_not(here))
                def _():
                    cross_copy(side, c).start()

                @pl.when(c == 0)
                def _():
                    @pl.when(head)
                    def _():
                        extra_in[side] = jnp.zeros_like(extra_in[side])

                    @pl.when(jnp.logical_not(head))
                    def _():
                        extra_copy(side).wait_recv()

                    extra_out[side, 0:local, :] = extra_in[side, 0:local, :] + factor
                    extra_out[side, local:, :] = extra_in[side, local:, :] + edge_part
                    extra_copy(side).start()

        return carry

    lax.fori_loop(0, SKEW * (last - 1) + chunks, chain_step, jnp.int32(0))

    for hop in hops:
        copies_copy(hop, lax.rem(x + hop, width)).wait_recv()

    def stage_copy(hop, a):
        return remote(
            staged.at[hop, a], pool.at[x, a // 2, o], stage_send.at[hop, a], pool_recv.at[x, a // 2, o],
            {"walk": lax.rem(x + hop, width), "orb": a % 2},
        )

    def swap_core():
        return remote(edge.at[o], edge.at[o], edge_sems.at[0], edge_sems.at[1], {"orb": 1 - o})

    for a in range(half):
        @pl.when(at_owner[a])
        def _():
            for hop in range(width):
                source = copies[lax.rem(x + hop, width), base + a]
                held = walkers[source % local]
                if hop > 0:
                    staged[hop, a] = held
                    stage_copy(hop, a).start()
                else:
                    @pl.when(a % 2 == o)
                    def _():
                        pool[x, a // 2, o] = held

                    @pl.when(a % 2 != o)
                    def _():
                        staged[hop, a] = held
                        stage_copy(hop, a).start()

            @pl.when(a % 2 != o)
            def _():
                def give(c, carry):
                    leaving[near, c] = part_of(near, c).astype(BF16)
                    swap_copy(c).start()
                    return carry

                lax.fori_loop(a * each, (a + 1) * each, give, jnp.int32(0))

        if insets[a]:
            @pl.when(at_end)
            def _():
                def back_step(c, carry):
                    leaving[near, c] = part_of(near, c).astype(BF16)
                    back_copy(c).start()
                    return carry

                lax.fori_loop(a * each, (a + 1) * each, back_step, jnp.int32(0))

    for side in range(2):
        @pl.when(at_end & (near == side))
        def _():
            extra_copy(side).wait_recv()

    owning = functools.reduce(jnp.logical_or, at_owner)

    @pl.when(owning)
    def _():
        edge[o] = edge_part + extra_in[0, local:, :] + extra_in[1, local:, :]
        swap_core().start()
        swap_core().wait_recv()

    share = rows // PARTS
    short = last <= REACH
    plans = [
        tuple(n for n in PLANS[min(half - a, len(PLANS)) - 1] if -insets[a] <= n <= last - insets[a])
        if short else (1,) + (-1,) * insets[a] for a in range(half)
    ]

    def passes(a, away):
        if not short:
            return (away > 0) & (away < last - insets[a])
        gaps = [away == n for n in range(1, last - insets[a]) if n + 1 not in plans[a]]
        return functools.reduce(jnp.logical_or, gaps, jnp.bool_(False))

    def place(w, part):
        return gathered.at[w, pl.ds(part * share, share)]

    def away_z(n):
        return jnp.where(near == 0, z + n, z - n)

    def spread_copies(a):
        w = base + a
        targets = []
        for n in plans[a]:
            for core in (1 - a % 2, a % 2):
                targets.append((core, {"vec": away_z(n), "orb": core}))
        targets.append((1 - a % 2, {"orb": 1 - o}))
        return [
            remote(
                result.at[a // 2, core, pl.ds(part * share, share)], place(w, part),
                own_send.at[a // 2, n, part], slot_recv.at[w, part], where,
            )
            for n, (core, where) in enumerate(targets)
            for part in range(PARTS)
        ]

    upper = lax.broadcasted_iota(jnp.int32, (block, block), 0) < lax.broadcasted_iota(jnp.int32, (block, block), 1)
    level_mask = lax.broadcasted_iota(jnp.int32, (block, block), 0) == lax.broadcasted_iota(jnp.int32, (block, block), 1)

    def finish(a):
        w = base + a
        i = a // 2

        def put(r, c, value):
            full[columns(r), columns(c)] = value

        for n in range(BLOCKS):
            first_c = a * each + n * SUB
            for c in range(first_c, first_c + SUB):
                remote(
                    leaving.at[near, c], arrived.at[near, c], chain_send.at[near, c], chain_recv.at[near, c], {"vec": inward}
                ).wait_recv()
                swap_copy(c).wait_recv()
                remote(
                    leaving.at[near, c], crossed.at[c], chain_send.at[near, c], cross_recv.at[c],
                    {"vec": inward, "orb": 1 - o},
                ).wait_recv()
                if insets[a]:
                    for core in range(2):
                        remote(
                            leaving.at[near, c], back.at[core, c], chain_send.at[near, c], back_recv.at[core, c],
                            {"vec": away_z(-1), "orb": core},
                        ).wait_recv()
            run = pl.ds(first_c, SUB)
            kept = partial[w, n] + arrived[near, run].reshape(block, block).astype(F32)
            taken = given[run].reshape(block, block).astype(F32) + crossed[run].reshape(block, block).astype(F32)
            if insets[a]:
                kept = kept + back[o, run].reshape(block, block).astype(F32)
                taken = taken + back[1 - o, run].reshape(block, block).astype(F32)
            for core, value in ((o, kept), (1 - o, taken)):
                if n == 0:
                    flipped = value.T
                    line = edge[core, pl.ds(w, 1), :]
                    put(2 * core, 2 * core, jnp.where(upper | level_mask, value, flipped).astype(BF16))
                    low = jnp.where(level_mask, jnp.broadcast_to(line, (block, block)), jnp.where(upper, flipped, value))
                    put(2 * core + 1, 2 * core + 1, low.astype(BF16))
                else:
                    r, k = ((2 * core, 1), (2 * core, 2 + core), (2 * core + 1, 3 * (1 - core)))[n - 1]
                    value = value.astype(BF16)
                    put(r, k, value)
                    put(k, r, value.T)

        for hop in range(width):
            other = lax.rem(x + hop, width)
            for core in range(2):
                arrival = remote(
                    staged.at[0, 0], pool.at[other, i, core], stage_send.at[0, 0], pool_recv.at[other, i, core],
                    {"walk": other, "orb": core},
                )
                if hop > 0:
                    arrival.wait_recv()
                else:
                    @pl.when(core != o)
                    def _():
                        arrival.wait_recv()
        column = copies[x, w] // local
        for core in range(2):
            start = pool[0, i, core]
            for other in hops:
                start = jnp.where(column == other, pool[other, i, core], start)
            term[core * rows:(core + 1) * rows, :] = start
        running = term[...].astype(F32)
        for degree in range(1, ORDER + 1):
            fresh = (jnp.dot(full[...], term[...], preferred_element_type=F32) * (1.0 / degree)).astype(BF16)
            running = running + fresh.astype(F32)
            if degree < ORDER:
                term[...] = fresh
        result[i] = running.astype(BF16).reshape(2, rows, electrons)
        for copy in spread_copies(a):
            copy.start()
        gathered[w] = result[i, o]

    for a in range(half):
        @pl.when(at_owner[a] & (a % 2 == o))
        def _():
            finish(a)

    new_log = old_log + factor + extra_in[0, 0:local, :] + extra_in[1, 0:local, :]
    out_log[...] = new_log

    def onward(w, part, hop_to):
        spot = place(w, part)
        return remote(spot, spot, next_send.at[w, part], slot_recv.at[w, part], {"vec": hop_to})

    def route(side, a):
        w = side * half + a
        away = jnp.where(side == 0, z, last - z) - insets[a]
        hop_to = jnp.where(side == 0, z + 1, z - 1)
        return w, away, hop_to

    for a in range(half):
        for side in (near, 1 - near):
            w, away, hop_to = route(side, a)

            @pl.when((away != 0) | (o != a % 2))
            def _():
                for part in range(PARTS):
                    onward(w, part, hop_to).wait_recv()

                    @pl.when(passes(a, away))
                    def _():
                        onward(w, part, hop_to).start()


    for copy in bias_copies:
        copy.wait_send()
    for hop in hops:
        facts_copy(hop, x).wait_send()
        copies_copy(hop, x).wait_send()

    def drain(c, carry):
        for side in range(2):
            @pl.when(downstream[side] - depth_of(c) > 0)
            def _():
                chain_copy(side, c).wait_send()

        return carry

    lax.fori_loop(0, chunks, drain, jnp.int32(0))
    for side in range(2):
        @pl.when(downstream[side] > 0)
        def _():
            extra_copy(side).wait_send()

    @pl.when(owning)
    def _():
        swap_core().wait_send()

    for a in range(half):
        @pl.when(at_owner[a])
        def _():
            for hop in hops:
                stage_copy(hop, a).wait_send()

            @pl.when(a % 2 != o)
            def _():
                stage_copy(0, a).wait_send()

                def taken_back(c, carry):
                    swap_copy(c).wait_send()
                    return carry

                lax.fori_loop(a * each, (a + 1) * each, taken_back, jnp.int32(0))

            @pl.when(a % 2 == o)
            def _():
                for copy in spread_copies(a):
                    copy.wait_send()

        if insets[a]:
            @pl.when(at_end)
            def _():
                def back_done(c, carry):
                    back_copy(c).wait_send()
                    return carry

                lax.fori_loop(a * each, (a + 1) * each, back_done, jnp.int32(0))

    for a in range(half):
        for side in range(2):
            w, away, hop_to = route(side, a)

            @pl.when(passes(a, away))
            def _():
                for part in range(PARTS):
                    onward(w, part, hop_to).wait_send()


def per_device(depth, width, walkers, inv_intersection, trial, vectors, aux_field, log_weight, copy_list):
    local, rows, electrons = walkers.shape
    count, _, orbitals = vectors.shape
    half = local // 2
    block = orbitals // 4
    span = 2 * block // count
    wide = count * span
    piece = block // SUB
    chunks = half * BLOCKS * SUB
    mine = half // 2
    lanes = 128
    reach = max(max(depth - 1, 1) if depth - 1 <= REACH else 1, 2)
    dma = pltpu.SemaphoreType.DMA
    anywhere = pl.BlockSpec(memory_space=pl.ANY)
    out, out_log = pl.pallas_call(
        functools.partial(kernel, depth, width),
        out_shape=(
            pltpu.VMEM(walkers.shape, BF16),
            pltpu.VMEM((local, 128), F32),
        ),
        in_specs=[anywhere] * 7,
        out_specs=(pl.BlockSpec(memory_space=pltpu.VMEM), pl.BlockSpec(memory_space=pltpu.VMEM)),
        scratch_shapes=[
            pltpu.VMEM(walkers.shape, BF16),
            pltpu.VMEM(inv_intersection.shape, BF16),
            pltpu.VMEM(trial.shape, BF16),
            pltpu.VMEM(vectors.shape, BF16),
            pltpu.VMEM(aux_field.shape, F32),
            pltpu.SMEM((local,), F32),
            pltpu.SMEM((width, local), jnp.int32),
            pltpu.VMEM((local, rows, electrons), BF16),
            pltpu.VMEM((count, rows, electrons), BF16),
            pltpu.VMEM((block // span, wide, BLOCKS * block), BF16),
            pltpu.VMEM((wide, block), BF16),
            pltpu.VMEM((2, width, local, wide), F32),
            pltpu.VMEM((width, local, lanes), F32),
            pltpu.VMEM((local, lanes), F32),
            pltpu.VMEM((local, wide), F32),
            pltpu.VMEM((local, BLOCKS, block, block), F32),
            pltpu.VMEM((2, chunks, piece, block), BF16),
            pltpu.VMEM((2, chunks, piece, block), BF16),
            pltpu.VMEM((chunks, piece, block), BF16),
            pltpu.VMEM((chunks, piece, block), BF16),
            pltpu.VMEM((2, chunks, piece, block), BF16),
            pltpu.VMEM((2, 2 * local, lanes), F32),
            pltpu.VMEM((2, 2 * local, lanes), F32),
            pltpu.VMEM((2, local, lanes), F32),
            pltpu.VMEM((width, half, rows, electrons), BF16),
            pltpu.VMEM((width, mine, 2, rows, electrons), BF16),
            pltpu.VMEM((orbitals, orbitals), BF16),
            pltpu.VMEM((orbitals, electrons), BF16),
            pltpu.VMEM((mine, 2, rows, electrons), BF16),
            dma((6 + LOADS,)),
            dma((width,)),
            dma((width,)),
            dma((width,)),
            dma((width,)),
            dma((2 * width,)),
            dma((2, width)),
            dma((2, chunks)),
            dma((2, chunks)),
            dma((chunks,)),
            dma((2, chunks)),
            dma((chunks,)),
            dma((chunks,)),
            dma((2,)),
            dma((2,)),
            dma((2,)),
            dma((width, half)),
            dma((width, mine, 2)),
            dma((mine, 2 * reach + 1, PARTS)),
            dma((local, PARTS)),
            dma((local, PARTS)),
        ],
        compiler_params=pltpu.CompilerParams(collective_id=0, has_side_effects=True),
    )(walkers, inv_intersection, trial, vectors, aux_field, log_weight, copy_list)

    def settle(out_ref, log_ref, o1, o2, flat, sems):
        c1 = pltpu.make_async_copy(out_ref, o1, sems.at[0])
        c1.start()
        for s in range(local):
            flat[s] = jnp.max(log_ref[s:s + 1, :])
        c2 = pltpu.make_async_copy(flat, o2, sems.at[1])
        c2.start()
        c1.wait()
        c2.wait()

    return pl.pallas_call(
        settle,
        out_shape=(jax.ShapeDtypeStruct(walkers.shape, BF16), jax.ShapeDtypeStruct((local,), F32)),
        in_specs=[pl.BlockSpec(memory_space=pltpu.VMEM)] * 2,
        out_specs=(anywhere, anywhere),
        scratch_shapes=[pltpu.SMEM((local,), F32), dma((2,))],
    )(pltpu.with_memory_space_constraint(out, pltpu.VMEM), pltpu.with_memory_space_constraint(out_log, pltpu.VMEM))


def solution(mesh):
    depth, width = mesh.shape["vec"], mesh.shape["walk"]
    assert mesh.shape["orb"] == 2 and depth > 1
    return jax.shard_map(
        functools.partial(per_device, depth, width),
        mesh=mesh,
        in_specs=(
            P(("grp", "walk"), "orb", None),
            P(("grp", "walk"), None, None),
            P(),
            P("vec", "orb", None),
            P(("grp", "walk"), "vec"),
            P(("grp", "walk")),
            P(("grp", "walk")),
        ),
        out_specs=(P(("grp", "walk"), "orb", None), P(("grp", "walk"))),
        check_vma=False,
    )
```

```python
import functools
import math

import jax
import jax.numpy as jnp
from jax import lax
from jax.experimental import pallas as pl
from jax.experimental.pallas import tpu as pltpu
from jax.sharding import PartitionSpec as P

ORDER = 6
BLOCKS = 4
SUB = 1
SKEW = 4
SKIPS = ()
PARTS = 1
LOADS = 4
REACH = 3
PLANS = ((2, -1, 1), (3, 2, 1), (3, 2, 1), (2, 1))
MESH = pl.DeviceIdType.MESH
F32 = jnp.float32
BF16 = jnp.bfloat16

step_root = math.sqrt(0.08)


def remote(src, dst, send, recv, where):
    return pltpu.make_async_remote_copy(
        src_ref=src, dst_ref=dst, send_sem=send, recv_sem=recv, device_id=where, device_id_type=MESH
    )


def kernel(
    depth, width,
    walkers_in, inverse_in, trial_in, vectors_in, aux_in, log_in, copies_in,
    out, out_log,
    walkers, inverse, trial, vectors, aux, log_weight, copies,
    green, mixed, strips, level, bias_all, facts, known, picked, partial, leaving, arrived, given, crossed,
    back, extra_in, extra_out, edge, staged, pool, full, term, result,
    load_sems, copies_send, copies_recv, facts_send, facts_recv, bias_send, bias_recv,
    chain_send, chain_recv, cross_recv, back_recv, swap_send, swap_recv, extra_send, extra_recv, edge_sems,
    stage_send, pool_recv, own_send, next_send, slot_recv, write_sems,
):
    gathered = out
    z = lax.axis_index("vec")
    x = lax.axis_index("walk")
    o = lax.axis_index("orb")
    last = depth - 1
    local, rows, electrons = walkers.shape
    count, _, orbitals = vectors.shape
    half = local // 2
    block = orbitals // 4
    span = 2 * block // count
    wide = count * span
    piece = block // SUB
    each = BLOCKS * SUB
    chunks = half * each
    mine = half // 2
    lanes = extra_in.shape[2]
    insets = [1 if a == half - 1 and last >= REACH else 0 for a in range(half)]
    skips = [last >= REACH and a in SKIPS and not insets[a] for a in range(half)]
    hops = range(1, width)

    barrier = pltpu.get_barrier_semaphore()

    def greet(where):
        pl.semaphore_signal(barrier, inc=1, device_id=where, device_id_type=MESH)

    greet({"orb": 1 - o})
    for hop in hops:
        for core in range(2):
            greet({"walk": lax.rem(x + hop, width), "orb": core})

    for hop in (1, 2):
        @pl.when(z >= hop)
        def _():
            for core in range(2):
                greet({"vec": z - hop, "orb": core})

        @pl.when(z <= last - hop)
        def _():
            for core in range(2):
                greet({"vec": z + hop, "orb": core})

    batch = count // LOADS
    pairs = [
        (inverse_in, inverse), (walkers_in, walkers), (trial_in, trial), (copies_in, copies.at[x]), (log_in, log_weight),
        (aux_in, aux),
    ]
    for n in range(LOADS):
        group = pl.ds(n * batch, batch)
        pairs.append((vectors_in.at[group], vectors.at[group]))
    loads = [pltpu.make_async_copy(src, dst, load_sems.at[n]) for n, (src, dst) in enumerate(pairs)]
    for load in loads:
        load.start()

    loads[0].wait()
    loads[1].wait()
    for w in range(local):
        green[w] = jnp.dot(walkers[w], inverse[w], preferred_element_type=F32).astype(BF16)
    for n in range(2, 6):
        loads[n].wait()
    walker_id = lax.broadcasted_iota(jnp.int32, (local, lanes), 0)
    weights = jnp.zeros((local, lanes), F32)
    for w in range(local):
        weights = jnp.where(walker_id == w, log_weight[w], weights)
    facts[x] = weights
    facts[x, :, 0:count] = aux[...]
    for n in range(LOADS):
        loads[6 + n].wait()
        for g in range(n * batch, (n + 1) * batch):
            mixed[g] = jnp.dot(vectors[g], trial[...], preferred_element_type=F32).astype(BF16)
    left = [green[:, j * span:(j + 1) * span, :].reshape(local * span, electrons) for j in range(rows // span)]
    right = [mixed[:, j * span:(j + 1) * span, :].reshape(wide, electrons) for j in range(rows // span)]
    gram = lax.dot_general(
        jnp.concatenate(left, axis=1), jnp.concatenate(right, axis=1), (((1,), (1,)), ((), ())), preferred_element_type=F32
    )
    row_id = lax.broadcasted_iota(jnp.int32, (local * span, wide), 0)
    col_id = lax.broadcasted_iota(jnp.int32, (local * span, wide), 1)
    same = row_id % span == col_id % span
    folded = jnp.sum(jnp.where(same, gram, 0.0).reshape(local, span, wide), axis=1)
    lane_id = lax.broadcasted_iota(jnp.int32, (local, wide), 1)
    reach = 1
    while reach < span:
        low = lane_id % (2 * reach) < reach
        folded = folded + jnp.where(low, pltpu.roll(folded, wide - reach, 1), pltpu.roll(folded, reach, 1))
        reach *= 2
    bias_all[o, x] = folded

    sides = sum(jnp.where(z >= hop, 2, 0) + jnp.where(z <= last - hop, 2, 0) for hop in (1, 2))
    pl.semaphore_wait(barrier, 1 + 2 * (width - 1) + sides)

    bias_peers = [{"walk": lax.rem(x + hop, width), "orb": core} for hop in hops for core in range(2)] + [{"orb": 1 - o}]
    bias_copies = [
        remote(bias_all.at[o, x], bias_all.at[o, x], bias_send.at[n], bias_recv.at[o, x], where)
        for n, where in enumerate(bias_peers)
    ]
    def facts_copy(hop, owner):
        return remote(
            facts.at[owner], facts.at[owner], facts_send.at[hop], facts_recv.at[owner], {"walk": lax.rem(x + hop, width)}
        )

    def copies_copy(hop, owner):
        return remote(
            copies.at[owner], copies.at[owner], copies_send.at[hop], copies_recv.at[owner],
            {"walk": lax.rem(x + hop, width)},
        )

    for copy in bias_copies:
        copy.start()
    for hop in hops:
        facts_copy(hop, x).start()
        copies_copy(hop, x).start()

    chunk_row = lax.broadcasted_iota(jnp.int32, (count, span, block), 1)
    chunk_col = lax.broadcasted_iota(jnp.int32, (count, span, block), 2)
    crossing = jnp.zeros((count, span, block), F32)

    def columns(n):
        return pl.ds(pl.multiple_of(n * block, block), block)

    for j in range(block // span):
        here = slice(j * span, (j + 1) * span)
        below = slice(block + j * span, block + (j + 1) * span)
        first = vectors[:, here, columns(2 * o)].astype(F32)
        second = vectors[:, below, columns(1 + 2 * o)].astype(F32)
        crossing = crossing + jnp.where(chunk_row + j * span == chunk_col, second, 0.0)
        joined = jnp.where(chunk_row + j * span <= chunk_col, first, second).astype(BF16)
        strips[j, :, 0:block] = joined.reshape(wide, block)
        strips[j, :, block:2 * block] = vectors[:, here, block:2 * block].reshape(wide, block)
        strips[j, :, 2 * block:3 * block] = vectors[:, here, columns(2 + o)].reshape(wide, block)
        strips[j, :, 3 * block:] = vectors[:, below, columns(3 * (1 - o))].reshape(wide, block)
    level[...] = crossing.reshape(wide, block).astype(BF16)

    for hop in hops:
        facts_copy(hop, lax.rem(x + hop, width)).wait_recv()
    sources = [(copies[x, s] // local, pl.ds(copies[x, s] % local, 1)) for s in range(local)]
    for s, (column, row) in enumerate(sources):
        known[s:s + 1, :] = facts[column, row, :]
    pick_row = lax.broadcasted_iota(jnp.int32, (count, wide), 0)
    pick_col = lax.broadcasted_iota(jnp.int32, (count, wide), 1)
    pick = jnp.where(pick_row == pick_col // span, 1.0, 0.0).astype(F32)
    drawn = jnp.dot(known[:, 0:count], pick, precision=lax.Precision.HIGHEST, preferred_element_type=F32)
    old_log = jnp.broadcast_to(known[:, count:count + 1], (local, lanes))

    for hop in hops:
        other = lax.rem(x + hop, width)
        for core in range(2):
            remote(
                bias_all.at[core, other], bias_all.at[core, other], bias_send.at[0], bias_recv.at[core, other], {"walk": other}
            ).wait_recv()
    remote(bias_all.at[1 - o, x], bias_all.at[1 - o, x], bias_send.at[0], bias_recv.at[1 - o, x], {"orb": 1 - o}).wait_recv()

    for s, (column, row) in enumerate(sources):
        picked[s:s + 1, :] = bias_all[0, column, row, :] + bias_all[1, column, row, :]
    bias = picked[...]
    shift = -step_root * bias
    field = drawn - shift
    factor = jnp.sum(drawn * shift - 0.5 * shift * shift, axis=1, keepdims=True) * (1.0 / span)
    factor = jnp.broadcast_to(factor, (local, lanes))
    weighted = (field * step_root).astype(BF16)
    spread = jnp.broadcast_to(weighted.astype(F32)[:, None, :], (local, span, wide)).reshape(local * span, wide)
    kron = jnp.where(same, spread, 0.0).astype(BF16)

    for j in range(block // span):
        summed = jnp.dot(kron, strips[j], preferred_element_type=F32)
        for n in range(BLOCKS):
            partial[:, n, j * span:(j + 1) * span, :] = summed[:, n * block:(n + 1) * block].reshape(local, span, block)
    edge_part = jnp.dot(weighted, level[...], preferred_element_type=F32)

    def to_next(side):
        return jnp.where(side == 0, z - 1, z + 1)

    def to_far(side):
        return jnp.where(side == 0, z - 2, z + 2)

    upstream = [last - z, z]
    downstream = [z, last - z]
    at_end = (z == 0) | (z == last)
    near = jnp.where(z <= last - z, 0, 1)
    base = near * half
    inward = jnp.where(near == 0, z + 1, z - 1)
    at_owner = [(z == n) | (z == last - n) for n in insets]

    def depth_of(c):
        return sum(jnp.where(c // each == a, n, 0) for a, n in enumerate(insets) if n) + jnp.int32(0)

    def skip_of(c):
        return functools.reduce(jnp.logical_or, [c // each == a for a in range(half) if skips[a]], jnp.bool_(False))

    def chain_copy(side, c, hop=to_next):
        return remote(
            leaving.at[side, c], arrived.at[side, c], chain_send.at[side, c // each], chain_recv.at[side, c], {"vec": hop(side)}
        )

    def cross_copy(side, c, hop=to_next):
        return remote(
            leaving.at[side, c], crossed.at[c], chain_send.at[side, c // each], cross_recv.at[c // (2 * each) * each + c % each], {"vec": hop(side), "orb": 1 - o}
        )

    def raw_copy(side, c):
        return remote(
            leaving.at[side, c], back.at[o, c], chain_send.at[side, c // each], back_recv.at[o, c // (2 * each)],
            {"vec": to_next(side), "orb": (c // each) % 2},
        )

    def swap_copy(c):
        return remote(leaving.at[near, c], given.at[c], swap_send.at[c // (2 * each)], swap_recv.at[c // (2 * each)], {"orb": 1 - o})

    def extra_copy(side):
        return remote(
            extra_out.at[side], extra_in.at[side], extra_send.at[side], extra_recv.at[side], {"vec": to_next(side)}
        )

    def back_copy(c):
        return remote(
            leaving.at[near, c], back.at[o, c], chain_send.at[near, c // each], back_recv.at[o, c // (2 * each)],
            {"vec": inward, "orb": (c // each) % 2},
        )

    def part_of(side, c):
        at = c % each
        return partial[side * half + c // each, at // SUB, pl.ds(pl.multiple_of((at % SUB) * piece, piece), piece), :]

    def chain_step(t, carry):
        for turn in range(2):
            side = jnp.where(z <= last - z, 1 - turn, turn)
            before = jnp.where(side == 0, last - z, z)
            after = last - before
            c = t - SKEW * before
            head = before == 0
            togo = after - depth_of(c)
            skip = skip_of(c)

            @pl.when((c >= 0) & (c < chunks) & ((togo > 1) | ((togo == 1) & jnp.logical_not(skip))))
            def _():
                own = part_of(side, c)
                here = (c // each) % 2 == o

                @pl.when(head)
                def _():
                    leaving[side, c] = own.astype(BF16)

                @pl.when(jnp.logical_not(head))
                def _():
                    chain_copy(side, c).wait_recv()
                    leaving[side, c] = (own + arrived[side, c].astype(F32)).astype(BF16)

                jump = skip & (togo == 2)

                @pl.when(jnp.logical_not(jump) & ((togo > 1) | here))
                def _():
                    chain_copy(side, c).start()

                @pl.when((togo == 1) & jnp.logical_not(here))
                def _():
                    cross_copy(side, c).start()

                @pl.when(jump & here)
                def _():
                    chain_copy(side, c, to_far).start()

                @pl.when(jump & jnp.logical_not(here))
                def _():
                    cross_copy(side, c, to_far).start()

            @pl.when((c == 0) & (after > 0))
            def _():
                @pl.when(head)
                def _():
                    extra_in[side] = jnp.zeros_like(extra_in[side])

                @pl.when(jnp.logical_not(head))
                def _():
                    extra_copy(side).wait_recv()

                extra_out[side, 0:local, :] = extra_in[side, 0:local, :] + factor
                extra_out[side, local:, :] = extra_in[side, local:, :] + edge_part
                extra_copy(side).start()

        return carry

    for side in range(2):
        @pl.when(downstream[side] == 1)
        def _():
            def raw_step(c, carry):
                leaving[side, c] = part_of(side, c).astype(BF16)
                raw_copy(side, c).start()
                return carry

            for a in range(half):
                if skips[a]:
                    lax.fori_loop(a * each, (a + 1) * each, raw_step, jnp.int32(0))

    lax.fori_loop(0, SKEW * (last - 1) + chunks, chain_step, jnp.int32(0))

    for hop in hops:
        copies_copy(hop, lax.rem(x + hop, width)).wait_recv()

    def stage_copy(hop, a):
        return remote(
            staged.at[hop, a], pool.at[x, a // 2, o], stage_send.at[hop, a], pool_recv.at[x, a // 2, o],
            {"walk": lax.rem(x + hop, width), "orb": a % 2},
        )

    def swap_core():
        return remote(edge.at[o], edge.at[o], edge_sems.at[0], edge_sems.at[1], {"orb": 1 - o})

    for a in range(half):
        @pl.when(at_owner[a])
        def _():
            for hop in range(width):
                source = copies[lax.rem(x + hop, width), base + a]
                held = walkers[source % local]
                if hop > 0:
                    staged[hop, a] = held
                    stage_copy(hop, a).start()
                else:
                    @pl.when(a % 2 == o)
                    def _():
                        pool[x, a // 2, o] = held

                    @pl.when(a % 2 != o)
                    def _():
                        staged[hop, a] = held
                        stage_copy(hop, a).start()

            @pl.when(a % 2 != o)
            def _():
                def give(c, carry):
                    leaving[near, c] = part_of(near, c).astype(BF16)
                    swap_copy(c).start()
                    return carry

                lax.fori_loop(a * each, (a + 1) * each, give, jnp.int32(0))

        if insets[a]:
            @pl.when(at_end)
            def _():
                def back_step(c, carry):
                    leaving[near, c] = part_of(near, c).astype(BF16)
                    back_copy(c).start()
                    return carry

                lax.fori_loop(a * each, (a + 1) * each, back_step, jnp.int32(0))

    for side in range(2):
        @pl.when(at_end & (near == side))
        def _():
            extra_copy(side).wait_recv()

    owning = functools.reduce(jnp.logical_or, at_owner)

    @pl.when(owning)
    def _():
        edge[o] = edge_part + extra_in[0, local:, :] + extra_in[1, local:, :]
        swap_core().start()
        swap_core().wait_recv()

    share = rows // PARTS
    short = last <= REACH
    plans = [
        tuple(n for n in PLANS[min(half - a, len(PLANS)) - 1] if -insets[a] <= n <= last - insets[a])
        if short else (1,) + (-1,) * insets[a] for a in range(half)
    ]

    def passes(a, away):
        if not short:
            return (away > 0) & (away < last - insets[a])
        gaps = [away == n for n in range(1, last - insets[a]) if n + 1 not in plans[a]]
        return functools.reduce(jnp.logical_or, gaps, jnp.bool_(False))

    def place(w, part):
        return gathered.at[w, pl.ds(part * share, share)]

    def away_z(n):
        return jnp.where(near == 0, z + n, z - n)

    def spread_copies(a):
        w = base + a
        targets = []
        for n in plans[a]:
            for core in (1 - a % 2, a % 2):
                targets.append((core, {"vec": away_z(n), "orb": core}))
        targets.append((1 - a % 2, {"orb": 1 - o}))
        return [
            remote(
                result.at[a // 2, core, pl.ds(part * share, share)], place(w, part),
                own_send.at[a // 2, n, part], slot_recv.at[w, part], where,
            )
            for n, (core, where) in enumerate(targets)
            for part in range(PARTS)
        ]

    upper = lax.broadcasted_iota(jnp.int32, (block, block), 0) < lax.broadcasted_iota(jnp.int32, (block, block), 1)
    level_mask = lax.broadcasted_iota(jnp.int32, (block, block), 0) == lax.broadcasted_iota(jnp.int32, (block, block), 1)

    def finish(a):
        w = base + a
        i = a // 2

        def put(r, c, value):
            full[columns(r), columns(c)] = value

        whole = pl.ds(a * each, each)
        remote(leaving.at[near, whole], given.at[whole], swap_send.at[i], swap_recv.at[i], {"orb": 1 - o}).wait_recv()
        if insets[a] or skips[a]:
            for core in range(2):
                remote(
                    leaving.at[near, whole], back.at[core, whole], chain_send.at[near, a], back_recv.at[core, i],
                    {"vec": inward, "orb": core},
                ).wait_recv()
        for n in range(BLOCKS):
            first_c = a * each + n * SUB
            for c in range(first_c, first_c + SUB):
                remote(
                    leaving.at[near, c], arrived.at[near, c], chain_send.at[near, c // each], chain_recv.at[near, c], {"vec": inward}
                ).wait_recv()
                remote(
                    leaving.at[near, c], crossed.at[c], chain_send.at[near, c // each], cross_recv.at[c // (2 * each) * each + c % each],
                    {"vec": inward, "orb": 1 - o},
                ).wait_recv()
            run = pl.ds(first_c, SUB)
            kept = partial[w, n] + arrived[near, run].reshape(block, block).astype(F32)
            taken = given[run].reshape(block, block).astype(F32) + crossed[run].reshape(block, block).astype(F32)
            if insets[a] or skips[a]:
                kept = kept + back[o, run].reshape(block, block).astype(F32)
                taken = taken + back[1 - o, run].reshape(block, block).astype(F32)
            for core, value in ((o, kept), (1 - o, taken)):
                if n == 0:
                    flipped = value.T
                    line = edge[core, pl.ds(w, 1), :]
                    put(2 * core, 2 * core, jnp.where(upper | level_mask, value, flipped).astype(BF16))
                    low = jnp.where(level_mask, jnp.broadcast_to(line, (block, block)), jnp.where(upper, flipped, value))
                    put(2 * core + 1, 2 * core + 1, low.astype(BF16))
                else:
                    r, k = ((2 * core, 1), (2 * core, 2 + core), (2 * core + 1, 3 * (1 - core)))[n - 1]
                    value = value.astype(BF16)
                    put(r, k, value)
                    put(k, r, value.T)

        for hop in range(width):
            other = lax.rem(x + hop, width)
            for core in range(2):
                arrival = remote(
                    staged.at[0, 0], pool.at[other, i, core], stage_send.at[0, 0], pool_recv.at[other, i, core],
                    {"walk": other, "orb": core},
                )
                if hop > 0:
                    arrival.wait_recv()
                else:
                    @pl.when(core != o)
                    def _():
                        arrival.wait_recv()
        column = copies[x, w] // local
        for core in range(2):
            start = pool[0, i, core]
            for other in hops:
                start = jnp.where(column == other, pool[other, i, core], start)
            term[core * rows:(core + 1) * rows, :] = start
        running = term[...].astype(F32)
        for degree in range(1, ORDER + 1):
            fresh = (jnp.dot(full[...], term[...], preferred_element_type=F32) * (1.0 / degree)).astype(BF16)
            running = running + fresh.astype(F32)
            if degree < ORDER:
                term[...] = fresh
        result[i] = running.astype(BF16).reshape(2, rows, electrons)
        for copy in spread_copies(a):
            copy.start()
        settle = pltpu.make_async_copy(result.at[i, o], gathered.at[w], write_sems.at[i])
        settle.start()

    for a in range(half):
        @pl.when(at_owner[a] & (a % 2 == o))
        def _():
            finish(a)

    new_log = old_log + factor + extra_in[0, 0:local, :] + extra_in[1, 0:local, :]
    out_log[...] = new_log

    def onward(w, part, hop_to):
        spot = place(w, part)
        return remote(spot, spot, next_send.at[w, part], slot_recv.at[w, part], {"vec": hop_to})

    def route(side, a):
        w = side * half + a
        away = jnp.where(side == 0, z, last - z) - insets[a]
        hop_to = jnp.where(side == 0, z + 1, z - 1)
        return w, away, hop_to

    for a in range(half):
        for side in (near, 1 - near):
            w, away, hop_to = route(side, a)

            @pl.when(passes(a, away))
            def _():
                for part in range(PARTS):
                    onward(w, part, hop_to).wait_recv()
                    onward(w, part, hop_to).start()

    for copy in bias_copies:
        copy.wait_send()
    for hop in hops:
        facts_copy(hop, x).wait_send()
        copies_copy(hop, x).wait_send()

    def sent(side, a):
        whole = pl.ds(a * each, each)
        return remote(
            leaving.at[side, whole], arrived.at[side, whole], chain_send.at[side, a], chain_recv.at[side, a], {"orb": 1 - o}
        )

    for side in range(2):
        for a in range(half):
            @pl.when(downstream[side] - insets[a] != 0)
            def _():
                sent(side, a).wait_send()

    for side in range(2):
        @pl.when(downstream[side] > 0)
        def _():
            extra_copy(side).wait_send()

    @pl.when(owning)
    def _():
        swap_core().wait_send()

    for a in range(half):
        @pl.when(at_owner[a])
        def _():
            for hop in hops:
                stage_copy(hop, a).wait_send()

            @pl.when(a % 2 != o)
            def _():
                stage_copy(0, a).wait_send()

                whole = pl.ds(a * each, each)
                remote(
                    leaving.at[near, whole], given.at[whole], swap_send.at[a // 2], swap_recv.at[a // 2], {"orb": 1 - o}
                ).wait_send()

    for a in range(half):
        for side in (near, 1 - near):
            w, away, hop_to = route(side, a)

            @pl.when(((away != 0) | (o != a % 2)) & jnp.logical_not(passes(a, away)))
            def _():
                for part in range(PARTS):
                    onward(w, part, hop_to).wait_recv()

    for a in range(half):
        @pl.when(at_owner[a] & (a % 2 == o))
        def _():
            for copy in spread_copies(a):
                copy.wait_send()
            pltpu.make_async_copy(result.at[a // 2, o], gathered.at[base + a], write_sems.at[a // 2]).wait()

    for a in range(half):
        for side in range(2):
            w, away, hop_to = route(side, a)

            @pl.when(passes(a, away))
            def _():
                for part in range(PARTS):
                    onward(w, part, hop_to).wait_send()


def per_device(depth, width, walkers, inv_intersection, trial, vectors, aux_field, log_weight, copy_list):
    local, rows, electrons = walkers.shape
    count, _, orbitals = vectors.shape
    half = local // 2
    block = orbitals // 4
    span = 2 * block // count
    wide = count * span
    piece = block // SUB
    chunks = half * BLOCKS * SUB
    mine = half // 2
    lanes = 128
    reach = max(max(depth - 1, 1) if depth - 1 <= REACH else 1, 2)
    dma = pltpu.SemaphoreType.DMA
    anywhere = pl.BlockSpec(memory_space=pl.ANY)
    out, out_log = pl.pallas_call(
        functools.partial(kernel, depth, width),
        out_shape=(
            pltpu.VMEM(walkers.shape, BF16),
            pltpu.VMEM((local, 128), F32),
        ),
        in_specs=[anywhere] * 7,
        out_specs=(anywhere, pl.BlockSpec(memory_space=pltpu.VMEM)),
        scratch_shapes=[
            pltpu.VMEM(walkers.shape, BF16),
            pltpu.VMEM(inv_intersection.shape, BF16),
            pltpu.VMEM(trial.shape, BF16),
            pltpu.VMEM(vectors.shape, BF16),
            pltpu.VMEM(aux_field.shape, F32),
            pltpu.SMEM((local,), F32),
            pltpu.SMEM((width, local), jnp.int32),
            pltpu.VMEM((local, rows, electrons), BF16),
            pltpu.VMEM((count, rows, electrons), BF16),
            pltpu.VMEM((block // span, wide, BLOCKS * block), BF16),
            pltpu.VMEM((wide, block), BF16),
            pltpu.VMEM((2, width, local, wide), F32),
            pltpu.VMEM((width, local, lanes), F32),
            pltpu.VMEM((local, lanes), F32),
            pltpu.VMEM((local, wide), F32),
            pltpu.VMEM((local, BLOCKS, block, block), F32),
            pltpu.VMEM((2, chunks, piece, block), BF16),
            pltpu.VMEM((2, chunks, piece, block), BF16),
            pltpu.VMEM((chunks, piece, block), BF16),
            pltpu.VMEM((chunks, piece, block), BF16),
            pltpu.VMEM((2, chunks, piece, block), BF16),
            pltpu.VMEM((2, 2 * local, lanes), F32),
            pltpu.VMEM((2, 2 * local, lanes), F32),
            pltpu.VMEM((2, local, lanes), F32),
            pltpu.VMEM((width, half, rows, electrons), BF16),
            pltpu.VMEM((width, mine, 2, rows, electrons), BF16),
            pltpu.VMEM((orbitals, orbitals), BF16),
            pltpu.VMEM((orbitals, electrons), BF16),
            pltpu.VMEM((mine, 2, rows, electrons), BF16),
            dma((6 + LOADS,)),
            dma((width,)),
            dma((width,)),
            dma((width,)),
            dma((width,)),
            dma((2 * width,)),
            dma((2, width)),
            dma((2, half)),
            dma((2, chunks)),
            dma((chunks // 2,)),
            dma((2, mine)),
            dma((mine,)),
            dma((mine,)),
            dma((2,)),
            dma((2,)),
            dma((2,)),
            dma((width, half)),
            dma((width, mine, 2)),
            dma((mine, 2 * reach + 1, PARTS)),
            dma((local, PARTS)),
            dma((local, PARTS)),
            dma((mine,)),
        ],
        compiler_params=pltpu.CompilerParams(collective_id=0, has_side_effects=True),
    )(walkers, inv_intersection, trial, vectors, aux_field, log_weight, copy_list)

    def settle(out_ref, log_ref, o1, o2, flat, sems):
        c1 = pltpu.make_async_copy(out_ref, o1, sems.at[0])
        c1.start()
        for s in range(local):
            flat[s] = jnp.max(log_ref[s:s + 1, :])
        c2 = pltpu.make_async_copy(flat, o2, sems.at[1])
        c2.start()
        c1.wait()
        c2.wait()

    return pl.pallas_call(
        settle,
        out_shape=(jax.ShapeDtypeStruct(walkers.shape, BF16), jax.ShapeDtypeStruct((local,), F32)),
        in_specs=[pl.BlockSpec(memory_space=pltpu.VMEM)] * 2,
        out_specs=(anywhere, anywhere),
        scratch_shapes=[pltpu.SMEM((local,), F32), dma((2,))],
    )(pltpu.with_memory_space_constraint(out, pltpu.VMEM), pltpu.with_memory_space_constraint(out_log, pltpu.VMEM))


def solution(mesh):
    depth, width = mesh.shape["vec"], mesh.shape["walk"]
    assert mesh.shape["orb"] == 2 and depth > 1
    return jax.shard_map(
        functools.partial(per_device, depth, width),
        mesh=mesh,
        in_specs=(
            P(("grp", "walk"), "orb", None),
            P(("grp", "walk"), None, None),
            P(),
            P("vec", "orb", None),
            P(("grp", "walk"), "vec"),
            P(("grp", "walk")),
            P(("grp", "walk")),
        ),
        out_specs=(P(("grp", "walk"), "orb", None), P(("grp", "walk"))),
        check_vma=False,
    )
```

```python
import functools
import math

import jax
import jax.numpy as jnp
from jax import lax
from jax.experimental import pallas as pl
from jax.experimental.pallas import tpu as pltpu
from jax.sharding import PartitionSpec as P

ORDER = 6
BLOCKS = 4
SUB = 1
SKEW = 4
SKIPS = ()
PARTS = 1
LOADS = 4
REACH = 3
PLANS = ((2, -1, 1), (3, 2, 1), (3, 2, 1), (2, 1))
MESH = pl.DeviceIdType.MESH
F32 = jnp.float32
BF16 = jnp.bfloat16

step_root = math.sqrt(0.08)


def remote(src, dst, send, recv, where):
    return pltpu.make_async_remote_copy(
        src_ref=src, dst_ref=dst, send_sem=send, recv_sem=recv, device_id=where, device_id_type=MESH
    )


def kernel(
    depth, width,
    walkers_in, inverse_in, trial_in, vectors_in, aux_in, log_in, copies_in,
    out, out_log,
    walkers, inverse, trial, vectors, aux, log_weight, copies,
    green, mixed, strips, level, bias_all, facts, known, picked, partial, leaving, arrived, given, crossed,
    back, extra_in, extra_out, edge, staged, pool, full, terms, result,
    load_sems, copies_send, copies_recv, facts_send, facts_recv, bias_send, bias_recv,
    chain_send, chain_recv, cross_recv, back_recv, swap_send, swap_recv, extra_send, extra_recv, edge_sems,
    stage_send, pool_recv, own_send, next_send, slot_recv, write_sems,
):
    gathered = out
    z = lax.axis_index("vec")
    x = lax.axis_index("walk")
    o = lax.axis_index("orb")
    last = depth - 1
    local, rows, electrons = walkers.shape
    count, _, orbitals = vectors.shape
    half = local // 2
    block = orbitals // 4
    span = 2 * block // count
    wide = count * span
    piece = block // SUB
    each = BLOCKS * SUB
    chunks = half * each
    mine = half // 2
    lanes = extra_in.shape[2]
    insets = [1 if a == half - 1 and last >= REACH else 0 for a in range(half)]
    skips = [last >= REACH and a in SKIPS and not insets[a] for a in range(half)]
    hops = range(1, width)

    barrier = pltpu.get_barrier_semaphore()

    def greet(where):
        pl.semaphore_signal(barrier, inc=1, device_id=where, device_id_type=MESH)

    greet({"orb": 1 - o})
    for hop in hops:
        for core in range(2):
            greet({"walk": lax.rem(x + hop, width), "orb": core})

    for hop in (1,):
        @pl.when(z >= hop)
        def _():
            for core in range(2):
                greet({"vec": z - hop, "orb": core})

        @pl.when(z <= last - hop)
        def _():
            for core in range(2):
                greet({"vec": z + hop, "orb": core})

    batch = count // LOADS
    pairs = [(trial_in, trial)]
    for n in range(LOADS):
        group = pl.ds(n * batch, batch)
        pairs.append((vectors_in.at[group], vectors.at[group]))
    pairs += [
        (inverse_in, inverse), (walkers_in, walkers), (copies_in, copies.at[x]), (log_in, log_weight), (aux_in, aux),
    ]
    loads = [pltpu.make_async_copy(src, dst, load_sems.at[n]) for n, (src, dst) in enumerate(pairs)]
    for load in loads:
        load.start()

    loads[0].wait()
    for n in range(LOADS):
        loads[1 + n].wait()
        for g in range(n * batch, (n + 1) * batch):
            mixed[g] = jnp.dot(vectors[g], trial[...], preferred_element_type=F32).astype(BF16)
    for load in loads[1 + LOADS:]:
        load.wait()
    for w in range(local):
        green[w] = jnp.dot(walkers[w], inverse[w], preferred_element_type=F32).astype(BF16)
    walker_id = lax.broadcasted_iota(jnp.int32, (local, lanes), 0)
    weights = jnp.zeros((local, lanes), F32)
    for w in range(local):
        weights = jnp.where(walker_id == w, log_weight[w], weights)
    facts[x] = weights
    facts[x, :, 0:count] = aux[...]
    left = [green[:, j * span:(j + 1) * span, :].reshape(local * span, electrons) for j in range(rows // span)]
    right = [mixed[:, j * span:(j + 1) * span, :].reshape(wide, electrons) for j in range(rows // span)]
    gram = lax.dot_general(
        jnp.concatenate(left, axis=1), jnp.concatenate(right, axis=1), (((1,), (1,)), ((), ())), preferred_element_type=F32
    )
    row_id = lax.broadcasted_iota(jnp.int32, (local * span, wide), 0)
    col_id = lax.broadcasted_iota(jnp.int32, (local * span, wide), 1)
    same = row_id % span == col_id % span
    folded = jnp.sum(jnp.where(same, gram, 0.0).reshape(local, span, wide), axis=1)
    lane_id = lax.broadcasted_iota(jnp.int32, (local, wide), 1)
    reach = 1
    while reach < span:
        low = lane_id % (2 * reach) < reach
        folded = folded + jnp.where(low, pltpu.roll(folded, wide - reach, 1), pltpu.roll(folded, reach, 1))
        reach *= 2
    bias_all[o, x] = folded

    sides = sum(jnp.where(z >= hop, 2, 0) + jnp.where(z <= last - hop, 2, 0) for hop in (1,))
    pl.semaphore_wait(barrier, 1 + 2 * (width - 1) + sides)

    bias_peers = [{"walk": lax.rem(x + hop, width), "orb": core} for hop in hops for core in range(2)] + [{"orb": 1 - o}]
    bias_copies = [
        remote(bias_all.at[o, x], bias_all.at[o, x], bias_send.at[n], bias_recv.at[o, x], where)
        for n, where in enumerate(bias_peers)
    ]
    def facts_copy(hop, owner):
        return remote(
            facts.at[owner], facts.at[owner], facts_send.at[hop], facts_recv.at[owner], {"walk": lax.rem(x + hop, width)}
        )

    def copies_copy(hop, owner):
        return remote(
            copies.at[owner], copies.at[owner], copies_send.at[hop], copies_recv.at[owner],
            {"walk": lax.rem(x + hop, width)},
        )

    for copy in bias_copies:
        copy.start()
    for hop in hops:
        facts_copy(hop, x).start()
        copies_copy(hop, x).start()

    chunk_row = lax.broadcasted_iota(jnp.int32, (count, span, block), 1)
    chunk_col = lax.broadcasted_iota(jnp.int32, (count, span, block), 2)
    crossing = jnp.zeros((count, span, block), F32)

    def columns(n):
        return pl.ds(pl.multiple_of(n * block, block), block)

    for j in range(block // span):
        here = slice(j * span, (j + 1) * span)
        below = slice(block + j * span, block + (j + 1) * span)
        first = vectors[:, here, columns(2 * o)].astype(F32)
        second = vectors[:, below, columns(1 + 2 * o)].astype(F32)
        crossing = crossing + jnp.where(chunk_row + j * span == chunk_col, second, 0.0)
        joined = jnp.where(chunk_row + j * span <= chunk_col, first, second).astype(BF16)
        strips[j, :, 0:block] = joined.reshape(wide, block)
        strips[j, :, block:2 * block] = vectors[:, here, block:2 * block].reshape(wide, block)
        strips[j, :, 2 * block:3 * block] = vectors[:, here, columns(2 + o)].reshape(wide, block)
        strips[j, :, 3 * block:] = vectors[:, below, columns(3 * (1 - o))].reshape(wide, block)
    level[...] = crossing.reshape(wide, block).astype(BF16)

    for hop in hops:
        facts_copy(hop, lax.rem(x + hop, width)).wait_recv()
    sources = [(copies[x, s] // local, pl.ds(copies[x, s] % local, 1)) for s in range(local)]
    for s, (column, row) in enumerate(sources):
        known[s:s + 1, :] = facts[column, row, :]
    pick_row = lax.broadcasted_iota(jnp.int32, (count, wide), 0)
    pick_col = lax.broadcasted_iota(jnp.int32, (count, wide), 1)
    pick = jnp.where(pick_row == pick_col // span, 1.0, 0.0).astype(F32)
    drawn = jnp.dot(known[:, 0:count], pick, precision=lax.Precision.HIGHEST, preferred_element_type=F32)
    old_log = jnp.broadcast_to(known[:, count:count + 1], (local, lanes))

    for hop in hops:
        other = lax.rem(x + hop, width)
        for core in range(2):
            remote(
                bias_all.at[core, other], bias_all.at[core, other], bias_send.at[0], bias_recv.at[core, other], {"walk": other}
            ).wait_recv()
    remote(bias_all.at[1 - o, x], bias_all.at[1 - o, x], bias_send.at[0], bias_recv.at[1 - o, x], {"orb": 1 - o}).wait_recv()

    for s, (column, row) in enumerate(sources):
        picked[s:s + 1, :] = bias_all[0, column, row, :] + bias_all[1, column, row, :]
    bias = picked[...]
    shift = -step_root * bias
    field = drawn - shift
    factor = jnp.sum(drawn * shift - 0.5 * shift * shift, axis=1, keepdims=True) * (1.0 / span)
    factor = jnp.broadcast_to(factor, (local, lanes))
    weighted = (field * step_root).astype(BF16)
    spread = jnp.broadcast_to(weighted.astype(F32)[:, None, :], (local, span, wide)).reshape(local * span, wide)
    kron = jnp.where(same, spread, 0.0).astype(BF16)

    for j in range(block // span):
        summed = jnp.dot(kron, strips[j], preferred_element_type=F32)
        for n in range(BLOCKS):
            partial[:, n, j * span:(j + 1) * span, :] = summed[:, n * block:(n + 1) * block].reshape(local, span, block)
    edge_part = jnp.dot(weighted, level[...], preferred_element_type=F32)

    def to_next(side):
        return jnp.where(side == 0, z - 1, z + 1)

    def to_far(side):
        return jnp.where(side == 0, z - 2, z + 2)

    upstream = [last - z, z]
    downstream = [z, last - z]
    at_end = (z == 0) | (z == last)
    near = jnp.where(z <= last - z, 0, 1)
    base = near * half
    inward = jnp.where(near == 0, z + 1, z - 1)
    at_owner = [(z == n) | (z == last - n) for n in insets]

    def depth_of(c):
        return sum(jnp.where(c // each == a, n, 0) for a, n in enumerate(insets) if n) + jnp.int32(0)

    def skip_of(c):
        return functools.reduce(jnp.logical_or, [c // each == a for a in range(half) if skips[a]], jnp.bool_(False))

    def chain_copy(side, c, hop=to_next):
        return remote(
            leaving.at[side, c], arrived.at[side, c], chain_send.at[side, c // each], chain_recv.at[side, c], {"vec": hop(side)}
        )

    def cross_copy(side, c, hop=to_next):
        return remote(
            leaving.at[side, c], crossed.at[c], chain_send.at[side, c // each], cross_recv.at[c // (2 * each) * each + c % each], {"vec": hop(side), "orb": 1 - o}
        )

    def raw_copy(side, c):
        return remote(
            leaving.at[side, c], back.at[o, c], chain_send.at[side, c // each], back_recv.at[o, c // (2 * each)],
            {"vec": to_next(side), "orb": (c // each) % 2},
        )

    def swap_copy(c):
        return remote(leaving.at[near, c], given.at[c], swap_send.at[c // (2 * each)], swap_recv.at[c // (2 * each)], {"orb": 1 - o})

    def extra_copy(side):
        return remote(
            extra_out.at[side], extra_in.at[side], extra_send.at[side], extra_recv.at[side], {"vec": to_next(side)}
        )

    def back_copy(c):
        return remote(
            leaving.at[near, c], back.at[o, c], chain_send.at[near, c // each], back_recv.at[o, c // (2 * each)],
            {"vec": inward, "orb": (c // each) % 2},
        )

    def part_of(side, c):
        at = c % each
        return partial[side * half + c // each, at // SUB, pl.ds(pl.multiple_of((at % SUB) * piece, piece), piece), :]

    def chain_step(t, carry):
        for turn in range(2):
            side = jnp.where(z <= last - z, 1 - turn, turn)
            before = jnp.where(side == 0, last - z, z)
            after = last - before
            c = t - SKEW * before
            head = before == 0
            togo = after - depth_of(c)
            skip = skip_of(c)

            @pl.when((c >= 0) & (c < chunks) & ((togo > 1) | ((togo == 1) & jnp.logical_not(skip))))
            def _():
                own = part_of(side, c)
                here = (c // each) % 2 == o

                @pl.when(head)
                def _():
                    leaving[side, c] = own.astype(BF16)

                @pl.when(jnp.logical_not(head))
                def _():
                    chain_copy(side, c).wait_recv()
                    leaving[side, c] = (own + arrived[side, c].astype(F32)).astype(BF16)

                jump = skip & (togo == 2)

                @pl.when(jnp.logical_not(jump) & ((togo > 1) | here))
                def _():
                    chain_copy(side, c).start()

                @pl.when((togo == 1) & jnp.logical_not(here))
                def _():
                    cross_copy(side, c).start()

                @pl.when(jump & here)
                def _():
                    chain_copy(side, c, to_far).start()

                @pl.when(jump & jnp.logical_not(here))
                def _():
                    cross_copy(side, c, to_far).start()

            @pl.when((c == 0) & (after > 0))
            def _():
                @pl.when(head)
                def _():
                    extra_in[side] = jnp.zeros_like(extra_in[side])

                @pl.when(jnp.logical_not(head))
                def _():
                    extra_copy(side).wait_recv()

                extra_out[side, 0:local, :] = extra_in[side, 0:local, :] + factor
                extra_out[side, local:, :] = extra_in[side, local:, :] + edge_part
                extra_copy(side).start()

        return carry

    for side in range(2):
        @pl.when(downstream[side] == 1)
        def _():
            def raw_step(c, carry):
                leaving[side, c] = part_of(side, c).astype(BF16)
                raw_copy(side, c).start()
                return carry

            for a in range(half):
                if skips[a]:
                    lax.fori_loop(a * each, (a + 1) * each, raw_step, jnp.int32(0))

    lax.fori_loop(0, SKEW * (last - 1) + chunks, chain_step, jnp.int32(0))

    for hop in hops:
        copies_copy(hop, lax.rem(x + hop, width)).wait_recv()

    def stage_copy(hop, a):
        return remote(
            staged.at[hop, a], pool.at[x, a // 2, o], stage_send.at[hop, a], pool_recv.at[x, a // 2, o],
            {"walk": lax.rem(x + hop, width), "orb": a % 2},
        )

    def swap_core():
        return remote(edge.at[o], edge.at[o], edge_sems.at[0], edge_sems.at[1], {"orb": 1 - o})

    for a in range(half):
        @pl.when(at_owner[a])
        def _():
            for hop in range(width):
                source = copies[lax.rem(x + hop, width), base + a]
                held = walkers[source % local]
                if hop > 0:
                    staged[hop, a] = held
                    stage_copy(hop, a).start()
                else:
                    @pl.when(a % 2 == o)
                    def _():
                        pool[x, a // 2, o] = held

                    @pl.when(a % 2 != o)
                    def _():
                        staged[hop, a] = held
                        stage_copy(hop, a).start()

            @pl.when(a % 2 != o)
            def _():
                def give(c, carry):
                    leaving[near, c] = part_of(near, c).astype(BF16)
                    swap_copy(c).start()
                    return carry

                lax.fori_loop(a * each, (a + 1) * each, give, jnp.int32(0))

        if insets[a]:
            @pl.when(at_end)
            def _():
                def back_step(c, carry):
                    leaving[near, c] = part_of(near, c).astype(BF16)
                    back_copy(c).start()
                    return carry

                lax.fori_loop(a * each, (a + 1) * each, back_step, jnp.int32(0))

    for side in range(2):
        @pl.when(at_end & (near == side))
        def _():
            extra_copy(side).wait_recv()

    owning = functools.reduce(jnp.logical_or, at_owner)

    @pl.when(owning)
    def _():
        edge[o] = edge_part + extra_in[0, local:, :] + extra_in[1, local:, :]
        swap_core().start()
        swap_core().wait_recv()

    share = rows // PARTS
    short = last <= REACH
    plans = [
        tuple(n for n in PLANS[min(half - a, len(PLANS)) - 1] if -insets[a] <= n <= last - insets[a])
        if short else (1,) + (-1,) * insets[a] for a in range(half)
    ]

    def passes(a, away):
        if not short:
            return (away > 0) & (away < last - insets[a])
        gaps = [away == n for n in range(1, last - insets[a]) if n + 1 not in plans[a]]
        return functools.reduce(jnp.logical_or, gaps, jnp.bool_(False))

    def place(w, part):
        return gathered.at[w, pl.ds(part * share, share)]

    def away_z(n):
        return jnp.where(near == 0, z + n, z - n)

    def spread_copies(a):
        w = base + a
        targets = []
        for n in plans[a]:
            for core in (1 - a % 2, a % 2):
                targets.append((core, {"vec": away_z(n), "orb": core}))
        targets.append((1 - a % 2, {"orb": 1 - o}))
        return [
            remote(
                result.at[a // 2, core, pl.ds(part * share, share)], place(w, part),
                own_send.at[a // 2, n, part], slot_recv.at[w, part], where,
            )
            for n, (core, where) in enumerate(targets)
            for part in range(PARTS)
        ]

    upper = lax.broadcasted_iota(jnp.int32, (block, block), 0) < lax.broadcasted_iota(jnp.int32, (block, block), 1)
    level_mask = lax.broadcasted_iota(jnp.int32, (block, block), 0) == lax.broadcasted_iota(jnp.int32, (block, block), 1)

    def finish(a):
        w = base + a
        i = a // 2

        def put(r, c, value):
            full[columns(r), columns(c)] = value

        for hop in range(width):
            other = lax.rem(x + hop, width)
            for core in range(2):
                arrival = remote(
                    staged.at[0, 0], pool.at[other, i, core], stage_send.at[0, 0], pool_recv.at[other, i, core],
                    {"walk": other, "orb": core},
                )
                if hop > 0:
                    arrival.wait_recv()
                else:
                    @pl.when(core != o)
                    def _():
                        arrival.wait_recv()
        column = copies[x, w] // local
        for core in range(2):
            start = pool[0, i, core]
            for other in hops:
                start = jnp.where(column == other, pool[other, i, core], start)
            terms[0, :, core * rows:(core + 1) * rows] = start.T
        whole = pl.ds(a * each, each)
        remote(leaving.at[near, whole], given.at[whole], swap_send.at[i], swap_recv.at[i], {"orb": 1 - o}).wait_recv()
        if insets[a] or skips[a]:
            for core in range(2):
                remote(
                    leaving.at[near, whole], back.at[core, whole], chain_send.at[near, a], back_recv.at[core, i],
                    {"vec": inward, "orb": core},
                ).wait_recv()
        for n in range(BLOCKS):
            first_c = a * each + n * SUB
            for c in range(first_c, first_c + SUB):
                remote(
                    leaving.at[near, c], arrived.at[near, c], chain_send.at[near, c // each], chain_recv.at[near, c], {"vec": inward}
                ).wait_recv()
                remote(
                    leaving.at[near, c], crossed.at[c], chain_send.at[near, c // each], cross_recv.at[c // (2 * each) * each + c % each],
                    {"vec": inward, "orb": 1 - o},
                ).wait_recv()
            run = pl.ds(first_c, SUB)
            kept = partial[w, n] + arrived[near, run].reshape(block, block).astype(F32)
            taken = given[run].reshape(block, block).astype(F32) + crossed[run].reshape(block, block).astype(F32)
            if insets[a] or skips[a]:
                kept = kept + back[o, run].reshape(block, block).astype(F32)
                taken = taken + back[1 - o, run].reshape(block, block).astype(F32)
            for core, value in ((o, kept), (1 - o, taken)):
                if n == 0:
                    flipped = value.T
                    line = edge[core, pl.ds(w, 1), :]
                    put(2 * core, 2 * core, jnp.where(upper | level_mask, value, flipped).astype(BF16))
                    low = jnp.where(level_mask, jnp.broadcast_to(line, (block, block)), jnp.where(upper, flipped, value))
                    put(2 * core + 1, 2 * core + 1, low.astype(BF16))
                else:
                    r, k = ((2 * core, 1), (2 * core, 2 + core), (2 * core + 1, 3 * (1 - core)))[n - 1]
                    value = value.astype(BF16)
                    put(r, k, value)
                    put(k, r, value.T)

        for degree in range(1, ORDER + 1):
            fresh = (jnp.dot(terms[degree - 1], full[...], preferred_element_type=F32) * (1.0 / degree)).astype(BF16)
            terms[degree] = fresh
        running = terms[0].astype(F32)
        for degree in range(1, ORDER + 1):
            running = running + terms[degree].astype(F32)
        result[i] = running.astype(BF16).T.reshape(2, rows, electrons)
        for copy in spread_copies(a):
            copy.start()
        settle = pltpu.make_async_copy(result.at[i, o], gathered.at[w], write_sems.at[i])
        settle.start()

    for a in range(half):
        @pl.when(at_owner[a] & (a % 2 == o))
        def _():
            finish(a)

    new_log = old_log + factor + extra_in[0, 0:local, :] + extra_in[1, 0:local, :]
    out_log[...] = new_log

    def onward(w, part, hop_to):
        spot = place(w, part)
        return remote(spot, spot, next_send.at[w, part], slot_recv.at[w, part], {"vec": hop_to})

    def route(side, a):
        w = side * half + a
        away = jnp.where(side == 0, z, last - z) - insets[a]
        hop_to = jnp.where(side == 0, z + 1, z - 1)
        return w, away, hop_to

    for a in range(half):
        for side in (near, 1 - near):
            w, away, hop_to = route(side, a)

            @pl.when(passes(a, away))
            def _():
                for part in range(PARTS):
                    onward(w, part, hop_to).wait_recv()
                    onward(w, part, hop_to).start()

    for copy in bias_copies:
        copy.wait_send()
    for hop in hops:
        facts_copy(hop, x).wait_send()
        copies_copy(hop, x).wait_send()

    def sent(side, a):
        whole = pl.ds(a * each, each)
        return remote(
            leaving.at[side, whole], arrived.at[side, whole], chain_send.at[side, a], chain_recv.at[side, a], {"orb": 1 - o}
        )

    for side in range(2):
        for a in range(half):
            @pl.when(downstream[side] - insets[a] != 0)
            def _():
                sent(side, a).wait_send()

    for side in range(2):
        @pl.when(downstream[side] > 0)
        def _():
            extra_copy(side).wait_send()

    @pl.when(owning)
    def _():
        swap_core().wait_send()

    for a in range(half):
        @pl.when(at_owner[a])
        def _():
            for hop in hops:
                stage_copy(hop, a).wait_send()

            @pl.when(a % 2 != o)
            def _():
                stage_copy(0, a).wait_send()

                whole = pl.ds(a * each, each)
                remote(
                    leaving.at[near, whole], given.at[whole], swap_send.at[a // 2], swap_recv.at[a // 2], {"orb": 1 - o}
                ).wait_send()

    for a in range(half):
        for side in (near, 1 - near):
            w, away, hop_to = route(side, a)

            @pl.when(((away != 0) | (o != a % 2)) & jnp.logical_not(passes(a, away)))
            def _():
                for part in range(PARTS):
                    onward(w, part, hop_to).wait_recv()

    for a in range(half):
        @pl.when(at_owner[a] & (a % 2 == o))
        def _():
            for copy in spread_copies(a):
                copy.wait_send()
            pltpu.make_async_copy(result.at[a // 2, o], gathered.at[base + a], write_sems.at[a // 2]).wait()

    for a in range(half):
        for side in range(2):
            w, away, hop_to = route(side, a)

            @pl.when(passes(a, away))
            def _():
                for part in range(PARTS):
                    onward(w, part, hop_to).wait_send()


def per_device(depth, width, walkers, inv_intersection, trial, vectors, aux_field, log_weight, copy_list):
    local, rows, electrons = walkers.shape
    count, _, orbitals = vectors.shape
    half = local // 2
    block = orbitals // 4
    span = 2 * block // count
    wide = count * span
    piece = block // SUB
    chunks = half * BLOCKS * SUB
    mine = half // 2
    lanes = 128
    reach = max(max(depth - 1, 1) if depth - 1 <= REACH else 1, 2)
    dma = pltpu.SemaphoreType.DMA
    anywhere = pl.BlockSpec(memory_space=pl.ANY)
    out, out_log = pl.pallas_call(
        functools.partial(kernel, depth, width),
        out_shape=(
            pltpu.VMEM(walkers.shape, BF16),
            pltpu.VMEM((local, 128), F32),
        ),
        in_specs=[anywhere] * 7,
        out_specs=(anywhere, pl.BlockSpec(memory_space=pltpu.VMEM)),
        scratch_shapes=[
            pltpu.VMEM(walkers.shape, BF16),
            pltpu.VMEM(inv_intersection.shape, BF16),
            pltpu.VMEM(trial.shape, BF16),
            pltpu.VMEM(vectors.shape, BF16),
            pltpu.VMEM(aux_field.shape, F32),
            pltpu.SMEM((local,), F32),
            pltpu.SMEM((width, local), jnp.int32),
            pltpu.VMEM((local, rows, electrons), BF16),
            pltpu.VMEM((count, rows, electrons), BF16),
            pltpu.VMEM((block // span, wide, BLOCKS * block), BF16),
            pltpu.VMEM((wide, block), BF16),
            pltpu.VMEM((2, width, local, wide), F32),
            pltpu.VMEM((width, local, lanes), F32),
            pltpu.VMEM((local, lanes), F32),
            pltpu.VMEM((local, wide), F32),
            pltpu.VMEM((local, BLOCKS, block, block), F32),
            pltpu.VMEM((2, chunks, piece, block), BF16),
            pltpu.VMEM((2, chunks, piece, block), BF16),
            pltpu.VMEM((chunks, piece, block), BF16),
            pltpu.VMEM((chunks, piece, block), BF16),
            pltpu.VMEM((2, chunks, piece, block), BF16),
            pltpu.VMEM((2, 2 * local, lanes), F32),
            pltpu.VMEM((2, 2 * local, lanes), F32),
            pltpu.VMEM((2, local, lanes), F32),
            pltpu.VMEM((width, half, rows, electrons), BF16),
            pltpu.VMEM((width, mine, 2, rows, electrons), BF16),
            pltpu.VMEM((orbitals, orbitals), BF16),
            pltpu.VMEM((ORDER + 1, electrons, orbitals), BF16),
            pltpu.VMEM((mine, 2, rows, electrons), BF16),
            dma((6 + LOADS,)),
            dma((width,)),
            dma((width,)),
            dma((width,)),
            dma((width,)),
            dma((2 * width,)),
            dma((2, width)),
            dma((2, half)),
            dma((2, chunks)),
            dma((chunks // 2,)),
            dma((2, mine)),
            dma((mine,)),
            dma((mine,)),
            dma((2,)),
            dma((2,)),
            dma((2,)),
            dma((width, half)),
            dma((width, mine, 2)),
            dma((mine, 2 * reach + 1, PARTS)),
            dma((local, PARTS)),
            dma((local, PARTS)),
            dma((mine,)),
        ],
        compiler_params=pltpu.CompilerParams(collective_id=0, has_side_effects=True),
    )(walkers, inv_intersection, trial, vectors, aux_field, log_weight, copy_list)

    def settle(out_ref, log_ref, o1, o2, flat, sems):
        c1 = pltpu.make_async_copy(out_ref, o1, sems.at[0])
        c1.start()
        for s in range(local):
            flat[s] = jnp.max(log_ref[s:s + 1, :])
        c2 = pltpu.make_async_copy(flat, o2, sems.at[1])
        c2.start()
        c1.wait()
        c2.wait()

    return pl.pallas_call(
        settle,
        out_shape=(jax.ShapeDtypeStruct(walkers.shape, BF16), jax.ShapeDtypeStruct((local,), F32)),
        in_specs=[pl.BlockSpec(memory_space=pltpu.VMEM)] * 2,
        out_specs=(anywhere, anywhere),
        scratch_shapes=[pltpu.SMEM((local,), F32), dma((2,))],
    )(pltpu.with_memory_space_constraint(out, pltpu.VMEM), pltpu.with_memory_space_constraint(out_log, pltpu.VMEM))


def solution(mesh):
    depth, width = mesh.shape["vec"], mesh.shape["walk"]
    assert mesh.shape["orb"] == 2 and depth > 1
    return jax.shard_map(
        functools.partial(per_device, depth, width),
        mesh=mesh,
        in_specs=(
            P(("grp", "walk"), "orb", None),
            P(("grp", "walk"), None, None),
            P(),
            P("vec", "orb", None),
            P(("grp", "walk"), "vec"),
            P(("grp", "walk")),
            P(("grp", "walk")),
        ),
        out_specs=(P(("grp", "walk"), "orb", None), P(("grp", "walk"))),
        check_vma=False,
    )
```

```python
import functools
import math

import jax
import jax.numpy as jnp
from jax import lax
from jax.experimental import pallas as pl
from jax.experimental.pallas import tpu as pltpu
from jax.sharding import PartitionSpec as P

ORDER = 6
BLOCKS = 4
SUB = 1
SKEW = 4
EARLY = 1
PARTS = 1
LOADS = 2
REACH = 3
PLANS = ((2, -1, 1), (3, 2, 1), (3, 2, 1), (2, 1))
MESH = pl.DeviceIdType.MESH
F32 = jnp.float32
BF16 = jnp.bfloat16

step_root = math.sqrt(0.08)


def remote(src, dst, send, recv, where):
    return pltpu.make_async_remote_copy(
        src_ref=src, dst_ref=dst, send_sem=send, recv_sem=recv, device_id=where, device_id_type=MESH
    )


def kernel(
    depth, width,
    walkers_in, inverse_in, trial_in, vectors_in, aux_in, log_in, copies_in,
    out, out_log,
    walkers, inverse, trial, vectors, aux, log_weight, copies,
    green, mixed, strips, level, bias_all, facts, known, picked, partial, leaving, arrived, given, crossed,
    back, extra_in, extra_out, edge, staged, pool, full, terms, result,
    load_sems, copies_send, copies_recv, facts_send, facts_recv, bias_send, bias_recv,
    chain_send, chain_recv, cross_recv, back_recv, swap_send, swap_recv, extra_send, extra_recv, edge_sems,
    stage_send, pool_recv, own_send, next_send, slot_recv, write_sems,
):
    gathered = out
    z = lax.axis_index("vec")
    x = lax.axis_index("walk")
    o = lax.axis_index("orb")
    last = depth - 1
    local, rows, electrons = walkers.shape
    count, _, orbitals = vectors.shape
    half = local // 2
    block = orbitals // 4
    span = 2 * block // count
    wide = count * span
    piece = block // SUB
    each = BLOCKS * SUB
    chunks = half * each
    mine = half // 2
    lanes = extra_in.shape[2]
    insets = [1 if a == half - 1 and last >= REACH else 0 for a in range(half)]
    hops = range(1, width)

    barrier = pltpu.get_barrier_semaphore()

    def greet(where):
        pl.semaphore_signal(barrier, inc=1, device_id=where, device_id_type=MESH)

    greet({"orb": 1 - o})
    for hop in hops:
        for core in range(2):
            greet({"walk": lax.rem(x + hop, width), "orb": core})

    @pl.when(z > 0)
    def _():
        for core in range(2):
            greet({"vec": z - 1, "orb": core})

    @pl.when(z < last)
    def _():
        for core in range(2):
            greet({"vec": z + 1, "orb": core})

    batch = count // LOADS
    pairs = [(trial_in, trial)]
    for n in range(LOADS):
        group = pl.ds(n * batch, batch)
        pairs.append((vectors_in.at[group], vectors.at[group]))
    pairs += [
        (inverse_in, inverse), (walkers_in, walkers), (copies_in, copies.at[x]), (log_in, log_weight), (aux_in, aux),
    ]
    loads = [pltpu.make_async_copy(src, dst, load_sems.at[n]) for n, (src, dst) in enumerate(pairs)]
    for load in loads:
        load.start()

    loads[0].wait()
    for n in range(LOADS):
        loads[1 + n].wait()
        for g in range(n * batch, (n + 1) * batch):
            mixed[g] = jnp.dot(vectors[g], trial[...], preferred_element_type=F32).astype(BF16)
    for load in loads[1 + LOADS:]:
        load.wait()
    for w in range(local):
        green[w] = jnp.dot(walkers[w], inverse[w], preferred_element_type=F32).astype(BF16)
    walker_id = lax.broadcasted_iota(jnp.int32, (local, lanes), 0)
    weights = jnp.zeros((local, lanes), F32)
    for w in range(local):
        weights = jnp.where(walker_id == w, log_weight[w], weights)
    facts[x] = weights
    facts[x, :, 0:count] = aux[...]
    left = [green[:, j * span:(j + 1) * span, :].reshape(local * span, electrons) for j in range(rows // span)]
    right = [mixed[:, j * span:(j + 1) * span, :].reshape(wide, electrons) for j in range(rows // span)]
    gram = lax.dot_general(
        jnp.concatenate(left, axis=1), jnp.concatenate(right, axis=1), (((1,), (1,)), ((), ())), preferred_element_type=F32
    )
    row_id = lax.broadcasted_iota(jnp.int32, (local * span, wide), 0)
    col_id = lax.broadcasted_iota(jnp.int32, (local * span, wide), 1)
    same = row_id % span == col_id % span
    folded = jnp.sum(jnp.where(same, gram, 0.0).reshape(local, span, wide), axis=1)
    lane_id = lax.broadcasted_iota(jnp.int32, (local, wide), 1)
    step = 1
    while step < span:
        low = lane_id % (2 * step) < step
        folded = folded + jnp.where(low, pltpu.roll(folded, wide - step, 1), pltpu.roll(folded, step, 1))
        step *= 2
    lane = lax.broadcasted_iota(jnp.int32, (local, lanes), 1) % span
    fold = span // 2
    bias_all[o, x] = jnp.where(lane < fold, folded[:, :lanes], folded[:, lanes:])

    sides = jnp.where(z > 0, 2, 0) + jnp.where(z < last, 2, 0)
    pl.semaphore_wait(barrier, 1 + 2 * (width - 1) + sides)

    bias_peers = [{"walk": lax.rem(x + hop, width), "orb": core} for hop in hops for core in range(2)] + [{"orb": 1 - o}]
    bias_copies = [
        remote(bias_all.at[o, x], bias_all.at[o, x], bias_send.at[n], bias_recv.at[o, x], where)
        for n, where in enumerate(bias_peers)
    ]
    def facts_copy(hop, owner):
        return remote(
            facts.at[owner], facts.at[owner], facts_send.at[hop], facts_recv.at[owner], {"walk": lax.rem(x + hop, width)}
        )

    def copies_copy(hop, owner):
        return remote(
            copies.at[owner], copies.at[owner], copies_send.at[hop], copies_recv.at[owner],
            {"walk": lax.rem(x + hop, width)},
        )

    for copy in bias_copies:
        copy.start()
    for hop in hops:
        facts_copy(hop, x).start()
        copies_copy(hop, x).start()

    chunk_row = lax.broadcasted_iota(jnp.int32, (count, span, block), 1)
    chunk_col = lax.broadcasted_iota(jnp.int32, (count, span, block), 2)
    crossing = jnp.zeros((count, span, block), F32)

    def columns(n):
        return pl.ds(pl.multiple_of(n * block, block), block)

    for j in range(block // span):
        here = slice(j * span, (j + 1) * span)
        below = slice(block + j * span, block + (j + 1) * span)
        first = vectors[:, here, columns(2 * o)].astype(F32)
        second = vectors[:, below, columns(1 + 2 * o)].astype(F32)
        crossing = crossing + jnp.where(chunk_row + j * span == chunk_col, second, 0.0)
        joined = jnp.where(chunk_row + j * span <= chunk_col, first, second).astype(BF16)
        strips[j, :, 0:block] = joined.reshape(wide, block)
        strips[j, :, block:2 * block] = vectors[:, here, block:2 * block].reshape(wide, block)
        strips[j, :, 2 * block:3 * block] = vectors[:, here, columns(2 + o)].reshape(wide, block)
        strips[j, :, 3 * block:] = vectors[:, below, columns(3 * (1 - o))].reshape(wide, block)
    level[...] = crossing.reshape(wide, block).astype(BF16)

    for hop in hops:
        facts_copy(hop, lax.rem(x + hop, width)).wait_recv()
    sources = [(copies[x, s] // local, pl.ds(copies[x, s] % local, 1)) for s in range(local)]
    for s, (column, row) in enumerate(sources):
        known[s:s + 1, :] = facts[column, row, :]
    pick_row = lax.broadcasted_iota(jnp.int32, (count, wide), 0)
    pick_col = lax.broadcasted_iota(jnp.int32, (count, wide), 1)
    pick = jnp.where(pick_row == pick_col // span, 1.0, 0.0).astype(F32)
    drawn = jnp.dot(known[:, 0:count], pick, precision=lax.Precision.HIGHEST, preferred_element_type=F32)
    old_log = jnp.broadcast_to(known[:, count:count + 1], (local, lanes))

    for hop in hops:
        other = lax.rem(x + hop, width)
        for core in range(2):
            remote(
                bias_all.at[core, other], bias_all.at[core, other], bias_send.at[0], bias_recv.at[core, other], {"walk": other}
            ).wait_recv()
    remote(bias_all.at[1 - o, x], bias_all.at[1 - o, x], bias_send.at[0], bias_recv.at[1 - o, x], {"orb": 1 - o}).wait_recv()

    for s, (column, row) in enumerate(sources):
        picked[s:s + 1, :] = bias_all[0, column, row, :] + bias_all[1, column, row, :]
    both = picked[...]
    bias = jnp.concatenate(
        [jnp.where(lane < fold, both, pltpu.roll(both, fold, 1)), jnp.where(lane < fold, pltpu.roll(both, lanes - fold, 1), both)],
        axis=1,
    )
    shift = -step_root * bias
    field = drawn - shift
    factor = jnp.sum(drawn * shift - 0.5 * shift * shift, axis=1, keepdims=True) * (1.0 / span)
    factor = jnp.broadcast_to(factor, (local, lanes))
    weighted = (field * step_root).astype(BF16)
    spread = jnp.broadcast_to(weighted.astype(F32)[:, None, :], (local, span, wide)).reshape(local * span, wide)
    kron = jnp.where(same, spread, 0.0).astype(BF16)

    for j in range(block // span):
        summed = jnp.dot(kron, strips[j], preferred_element_type=F32)
        for n in range(BLOCKS):
            partial[:, n, j * span:(j + 1) * span, :] = summed[:, n * block:(n + 1) * block].reshape(local, span, block)
    edge_part = jnp.dot(weighted, level[...], preferred_element_type=F32)

    def to_next(side):
        return jnp.where(side == 0, z - 1, z + 1)

    upstream = [last - z, z]
    downstream = [z, last - z]
    at_end = (z == 0) | (z == last)
    near = jnp.where(z <= last - z, 0, 1)
    base = near * half
    inward = jnp.where(near == 0, z + 1, z - 1)
    at_owner = [(z == n) | (z == last - n) for n in insets]

    def depth_of(c):
        return sum(jnp.where(c // each == a, n, 0) for a, n in enumerate(insets) if n) + jnp.int32(0)

    def chain_copy(side, c):
        return remote(
            leaving.at[side, c], arrived.at[side, c], chain_send.at[side, c // each], chain_recv.at[side, c], {"vec": to_next(side)}
        )

    def cross_copy(side, c):
        return remote(
            leaving.at[side, c], crossed.at[c], chain_send.at[side, c // each], cross_recv.at[c // (2 * each) * each + c % each], {"vec": to_next(side), "orb": 1 - o}
        )

    def swap_copy(c):
        return remote(leaving.at[near, c], given.at[c], swap_send.at[c // (2 * each)], swap_recv.at[c // (2 * each)], {"orb": 1 - o})

    def extra_copy(side):
        return remote(
            extra_out.at[side], extra_in.at[side], extra_send.at[side], extra_recv.at[side], {"vec": to_next(side)}
        )

    def back_copy(c):
        return remote(
            leaving.at[near, c], back.at[o, c], chain_send.at[near, c // each], back_recv.at[o, c // (2 * each)],
            {"vec": inward, "orb": (c // each) % 2},
        )

    def part_of(side, c):
        at = c % each
        return partial[side * half + c // each, at // SUB, pl.ds(pl.multiple_of((at % SUB) * piece, piece), piece), :]

    def chain_step(t, carry):
        for turn in range(2):
            side = jnp.where(z <= last - z, 1 - turn, turn)
            before = jnp.where(side == 0, last - z, z)
            after = last - before
            c = t - SKEW * before
            head = before == 0
            togo = after - depth_of(c)

            @pl.when((c >= 0) & (c < chunks) & (togo > 0))
            def _():
                own = part_of(side, c)
                here = (c // each) % 2 == o

                @pl.when(head)
                def _():
                    leaving[side, c] = own.astype(BF16)

                @pl.when(jnp.logical_not(head))
                def _():
                    chain_copy(side, c).wait_recv()
                    leaving[side, c] = (own + arrived[side, c].astype(F32)).astype(BF16)

                @pl.when((togo > 1) | here)
                def _():
                    chain_copy(side, c).start()

                @pl.when((togo == 1) & jnp.logical_not(here))
                def _():
                    cross_copy(side, c).start()

            @pl.when((c == 0) & (after > 0))
            def _():
                @pl.when(head)
                def _():
                    extra_in[side] = jnp.zeros_like(extra_in[side])

                @pl.when(jnp.logical_not(head))
                def _():
                    extra_copy(side).wait_recv()

                extra_out[side, 0:local, :] = extra_in[side, 0:local, :] + factor
                extra_out[side, local:, :] = extra_in[side, local:, :] + edge_part
                extra_copy(side).start()

        return carry

    lax.fori_loop(0, SKEW * (last - 1) + chunks, chain_step, jnp.int32(0))

    for hop in hops:
        copies_copy(hop, lax.rem(x + hop, width)).wait_recv()

    def stage_copy(hop, a):
        return remote(
            staged.at[hop, a], pool.at[x, a // 2, o], stage_send.at[a], pool_recv.at[a // 2],
            {"walk": lax.rem(x + hop, width), "orb": a % 2},
        )

    def swap_core():
        return remote(edge.at[o], edge.at[o], edge_sems.at[0], edge_sems.at[1], {"orb": 1 - o})

    for a in range(half):
        @pl.when(at_owner[a])
        def _():
            for hop in range(width):
                source = copies[lax.rem(x + hop, width), base + a]
                held = walkers[source % local]
                if hop > 0:
                    staged[hop, a] = held
                    stage_copy(hop, a).start()
                else:
                    @pl.when(a % 2 == o)
                    def _():
                        pool[x, a // 2, o] = held

                    @pl.when(a % 2 != o)
                    def _():
                        staged[hop, a] = held
                        stage_copy(hop, a).start()

            @pl.when(a % 2 != o)
            def _():
                def give(c, carry):
                    leaving[near, c] = part_of(near, c).astype(BF16)
                    swap_copy(c).start()
                    return carry

                lax.fori_loop(a * each, (a + 1) * each, give, jnp.int32(0))

        if insets[a]:
            @pl.when(at_end)
            def _():
                def back_step(c, carry):
                    leaving[near, c] = part_of(near, c).astype(BF16)
                    back_copy(c).start()
                    return carry

                lax.fori_loop(a * each, (a + 1) * each, back_step, jnp.int32(0))

    for side in range(2):
        @pl.when(at_end & (near == side))
        def _():
            extra_copy(side).wait_recv()

    owning = functools.reduce(jnp.logical_or, at_owner)

    @pl.when(owning)
    def _():
        edge[o] = edge_part + extra_in[0, local:, :] + extra_in[1, local:, :]
        swap_core().start()
        swap_core().wait_recv()

    share = rows // PARTS
    short = last <= REACH
    plans = [
        tuple(n for n in PLANS[min(half - a, len(PLANS)) - 1] if -insets[a] <= n <= last - insets[a])
        if short else (1,) + (-1,) * insets[a] for a in range(half)
    ]

    def passes(a, away):
        if not short:
            return (away > 0) & (away < last - insets[a])
        gaps = [away == n for n in range(1, last - insets[a]) if n + 1 not in plans[a]]
        return functools.reduce(jnp.logical_or, gaps, jnp.bool_(False))

    def place(w, part):
        return gathered.at[w, pl.ds(part * share, share)]

    def away_z(n):
        return jnp.where(near == 0, z + n, z - n)

    def spread_copies(a):
        w = base + a
        targets = []
        for n in plans[a]:
            for core in (1 - a % 2, a % 2):
                targets.append((core, {"vec": away_z(n), "orb": core}))
        targets.append((1 - a % 2, {"orb": 1 - o}))
        return [
            remote(
                result.at[a // 2, core, pl.ds(part * share, share)], place(w, part),
                own_send.at[a // 2], slot_recv.at[w, part], where,
            )
            for n, (core, where) in enumerate(targets)
            for part in range(PARTS)
        ]

    upper = lax.broadcasted_iota(jnp.int32, (block, block), 0) < lax.broadcasted_iota(jnp.int32, (block, block), 1)
    level_mask = lax.broadcasted_iota(jnp.int32, (block, block), 0) == lax.broadcasted_iota(jnp.int32, (block, block), 1)

    def finish(a):
        w = base + a
        i = a // 2

        def put(r, c, value):
            full[columns(r), columns(c)] = value

        come = gathered.at[pl.ds(0, 2 * width - 1)]
        remote(come, come, stage_send.at[0], pool_recv.at[i], {"orb": 1 - o}).wait_recv()
        column = copies[x, w] // local
        for core in range(2):
            start = pool[0, i, core]
            for other in hops:
                start = jnp.where(column == other, pool[other, i, core], start)
            terms[0, :, core * rows:(core + 1) * rows] = start.T
        whole = pl.ds(a * each, each)
        remote(leaving.at[near, whole], given.at[whole], swap_send.at[i], swap_recv.at[i], {"orb": 1 - o}).wait_recv()
        if insets[a]:
            for core in range(2):
                remote(
                    leaving.at[near, whole], back.at[core, whole], chain_send.at[near, a], back_recv.at[core, i],
                    {"vec": inward, "orb": core},
                ).wait_recv()
        for n in range(BLOCKS):
            first_c = a * each + n * SUB
            for c in range(first_c, first_c + SUB):
                remote(
                    leaving.at[near, c], arrived.at[near, c], chain_send.at[near, c // each], chain_recv.at[near, c], {"vec": inward}
                ).wait_recv()
                remote(
                    leaving.at[near, c], crossed.at[c], chain_send.at[near, c // each], cross_recv.at[c // (2 * each) * each + c % each],
                    {"vec": inward, "orb": 1 - o},
                ).wait_recv()
            run = pl.ds(first_c, SUB)
            kept = partial[w, n] + arrived[near, run].reshape(block, block).astype(F32)
            taken = given[run].reshape(block, block).astype(F32) + crossed[run].reshape(block, block).astype(F32)
            if insets[a]:
                kept = kept + back[o, run].reshape(block, block).astype(F32)
                taken = taken + back[1 - o, run].reshape(block, block).astype(F32)
            for core, value in ((o, kept), (1 - o, taken)):
                if n == 0:
                    flipped = value.T
                    line = edge[core, pl.ds(w, 1), :]
                    put(2 * core, 2 * core, jnp.where(upper | level_mask, value, flipped).astype(BF16))
                    low = jnp.where(level_mask, jnp.broadcast_to(line, (block, block)), jnp.where(upper, flipped, value))
                    put(2 * core + 1, 2 * core + 1, low.astype(BF16))
                else:
                    r, k = ((2 * core, 1), (2 * core, 2 + core), (2 * core + 1, 3 * (1 - core)))[n - 1]
                    value = value.astype(BF16)
                    put(r, k, value)
                    put(k, r, value.T)

        for degree in range(1, ORDER + 1):
            fresh = (jnp.dot(terms[degree - 1], full[...], preferred_element_type=F32) * (1.0 / degree)).astype(BF16)
            terms[degree] = fresh
        running = terms[0].astype(F32)
        for degree in range(1, ORDER + 1):
            running = running + terms[degree].astype(F32)
        result[i] = running.astype(BF16).T.reshape(2, rows, electrons)
        for copy in spread_copies(a):
            copy.start()
        settle = pltpu.make_async_copy(result.at[i, o], gathered.at[w], write_sems.at[i])
        settle.start()

    def onward(w, part, hop_to):
        spot = place(w, part)
        return remote(spot, spot, next_send.at[w, part], slot_recv.at[w, part], {"vec": hop_to})

    def route(side, a):
        w = side * half + a
        away = jnp.where(side == 0, z, last - z) - insets[a]
        hop_to = jnp.where(side == 0, z + 1, z - 1)
        return w, away, hop_to

    def forward(slots):
        for a in slots:
            for side in (near, 1 - near):
                w, away, hop_to = route(side, a)

                @pl.when(passes(a, away))
                def _():
                    for part in range(PARTS):
                        onward(w, part, hop_to).wait_recv()
                        onward(w, part, hop_to).start()

    early = [a for a in range(half) if short and a < EARLY]
    forward(early)
    for a in range(half):
        @pl.when(at_owner[a] & (a % 2 == o))
        def _():
            finish(a)

    new_log = old_log + factor + extra_in[0, 0:local, :] + extra_in[1, 0:local, :]
    out_log[...] = new_log

    forward([a for a in range(half) if a not in early])

    for copy in bias_copies:
        copy.wait_send()
    for hop in hops:
        facts_copy(hop, x).wait_send()
        copies_copy(hop, x).wait_send()

    def sent(side, a):
        whole = pl.ds(a * each, each)
        return remote(
            leaving.at[side, whole], arrived.at[side, whole], chain_send.at[side, a], chain_recv.at[side, a], {"orb": 1 - o}
        )

    for side in range(2):
        for a in range(half):
            @pl.when(downstream[side] - insets[a] != 0)
            def _():
                sent(side, a).wait_send()

    for side in range(2):
        @pl.when(downstream[side] > 0)
        def _():
            extra_copy(side).wait_send()

    @pl.when(owning)
    def _():
        swap_core().wait_send()

    for a in range(half):
        @pl.when(at_owner[a])
        def _():
            def moved(n):
                run = gathered.at[pl.ds(0, n)]
                return remote(run, run, stage_send.at[a], slot_recv.at[0, 0], {"orb": 1 - o})

            @pl.when(a % 2 == o)
            def _():
                moved(width - 1).wait_send()

            @pl.when(a % 2 != o)
            def _():
                moved(width).wait_send()

                whole = pl.ds(a * each, each)
                remote(
                    leaving.at[near, whole], given.at[whole], swap_send.at[a // 2], swap_recv.at[a // 2], {"orb": 1 - o}
                ).wait_send()

    for a in range(half):
        for side in (near, 1 - near):
            w, away, hop_to = route(side, a)

            @pl.when(((away != 0) | (o != a % 2)) & jnp.logical_not(passes(a, away)))
            def _():
                for part in range(PARTS):
                    onward(w, part, hop_to).wait_recv()

    for a in range(half):
        @pl.when(at_owner[a] & (a % 2 == o))
        def _():
            run = gathered.at[pl.ds(0, 2 * len(plans[a]) + 1)]
            remote(run, run, own_send.at[a // 2], slot_recv.at[0, 0], {"orb": 1 - o}).wait_send()
            pltpu.make_async_copy(result.at[a // 2, o], gathered.at[base + a], write_sems.at[a // 2]).wait()

    for a in range(half):
        for side in range(2):
            w, away, hop_to = route(side, a)

            @pl.when(passes(a, away))
            def _():
                for part in range(PARTS):
                    onward(w, part, hop_to).wait_send()


def per_device(depth, width, walkers, inv_intersection, trial, vectors, aux_field, log_weight, copy_list):
    local, rows, electrons = walkers.shape
    count, _, orbitals = vectors.shape
    half = local // 2
    block = orbitals // 4
    span = 2 * block // count
    wide = count * span
    piece = block // SUB
    chunks = half * BLOCKS * SUB
    mine = half // 2
    lanes = 128
    dma = pltpu.SemaphoreType.DMA
    anywhere = pl.BlockSpec(memory_space=pl.ANY)
    out, out_log = pl.pallas_call(
        functools.partial(kernel, depth, width),
        out_shape=(
            pltpu.VMEM(walkers.shape, BF16),
            pltpu.VMEM((local, 128), F32),
        ),
        in_specs=[anywhere] * 7,
        out_specs=(anywhere, pl.BlockSpec(memory_space=pltpu.VMEM)),
        scratch_shapes=[
            pltpu.VMEM(walkers.shape, BF16),
            pltpu.VMEM(inv_intersection.shape, BF16),
            pltpu.VMEM(trial.shape, BF16),
            pltpu.VMEM(vectors.shape, BF16),
            pltpu.VMEM(aux_field.shape, F32),
            pltpu.SMEM((local,), F32),
            pltpu.SMEM((width, local), jnp.int32),
            pltpu.VMEM((local, rows, electrons), BF16),
            pltpu.VMEM((count, rows, electrons), BF16),
            pltpu.VMEM((block // span, wide, BLOCKS * block), BF16),
            pltpu.VMEM((wide, block), BF16),
            pltpu.VMEM((2, width, local, lanes), F32),
            pltpu.VMEM((width, local, lanes), F32),
            pltpu.VMEM((local, lanes), F32),
            pltpu.VMEM((local, lanes), F32),
            pltpu.VMEM((local, BLOCKS, block, block), F32),
            pltpu.VMEM((2, chunks, piece, block), BF16),
            pltpu.VMEM((2, chunks, piece, block), BF16),
            pltpu.VMEM((chunks, piece, block), BF16),
            pltpu.VMEM((chunks, piece, block), BF16),
            pltpu.VMEM((2, chunks, piece, block), BF16),
            pltpu.VMEM((2, 2 * local, lanes), F32),
            pltpu.VMEM((2, 2 * local, lanes), F32),
            pltpu.VMEM((2, local, lanes), F32),
            pltpu.VMEM((width, half, rows, electrons), BF16),
            pltpu.VMEM((width, mine, 2, rows, electrons), BF16),
            pltpu.VMEM((orbitals, orbitals), BF16),
            pltpu.VMEM((ORDER + 1, electrons, orbitals), BF16),
            pltpu.VMEM((mine, 2, rows, electrons), BF16),
            dma((6 + LOADS,)),
            dma((width,)),
            dma((width,)),
            dma((width,)),
            dma((width,)),
            dma((2 * width,)),
            dma((2, width)),
            dma((2, half)),
            dma((2, chunks)),
            dma((chunks // 2,)),
            dma((2, mine)),
            dma((mine,)),
            dma((mine,)),
            dma((2,)),
            dma((2,)),
            dma((2,)),
            dma((half,)),
            dma((mine,)),
            dma((mine,)),
            dma((local, PARTS)),
            dma((local, PARTS)),
            dma((mine,)),
        ],
        compiler_params=pltpu.CompilerParams(collective_id=0, has_side_effects=True),
    )(walkers, inv_intersection, trial, vectors, aux_field, log_weight, copy_list)

    def settle(out_ref, log_ref, o1, o2, flat, sems):
        c1 = pltpu.make_async_copy(out_ref, o1, sems.at[0])
        c1.start()
        for s in range(local):
            flat[s] = jnp.max(log_ref[s:s + 1, :])
        c2 = pltpu.make_async_copy(flat, o2, sems.at[1])
        c2.start()
        c1.wait()
        c2.wait()

    return pl.pallas_call(
        settle,
        out_shape=(jax.ShapeDtypeStruct(walkers.shape, BF16), jax.ShapeDtypeStruct((local,), F32)),
        in_specs=[pl.BlockSpec(memory_space=pltpu.VMEM)] * 2,
        out_specs=(anywhere, anywhere),
        scratch_shapes=[pltpu.SMEM((local,), F32), dma((2,))],
    )(pltpu.with_memory_space_constraint(out, pltpu.VMEM), pltpu.with_memory_space_constraint(out_log, pltpu.VMEM))


def solution(mesh):
    depth, width = mesh.shape["vec"], mesh.shape["walk"]
    assert mesh.shape["orb"] == 2 and depth > 1
    return jax.shard_map(
        functools.partial(per_device, depth, width),
        mesh=mesh,
        in_specs=(
            P(("grp", "walk"), "orb", None),
            P(("grp", "walk"), None, None),
            P(),
            P("vec", "orb", None),
            P(("grp", "walk"), "vec"),
            P(("grp", "walk")),
            P(("grp", "walk")),
        ),
        out_specs=(P(("grp", "walk"), "orb", None), P(("grp", "walk"))),
        check_vma=False,
    )
```

```python
import functools
import math

import jax
import jax.numpy as jnp
from jax import lax
from jax.experimental import pallas as pl
from jax.experimental.pallas import tpu as pltpu
from jax.sharding import PartitionSpec as P

ORDER = 6
BLOCKS = 4
SUB = 1
SKEW = 4
EARLY = 1
PARTS = 1
LOADS = 2
REACH = 3
PLANS = ((2, -1, 1), (3, 2, 1), (3, 2, 1), (2, 1))
MESH = pl.DeviceIdType.MESH
F32 = jnp.float32
BF16 = jnp.bfloat16

step_root = math.sqrt(0.08)


def remote(src, dst, send, recv, where):
    return pltpu.make_async_remote_copy(
        src_ref=src, dst_ref=dst, send_sem=send, recv_sem=recv, device_id=where, device_id_type=MESH
    )


def kernel(
    depth, width,
    walkers_in, inverse_in, trial_in, vectors_in, aux_in, log_in, copies_in,
    out, out_log,
    walkers, inverse, trial, vectors, aux, log_weight, copies,
    green, mixed, strips, level, bias_all, facts, known, picked, partial, leaving, arrived, given, crossed,
    back, extra_in, extra_out, edge, staged, pool, full, terms, result,
    load_sems, copies_send, copies_recv, facts_send, facts_recv, bias_send, bias_recv,
    chain_send, chain_recv, cross_recv, back_recv, swap_send, swap_recv, extra_send, extra_recv, edge_sems,
    stage_send, pool_recv, own_send, next_send, slot_recv, write_sems,
):
    gathered = out
    z = lax.axis_index("vec")
    x = lax.axis_index("walk")
    o = lax.axis_index("orb")
    last = depth - 1
    local, rows, electrons = walkers.shape
    count, _, orbitals = vectors.shape
    half = local // 2
    block = orbitals // 4
    span = 2 * block // count
    wide = count * span
    piece = block // SUB
    each = BLOCKS * SUB
    chunks = half * each
    mine = half // 2
    lanes = extra_in.shape[2]
    insets = [1 if a == half - 1 and last >= REACH else 0 for a in range(half)]
    hops = range(1, width)

    barrier = pltpu.get_barrier_semaphore()

    def greet(where):
        pl.semaphore_signal(barrier, inc=1, device_id=where, device_id_type=MESH)

    greet({"orb": 1 - o})
    for hop in hops:
        for core in range(2):
            greet({"walk": lax.rem(x + hop, width), "orb": core})

    @pl.when(z > 0)
    def _():
        for core in range(2):
            greet({"vec": z - 1, "orb": core})

    @pl.when(z < last)
    def _():
        for core in range(2):
            greet({"vec": z + 1, "orb": core})

    batch = count // LOADS
    pairs = [(trial_in, trial)]
    for n in range(LOADS):
        group = pl.ds(n * batch, batch)
        pairs.append((vectors_in.at[group], vectors.at[group]))
    pairs += [
        (inverse_in, inverse), (walkers_in, walkers), (copies_in, copies.at[x]), (log_in, log_weight), (aux_in, aux),
    ]
    loads = [pltpu.make_async_copy(src, dst, load_sems.at[n]) for n, (src, dst) in enumerate(pairs)]
    for load in loads:
        load.start()

    loads[0].wait()
    for n in range(LOADS):
        loads[1 + n].wait()
        for g in range(n * batch, (n + 1) * batch):
            mixed[g] = jnp.dot(vectors[g], trial[...], preferred_element_type=F32).astype(BF16)
    for load in loads[1 + LOADS:]:
        load.wait()
    for w in range(local):
        green[w] = jnp.dot(walkers[w], inverse[w], preferred_element_type=F32).astype(BF16)
    walker_id = lax.broadcasted_iota(jnp.int32, (local, lanes), 0)
    weights = jnp.zeros((local, lanes), F32)
    for w in range(local):
        weights = jnp.where(walker_id == w, log_weight[w], weights)
    facts[x] = weights
    facts[x, :, 0:count] = aux[...]
    left = [green[:, j * span:(j + 1) * span, :].reshape(local * span, electrons) for j in range(rows // span)]
    right = [mixed[:, j * span:(j + 1) * span, :].reshape(wide, electrons) for j in range(rows // span)]
    gram = lax.dot_general(
        jnp.concatenate(left, axis=1), jnp.concatenate(right, axis=1), (((1,), (1,)), ((), ())), preferred_element_type=F32
    )
    row_id = lax.broadcasted_iota(jnp.int32, (local * span, wide), 0)
    col_id = lax.broadcasted_iota(jnp.int32, (local * span, wide), 1)
    same = row_id % span == col_id % span
    folded = jnp.sum(jnp.where(same, gram, 0.0).reshape(local, span, wide), axis=1)
    lane_id = lax.broadcasted_iota(jnp.int32, (local, wide), 1)
    step = 1
    while step < span:
        low = lane_id % (2 * step) < step
        folded = folded + jnp.where(low, pltpu.roll(folded, wide - step, 1), pltpu.roll(folded, step, 1))
        step *= 2
    lane = lax.broadcasted_iota(jnp.int32, (local, lanes), 1) % span
    fold = span // 2
    bias_all[o, x] = jnp.where(lane < fold, folded[:, :lanes], folded[:, lanes:])

    sides = jnp.where(z > 0, 2, 0) + jnp.where(z < last, 2, 0)
    pl.semaphore_wait(barrier, 1 + 2 * (width - 1) + sides)

    bias_peers = [{"walk": lax.rem(x + hop, width), "orb": core} for hop in hops for core in range(2)] + [{"orb": 1 - o}]
    bias_copies = [
        remote(bias_all.at[o, x], bias_all.at[o, x], bias_send.at[n], bias_recv.at[o, x], where)
        for n, where in enumerate(bias_peers)
    ]
    def facts_copy(hop, owner):
        return remote(
            facts.at[owner], facts.at[owner], facts_send.at[hop], facts_recv.at[owner], {"walk": lax.rem(x + hop, width)}
        )

    def copies_copy(hop, owner):
        return remote(
            copies.at[owner], copies.at[owner], copies_send.at[hop], copies_recv.at[owner],
            {"walk": lax.rem(x + hop, width)},
        )

    for copy in bias_copies:
        copy.start()
    for hop in hops:
        facts_copy(hop, x).start()
        copies_copy(hop, x).start()

    chunk_row = lax.broadcasted_iota(jnp.int32, (count, span, block), 1)
    chunk_col = lax.broadcasted_iota(jnp.int32, (count, span, block), 2)
    crossing = jnp.zeros((count, span, block), F32)

    def columns(n):
        return pl.ds(pl.multiple_of(n * block, block), block)

    for j in range(block // span):
        here = slice(j * span, (j + 1) * span)
        below = slice(block + j * span, block + (j + 1) * span)
        first = vectors[:, here, columns(2 * o)].astype(F32)
        second = vectors[:, below, columns(1 + 2 * o)].astype(F32)
        crossing = crossing + jnp.where(chunk_row + j * span == chunk_col, second, 0.0)
        joined = jnp.where(chunk_row + j * span <= chunk_col, first, second).astype(BF16)
        strips[j, :, 0:block] = joined.reshape(wide, block)
        strips[j, :, block:2 * block] = vectors[:, here, block:2 * block].reshape(wide, block)
        strips[j, :, 2 * block:3 * block] = vectors[:, here, columns(2 + o)].reshape(wide, block)
        strips[j, :, 3 * block:] = vectors[:, below, columns(3 * (1 - o))].reshape(wide, block)
    level[...] = crossing.reshape(wide, block).astype(BF16)

    for hop in hops:
        facts_copy(hop, lax.rem(x + hop, width)).wait_recv()
    sources = [(copies[x, s] // local, pl.ds(copies[x, s] % local, 1)) for s in range(local)]
    for s, (column, row) in enumerate(sources):
        known[s:s + 1, :] = facts[column, row, :]
    pick_row = lax.broadcasted_iota(jnp.int32, (count, wide), 0)
    pick_col = lax.broadcasted_iota(jnp.int32, (count, wide), 1)
    pick = jnp.where(pick_row == pick_col // span, 1.0, 0.0).astype(F32)
    drawn = jnp.dot(known[:, 0:count], pick, precision=lax.Precision.HIGHEST, preferred_element_type=F32)
    old_log = jnp.broadcast_to(known[:, count:count + 1], (local, lanes))

    for hop in hops:
        other = lax.rem(x + hop, width)
        for core in range(2):
            remote(
                bias_all.at[core, other], bias_all.at[core, other], bias_send.at[0], bias_recv.at[core, other], {"walk": other}
            ).wait_recv()
    remote(bias_all.at[1 - o, x], bias_all.at[1 - o, x], bias_send.at[0], bias_recv.at[1 - o, x], {"orb": 1 - o}).wait_recv()

    for s, (column, row) in enumerate(sources):
        picked[s:s + 1, :] = bias_all[0, column, row, :] + bias_all[1, column, row, :]
    both = picked[...]
    bias = jnp.concatenate(
        [jnp.where(lane < fold, both, pltpu.roll(both, fold, 1)), jnp.where(lane < fold, pltpu.roll(both, lanes - fold, 1), both)],
        axis=1,
    )
    shift = -step_root * bias
    field = drawn - shift
    factor = jnp.sum(drawn * shift - 0.5 * shift * shift, axis=1, keepdims=True) * (1.0 / span)
    factor = jnp.broadcast_to(factor, (local, lanes))
    weighted = (field * step_root).astype(BF16)
    spread = jnp.broadcast_to(weighted.astype(F32)[:, None, :], (local, span, wide)).reshape(local * span, wide)
    kron = jnp.where(same, spread, 0.0).astype(BF16)

    def to_next(side):
        return jnp.where(side == 0, z - 1, z + 1)

    upstream = [last - z, z]
    downstream = [z, last - z]
    at_end = (z == 0) | (z == last)
    near = jnp.where(z <= last - z, 0, 1)
    base = near * half
    inward = jnp.where(near == 0, z + 1, z - 1)
    at_owner = [(z == n) | (z == last - n) for n in insets]

    def depth_of(c):
        return sum(jnp.where(c // each == a, n, 0) for a, n in enumerate(insets) if n) + jnp.int32(0)

    def chain_copy(side, c):
        return remote(
            leaving.at[side, c], arrived.at[side, c], chain_send.at[side, c // each], chain_recv.at[side, c], {"vec": to_next(side)}
        )

    def cross_copy(side, c):
        return remote(
            leaving.at[side, c], crossed.at[c], chain_send.at[side, c // each], cross_recv.at[c // (2 * each) * each + c % each], {"vec": to_next(side), "orb": 1 - o}
        )

    def swap_copy(c):
        return remote(leaving.at[near, c], given.at[c], swap_send.at[c // (2 * each)], swap_recv.at[c // (2 * each)], {"orb": 1 - o})

    def extra_copy(side):
        return remote(
            extra_out.at[side], extra_in.at[side], extra_send.at[side], extra_recv.at[side], {"vec": to_next(side)}
        )

    def back_copy(c):
        return remote(
            leaving.at[near, c], back.at[o, c], chain_send.at[near, c // each], back_recv.at[o, c // (2 * each)],
            {"vec": inward, "orb": (c // each) % 2},
        )

    def part_of(side, c):
        at = c % each
        return partial[side * half + c // each, at // SUB, pl.ds(pl.multiple_of((at % SUB) * piece, piece), piece), :]

    def pass_on(side, c, togo):
        here = (c // each) % 2 == o

        @pl.when((togo > 1) | here)
        def _():
            chain_copy(side, c).start()

        @pl.when((togo == 1) & jnp.logical_not(here))
        def _():
            cross_copy(side, c).start()

    pair = BLOCKS // 2
    ahead = pair * SUB
    for n0 in range(0, BLOCKS, pair):
        for j in range(block // span):
            summed = jnp.dot(kron, strips[j, :, n0 * block:(n0 + pair) * block], preferred_element_type=F32)
            for n in range(pair):
                partial[:, n0 + n, j * span:(j + 1) * span, :] = summed[:, n * block:(n + 1) * block].reshape(
                    local, span, block
                )
        if n0 == 0:
            @pl.when(at_end)
            def _():
                for c in range(ahead):
                    leaving[1 - near, c] = part_of(1 - near, c).astype(BF16)
                    pass_on(1 - near, c, last - insets[0])
    edge_part = jnp.dot(weighted, level[...], preferred_element_type=F32)

    def chain_step(t, carry):
        for turn in range(2):
            side = jnp.where(z <= last - z, 1 - turn, turn)
            before = jnp.where(side == 0, last - z, z)
            after = last - before
            c = t - SKEW * before
            head = before == 0
            togo = after - depth_of(c)

            @pl.when((c >= jnp.where(head, ahead, 0)) & (c < chunks) & (togo > 0))
            def _():
                own = part_of(side, c)

                @pl.when(head)
                def _():
                    leaving[side, c] = own.astype(BF16)

                @pl.when(jnp.logical_not(head))
                def _():
                    chain_copy(side, c).wait_recv()
                    leaving[side, c] = (own + arrived[side, c].astype(F32)).astype(BF16)

                pass_on(side, c, togo)

            @pl.when((c == 0) & (after > 0))
            def _():
                @pl.when(head)
                def _():
                    extra_in[side] = jnp.zeros_like(extra_in[side])

                @pl.when(jnp.logical_not(head))
                def _():
                    extra_copy(side).wait_recv()

                extra_out[side, 0:local, :] = extra_in[side, 0:local, :] + factor
                extra_out[side, local:, :] = extra_in[side, local:, :] + edge_part
                extra_copy(side).start()

        return carry

    lax.fori_loop(0, SKEW * (last - 1) + chunks, chain_step, jnp.int32(0))

    for hop in hops:
        copies_copy(hop, lax.rem(x + hop, width)).wait_recv()

    def stage_copy(hop, a):
        return remote(
            staged.at[hop, a], pool.at[x, a // 2, o], stage_send.at[a], pool_recv.at[a // 2],
            {"walk": lax.rem(x + hop, width), "orb": a % 2},
        )

    def swap_core():
        return remote(edge.at[o], edge.at[o], edge_sems.at[0], edge_sems.at[1], {"orb": 1 - o})

    for a in range(half):
        @pl.when(at_owner[a])
        def _():
            for hop in range(width):
                source = copies[lax.rem(x + hop, width), base + a]
                held = walkers[source % local]
                if hop > 0:
                    staged[hop, a] = held
                    stage_copy(hop, a).start()
                else:
                    @pl.when(a % 2 == o)
                    def _():
                        pool[x, a // 2, o] = held

                    @pl.when(a % 2 != o)
                    def _():
                        staged[hop, a] = held
                        stage_copy(hop, a).start()

            @pl.when(a % 2 != o)
            def _():
                def give(c, carry):
                    leaving[near, c] = part_of(near, c).astype(BF16)
                    swap_copy(c).start()
                    return carry

                lax.fori_loop(a * each, (a + 1) * each, give, jnp.int32(0))

        if insets[a]:
            @pl.when(at_end)
            def _():
                def back_step(c, carry):
                    leaving[near, c] = part_of(near, c).astype(BF16)
                    back_copy(c).start()
                    return carry

                lax.fori_loop(a * each, (a + 1) * each, back_step, jnp.int32(0))

    for side in range(2):
        @pl.when(at_end & (near == side))
        def _():
            extra_copy(side).wait_recv()

    owning = functools.reduce(jnp.logical_or, at_owner)

    @pl.when(owning)
    def _():
        edge[o] = edge_part + extra_in[0, local:, :] + extra_in[1, local:, :]
        swap_core().start()
        swap_core().wait_recv()

    share = rows // PARTS
    short = last <= REACH
    plans = [
        tuple(n for n in PLANS[min(half - a, len(PLANS)) - 1] if -insets[a] <= n <= last - insets[a])
        if short else (1,) + (-1,) * insets[a] for a in range(half)
    ]

    def passes(a, away):
        if not short:
            return (away > 0) & (away < last - insets[a])
        gaps = [away == n for n in range(1, last - insets[a]) if n + 1 not in plans[a]]
        return functools.reduce(jnp.logical_or, gaps, jnp.bool_(False))

    def place(w, part):
        return gathered.at[w, pl.ds(part * share, share)]

    def away_z(n):
        return jnp.where(near == 0, z + n, z - n)

    def spread_copies(a):
        w = base + a
        targets = []
        for n in plans[a]:
            for core in (1 - a % 2, a % 2):
                targets.append((core, {"vec": away_z(n), "orb": core}))
        targets.append((1 - a % 2, {"orb": 1 - o}))
        return [
            remote(
                result.at[a // 2, core, pl.ds(part * share, share)], place(w, part),
                own_send.at[a // 2], slot_recv.at[w, part], where,
            )
            for n, (core, where) in enumerate(targets)
            for part in range(PARTS)
        ]

    upper = lax.broadcasted_iota(jnp.int32, (block, block), 0) < lax.broadcasted_iota(jnp.int32, (block, block), 1)
    level_mask = lax.broadcasted_iota(jnp.int32, (block, block), 0) == lax.broadcasted_iota(jnp.int32, (block, block), 1)

    def finish(a):
        w = base + a
        i = a // 2

        def put(r, c, value):
            full[columns(r), columns(c)] = value

        come = gathered.at[pl.ds(0, 2 * width - 1)]
        remote(come, come, stage_send.at[0], pool_recv.at[i], {"orb": 1 - o}).wait_recv()
        column = copies[x, w] // local
        for core in range(2):
            start = pool[0, i, core]
            for other in hops:
                start = jnp.where(column == other, pool[other, i, core], start)
            terms[0, :, core * rows:(core + 1) * rows] = start.T
        whole = pl.ds(a * each, each)
        remote(leaving.at[near, whole], given.at[whole], swap_send.at[i], swap_recv.at[i], {"orb": 1 - o}).wait_recv()
        if insets[a]:
            for core in range(2):
                remote(
                    leaving.at[near, whole], back.at[core, whole], chain_send.at[near, a], back_recv.at[core, i],
                    {"vec": inward, "orb": core},
                ).wait_recv()
        for n in range(BLOCKS):
            first_c = a * each + n * SUB
            for c in range(first_c, first_c + SUB):
                remote(
                    leaving.at[near, c], arrived.at[near, c], chain_send.at[near, c // each], chain_recv.at[near, c], {"vec": inward}
                ).wait_recv()
                remote(
                    leaving.at[near, c], crossed.at[c], chain_send.at[near, c // each], cross_recv.at[c // (2 * each) * each + c % each],
                    {"vec": inward, "orb": 1 - o},
                ).wait_recv()
            run = pl.ds(first_c, SUB)
            kept = partial[w, n] + arrived[near, run].reshape(block, block).astype(F32)
            taken = given[run].reshape(block, block).astype(F32) + crossed[run].reshape(block, block).astype(F32)
            if insets[a]:
                kept = kept + back[o, run].reshape(block, block).astype(F32)
                taken = taken + back[1 - o, run].reshape(block, block).astype(F32)
            for core, value in ((o, kept), (1 - o, taken)):
                if n == 0:
                    flipped = value.T
                    line = edge[core, pl.ds(w, 1), :]
                    put(2 * core, 2 * core, jnp.where(upper | level_mask, value, flipped).astype(BF16))
                    low = jnp.where(level_mask, jnp.broadcast_to(line, (block, block)), jnp.where(upper, flipped, value))
                    put(2 * core + 1, 2 * core + 1, low.astype(BF16))
                else:
                    r, k = ((2 * core, 1), (2 * core, 2 + core), (2 * core + 1, 3 * (1 - core)))[n - 1]
                    value = value.astype(BF16)
                    put(r, k, value)
                    put(k, r, value.T)

        for degree in range(1, ORDER + 1):
            fresh = (jnp.dot(terms[degree - 1], full[...], preferred_element_type=F32) * (1.0 / degree)).astype(BF16)
            terms[degree] = fresh
        running = terms[0].astype(F32)
        for degree in range(1, ORDER + 1):
            running = running + terms[degree].astype(F32)
        result[i] = running.astype(BF16).T.reshape(2, rows, electrons)
        for copy in spread_copies(a):
            copy.start()
        settle = pltpu.make_async_copy(result.at[i, o], gathered.at[w], write_sems.at[i])
        settle.start()

    def onward(w, part, hop_to):
        spot = place(w, part)
        return remote(spot, spot, next_send.at[w, part], slot_recv.at[w, part], {"vec": hop_to})

    def route(side, a):
        w = side * half + a
        away = jnp.where(side == 0, z, last - z) - insets[a]
        hop_to = jnp.where(side == 0, z + 1, z - 1)
        return w, away, hop_to

    def forward(slots):
        for a in slots:
            for side in (near, 1 - near):
                w, away, hop_to = route(side, a)

                @pl.when(passes(a, away))
                def _():
                    for part in range(PARTS):
                        onward(w, part, hop_to).wait_recv()
                        onward(w, part, hop_to).start()

    early = [a for a in range(half) if short and a < EARLY]
    forward(early)
    for a in range(half):
        @pl.when(at_owner[a] & (a % 2 == o))
        def _():
            finish(a)

    new_log = old_log + factor + extra_in[0, 0:local, :] + extra_in[1, 0:local, :]
    out_log[...] = new_log

    forward([a for a in range(half) if a not in early])

    for copy in bias_copies:
        copy.wait_send()
    for hop in hops:
        facts_copy(hop, x).wait_send()
        copies_copy(hop, x).wait_send()

    def sent(side, a):
        whole = pl.ds(a * each, each)
        return remote(
            leaving.at[side, whole], arrived.at[side, whole], chain_send.at[side, a], chain_recv.at[side, a], {"orb": 1 - o}
        )

    for side in range(2):
        for a in range(half):
            @pl.when(downstream[side] - insets[a] != 0)
            def _():
                sent(side, a).wait_send()

    for side in range(2):
        @pl.when(downstream[side] > 0)
        def _():
            extra_copy(side).wait_send()

    @pl.when(owning)
    def _():
        swap_core().wait_send()

    for a in range(half):
        @pl.when(at_owner[a])
        def _():
            def moved(n):
                run = gathered.at[pl.ds(0, n)]
                return remote(run, run, stage_send.at[a], slot_recv.at[0, 0], {"orb": 1 - o})

            @pl.when(a % 2 == o)
            def _():
                moved(width - 1).wait_send()

            @pl.when(a % 2 != o)
            def _():
                moved(width).wait_send()

                whole = pl.ds(a * each, each)
                remote(
                    leaving.at[near, whole], given.at[whole], swap_send.at[a // 2], swap_recv.at[a // 2], {"orb": 1 - o}
                ).wait_send()

    for a in range(half):
        for side in (near, 1 - near):
            w, away, hop_to = route(side, a)

            @pl.when(((away != 0) | (o != a % 2)) & jnp.logical_not(passes(a, away)))
            def _():
                for part in range(PARTS):
                    onward(w, part, hop_to).wait_recv()

    for a in range(half):
        @pl.when(at_owner[a] & (a % 2 == o))
        def _():
            run = gathered.at[pl.ds(0, 2 * len(plans[a]) + 1)]
            remote(run, run, own_send.at[a // 2], slot_recv.at[0, 0], {"orb": 1 - o}).wait_send()
            pltpu.make_async_copy(result.at[a // 2, o], gathered.at[base + a], write_sems.at[a // 2]).wait()

    for a in range(half):
        for side in range(2):
            w, away, hop_to = route(side, a)

            @pl.when(passes(a, away))
            def _():
                for part in range(PARTS):
                    onward(w, part, hop_to).wait_send()


def per_device(depth, width, walkers, inv_intersection, trial, vectors, aux_field, log_weight, copy_list):
    local, rows, electrons = walkers.shape
    count, _, orbitals = vectors.shape
    half = local // 2
    block = orbitals // 4
    span = 2 * block // count
    wide = count * span
    piece = block // SUB
    chunks = half * BLOCKS * SUB
    mine = half // 2
    lanes = 128
    dma = pltpu.SemaphoreType.DMA
    anywhere = pl.BlockSpec(memory_space=pl.ANY)
    out, out_log = pl.pallas_call(
        functools.partial(kernel, depth, width),
        out_shape=(
            pltpu.VMEM(walkers.shape, BF16),
            pltpu.VMEM((local, 128), F32),
        ),
        in_specs=[anywhere] * 7,
        out_specs=(anywhere, pl.BlockSpec(memory_space=pltpu.VMEM)),
        scratch_shapes=[
            pltpu.VMEM(walkers.shape, BF16),
            pltpu.VMEM(inv_intersection.shape, BF16),
            pltpu.VMEM(trial.shape, BF16),
            pltpu.VMEM(vectors.shape, BF16),
            pltpu.VMEM(aux_field.shape, F32),
            pltpu.SMEM((local,), F32),
            pltpu.SMEM((width, local), jnp.int32),
            pltpu.VMEM((local, rows, electrons), BF16),
            pltpu.VMEM((count, rows, electrons), BF16),
            pltpu.VMEM((block // span, wide, BLOCKS * block), BF16),
            pltpu.VMEM((wide, block), BF16),
            pltpu.VMEM((2, width, local, lanes), F32),
            pltpu.VMEM((width, local, lanes), F32),
            pltpu.VMEM((local, lanes), F32),
            pltpu.VMEM((local, lanes), F32),
            pltpu.VMEM((local, BLOCKS, block, block), F32),
            pltpu.VMEM((2, chunks, piece, block), BF16),
            pltpu.VMEM((2, chunks, piece, block), BF16),
            pltpu.VMEM((chunks, piece, block), BF16),
            pltpu.VMEM((chunks, piece, block), BF16),
            pltpu.VMEM((2, chunks, piece, block), BF16),
            pltpu.VMEM((2, 2 * local, lanes), F32),
            pltpu.VMEM((2, 2 * local, lanes), F32),
            pltpu.VMEM((2, local, lanes), F32),
            pltpu.VMEM((width, half, rows, electrons), BF16),
            pltpu.VMEM((width, mine, 2, rows, electrons), BF16),
            pltpu.VMEM((orbitals, orbitals), BF16),
            pltpu.VMEM((ORDER + 1, electrons, orbitals), BF16),
            pltpu.VMEM((mine, 2, rows, electrons), BF16),
            dma((6 + LOADS,)),
            dma((width,)),
            dma((width,)),
            dma((width,)),
            dma((width,)),
            dma((2 * width,)),
            dma((2, width)),
            dma((2, half)),
            dma((2, chunks)),
            dma((chunks // 2,)),
            dma((2, mine)),
            dma((mine,)),
            dma((mine,)),
            dma((2,)),
            dma((2,)),
            dma((2,)),
            dma((half,)),
            dma((mine,)),
            dma((mine,)),
            dma((local, PARTS)),
            dma((local, PARTS)),
            dma((mine,)),
        ],
        compiler_params=pltpu.CompilerParams(collective_id=0, has_side_effects=True),
    )(walkers, inv_intersection, trial, vectors, aux_field, log_weight, copy_list)

    def settle(out_ref, log_ref, o1, o2, flat, sems):
        c1 = pltpu.make_async_copy(out_ref, o1, sems.at[0])
        c1.start()
        for s in range(local):
            flat[s] = jnp.max(log_ref[s:s + 1, :])
        c2 = pltpu.make_async_copy(flat, o2, sems.at[1])
        c2.start()
        c1.wait()
        c2.wait()

    return pl.pallas_call(
        settle,
        out_shape=(jax.ShapeDtypeStruct(walkers.shape, BF16), jax.ShapeDtypeStruct((local,), F32)),
        in_specs=[pl.BlockSpec(memory_space=pltpu.VMEM)] * 2,
        out_specs=(anywhere, anywhere),
        scratch_shapes=[pltpu.SMEM((local,), F32), dma((2,))],
    )(pltpu.with_memory_space_constraint(out, pltpu.VMEM), pltpu.with_memory_space_constraint(out_log, pltpu.VMEM))


def solution(mesh):
    depth, width = mesh.shape["vec"], mesh.shape["walk"]
    assert mesh.shape["orb"] == 2 and depth > 1
    return jax.shard_map(
        functools.partial(per_device, depth, width),
        mesh=mesh,
        in_specs=(
            P(("grp", "walk"), "orb", None),
            P(("grp", "walk"), None, None),
            P(),
            P("vec", "orb", None),
            P(("grp", "walk"), "vec"),
            P(("grp", "walk")),
            P(("grp", "walk")),
        ),
        out_specs=(P(("grp", "walk"), "orb", None), P(("grp", "walk"))),
        check_vma=False,
    )
```

```python
import functools
import math

import jax
import jax.numpy as jnp
from jax import lax
from jax.experimental import pallas as pl
from jax.experimental.pallas import tpu as pltpu
from jax.sharding import PartitionSpec as P

ORDER = 6
BLOCKS = 4
SUB = 1
SKEW = 5
EARLY = 1
PARTS = 1
LOADS = 2
REACH = 3
PLANS = ((2, -1, 1), (3, 2, 1), (3, 2, 1), (2, 1))
MESH = pl.DeviceIdType.MESH
F32 = jnp.float32
BF16 = jnp.bfloat16

step_root = math.sqrt(0.08)


def remote(src, dst, send, recv, where):
    return pltpu.make_async_remote_copy(
        src_ref=src, dst_ref=dst, send_sem=send, recv_sem=recv, device_id=where, device_id_type=MESH
    )


def kernel(
    depth, width,
    walkers_in, inverse_in, trial_in, vectors_in, aux_in, log_in, copies_in,
    out, out_log,
    walkers, inverse, trial, vectors, aux, log_weight, copies,
    green, mixed, strips, level, bias_all, facts, known, picked, partial, leaving, arrived, given, crossed,
    back, extra_in, extra_out, edge, staged, pool, full, terms, result,
    load_sems, copies_send, copies_recv, facts_send, facts_recv, bias_send, bias_recv,
    chain_send, chain_recv, cross_recv, back_recv, swap_send, swap_recv, extra_send, extra_recv, edge_sems,
    stage_send, pool_recv, own_send, next_send, slot_recv, write_sems,
):
    gathered = out
    z = lax.axis_index("vec")
    x = lax.axis_index("walk")
    o = lax.axis_index("orb")
    last = depth - 1
    local, rows, electrons = walkers.shape
    count, _, orbitals = vectors.shape
    half = local // 2
    block = orbitals // 4
    span = 2 * block // count
    wide = count * span
    piece = block // SUB
    each = BLOCKS * SUB
    chunks = half * each
    mine = half // 2
    lanes = extra_in.shape[2]
    insets = [1 if a == half - 1 and last >= REACH else 0 for a in range(half)]
    hops = range(1, width)

    barrier = pltpu.get_barrier_semaphore()

    def greet(where):
        pl.semaphore_signal(barrier, inc=1, device_id=where, device_id_type=MESH)

    greet({"orb": 1 - o})
    for hop in hops:
        for core in range(2):
            greet({"walk": lax.rem(x + hop, width), "orb": core})

    @pl.when(z > 0)
    def _():
        for core in range(2):
            greet({"vec": z - 1, "orb": core})

    @pl.when(z < last)
    def _():
        for core in range(2):
            greet({"vec": z + 1, "orb": core})

    batch = count // LOADS
    pairs = [(trial_in, trial)]
    for n in range(LOADS):
        group = pl.ds(n * batch, batch)
        pairs.append((vectors_in.at[group], vectors.at[group]))
    pairs += [
        (inverse_in, inverse), (walkers_in, walkers), (copies_in, copies.at[x]), (log_in, log_weight), (aux_in, aux),
    ]
    loads = [pltpu.make_async_copy(src, dst, load_sems.at[n]) for n, (src, dst) in enumerate(pairs)]
    for load in loads:
        load.start()

    loads[0].wait()
    for n in range(LOADS):
        loads[1 + n].wait()
        for g in range(n * batch, (n + 1) * batch):
            mixed[g] = jnp.dot(vectors[g], trial[...], preferred_element_type=F32).astype(BF16)
    for load in loads[1 + LOADS:]:
        load.wait()
    for w in range(local):
        green[w] = jnp.dot(walkers[w], inverse[w], preferred_element_type=F32).astype(BF16)
    walker_id = lax.broadcasted_iota(jnp.int32, (local, lanes), 0)
    weights = jnp.zeros((local, lanes), F32)
    for w in range(local):
        weights = jnp.where(walker_id == w, log_weight[w], weights)
    facts[x] = weights
    facts[x, :, 0:count] = aux[...]
    left = [green[:, j * span:(j + 1) * span, :].reshape(local * span, electrons) for j in range(rows // span)]
    right = [mixed[:, j * span:(j + 1) * span, :].reshape(wide, electrons) for j in range(rows // span)]
    gram = lax.dot_general(
        jnp.concatenate(left, axis=1), jnp.concatenate(right, axis=1), (((1,), (1,)), ((), ())), preferred_element_type=F32
    )
    row_id = lax.broadcasted_iota(jnp.int32, (local * span, wide), 0)
    col_id = lax.broadcasted_iota(jnp.int32, (local * span, wide), 1)
    same = row_id % span == col_id % span
    folded = jnp.sum(jnp.where(same, gram, 0.0).reshape(local, span, wide), axis=1)
    lane_id = lax.broadcasted_iota(jnp.int32, (local, wide), 1)
    step = 1
    while step < span:
        low = lane_id % (2 * step) < step
        folded = folded + jnp.where(low, pltpu.roll(folded, wide - step, 1), pltpu.roll(folded, step, 1))
        step *= 2
    lane = lax.broadcasted_iota(jnp.int32, (local, lanes), 1) % span
    fold = span // 2
    bias_all[o, x] = jnp.where(lane < fold, folded[:, :lanes], folded[:, lanes:])

    sides = jnp.where(z > 0, 2, 0) + jnp.where(z < last, 2, 0)
    pl.semaphore_wait(barrier, 1 + 2 * (width - 1) + sides)

    bias_peers = [{"walk": lax.rem(x + hop, width), "orb": core} for hop in hops for core in range(2)] + [{"orb": 1 - o}]
    bias_copies = [
        remote(bias_all.at[o, x], bias_all.at[o, x], bias_send.at[n], bias_recv.at[o, x], where)
        for n, where in enumerate(bias_peers)
    ]
    def facts_copy(hop, owner):
        return remote(
            facts.at[owner], facts.at[owner], facts_send.at[hop], facts_recv.at[owner], {"walk": lax.rem(x + hop, width)}
        )

    def copies_copy(hop, owner):
        return remote(
            copies.at[owner], copies.at[owner], copies_send.at[hop], copies_recv.at[owner],
            {"walk": lax.rem(x + hop, width)},
        )

    for copy in bias_copies:
        copy.start()
    for hop in hops:
        facts_copy(hop, x).start()
        copies_copy(hop, x).start()

    chunk_row = lax.broadcasted_iota(jnp.int32, (count, span, block), 1)
    chunk_col = lax.broadcasted_iota(jnp.int32, (count, span, block), 2)
    crossing = jnp.zeros((count, span, block), F32)

    def columns(n):
        return pl.ds(pl.multiple_of(n * block, block), block)

    for j in range(block // span):
        here = slice(j * span, (j + 1) * span)
        below = slice(block + j * span, block + (j + 1) * span)
        first = vectors[:, here, columns(2 * o)].astype(F32)
        second = vectors[:, below, columns(1 + 2 * o)].astype(F32)
        crossing = crossing + jnp.where(chunk_row + j * span == chunk_col, second, 0.0)
        joined = jnp.where(chunk_row + j * span <= chunk_col, first, second).astype(BF16)
        strips[j, :, 0:block] = joined.reshape(wide, block)
        strips[j, :, block:2 * block] = vectors[:, here, block:2 * block].reshape(wide, block)
        strips[j, :, 2 * block:3 * block] = vectors[:, here, columns(2 + o)].reshape(wide, block)
        strips[j, :, 3 * block:] = vectors[:, below, columns(3 * (1 - o))].reshape(wide, block)
    level[...] = crossing.reshape(wide, block).astype(BF16)

    for hop in hops:
        facts_copy(hop, lax.rem(x + hop, width)).wait_recv()
    sources = [(copies[x, s] // local, pl.ds(copies[x, s] % local, 1)) for s in range(local)]
    for s, (column, row) in enumerate(sources):
        known[s:s + 1, :] = facts[column, row, :]
    pick_row = lax.broadcasted_iota(jnp.int32, (count, wide), 0)
    pick_col = lax.broadcasted_iota(jnp.int32, (count, wide), 1)
    pick = jnp.where(pick_row == pick_col // span, 1.0, 0.0).astype(F32)
    drawn = jnp.dot(known[:, 0:count], pick, precision=lax.Precision.HIGHEST, preferred_element_type=F32)
    old_log = jnp.broadcast_to(known[:, count:count + 1], (local, lanes))

    for hop in hops:
        other = lax.rem(x + hop, width)
        for core in range(2):
            remote(
                bias_all.at[core, other], bias_all.at[core, other], bias_send.at[0], bias_recv.at[core, other], {"walk": other}
            ).wait_recv()
    remote(bias_all.at[1 - o, x], bias_all.at[1 - o, x], bias_send.at[0], bias_recv.at[1 - o, x], {"orb": 1 - o}).wait_recv()

    for s, (column, row) in enumerate(sources):
        picked[s:s + 1, :] = bias_all[0, column, row, :] + bias_all[1, column, row, :]
    both = picked[...]
    bias = jnp.concatenate(
        [jnp.where(lane < fold, both, pltpu.roll(both, fold, 1)), jnp.where(lane < fold, pltpu.roll(both, lanes - fold, 1), both)],
        axis=1,
    )
    shift = -step_root * bias
    field = drawn - shift
    factor = jnp.sum(drawn * shift - 0.5 * shift * shift, axis=1, keepdims=True) * (1.0 / span)
    factor = jnp.broadcast_to(factor, (local, lanes))
    weighted = (field * step_root).astype(BF16)
    spread = jnp.broadcast_to(weighted.astype(F32)[:, None, :], (local, span, wide)).reshape(local * span, wide)
    kron = jnp.where(same, spread, 0.0).astype(BF16)

    def to_next(side):
        return jnp.where(side == 0, z - 1, z + 1)

    upstream = [last - z, z]
    downstream = [z, last - z]
    at_end = (z == 0) | (z == last)
    near = jnp.where(z <= last - z, 0, 1)
    base = near * half
    inward = jnp.where(near == 0, z + 1, z - 1)
    at_owner = [(z == n) | (z == last - n) for n in insets]

    def depth_of(c):
        return sum(jnp.where(c // each == a, n, 0) for a, n in enumerate(insets) if n) + jnp.int32(0)

    def chain_copy(side, c):
        return remote(
            leaving.at[side, c], arrived.at[side, c], chain_send.at[side, c // each], chain_recv.at[side, c], {"vec": to_next(side)}
        )

    def cross_copy(side, c):
        return remote(
            leaving.at[side, c], crossed.at[c], chain_send.at[side, c // each], cross_recv.at[c // (2 * each) * each + c % each], {"vec": to_next(side), "orb": 1 - o}
        )

    def swap_copy(c):
        return remote(leaving.at[near, c], given.at[c], swap_send.at[c // (2 * each)], swap_recv.at[c // (2 * each)], {"orb": 1 - o})

    def extra_copy(side):
        return remote(
            extra_out.at[side], extra_in.at[side], extra_send.at[side], extra_recv.at[side], {"vec": to_next(side)}
        )

    def back_copy(c):
        return remote(
            leaving.at[near, c], back.at[o, c], chain_send.at[near, c // each], back_recv.at[o, c // (2 * each)],
            {"vec": inward, "orb": (c // each) % 2},
        )

    def part_of(side, c):
        at = c % each
        return partial[side * half + c // each, at // SUB, pl.ds(pl.multiple_of((at % SUB) * piece, piece), piece), :]

    def pass_on(side, c, togo):
        here = (c // each) % 2 == o

        @pl.when((togo > 1) | here)
        def _():
            chain_copy(side, c).start()

        @pl.when((togo == 1) & jnp.logical_not(here))
        def _():
            cross_copy(side, c).start()

    pair = BLOCKS // 2
    ahead = pair * SUB
    for n0 in range(0, BLOCKS, pair):
        for j in range(block // span):
            summed = jnp.dot(kron, strips[j, :, n0 * block:(n0 + pair) * block], preferred_element_type=F32)
            for n in range(pair):
                partial[:, n0 + n, j * span:(j + 1) * span, :] = summed[:, n * block:(n + 1) * block].reshape(
                    local, span, block
                )
        if n0 == 0:
            @pl.when(at_end)
            def _():
                for c in range(ahead):
                    leaving[1 - near, c] = part_of(1 - near, c).astype(BF16)
                    pass_on(1 - near, c, last - insets[0])
    edge_part = jnp.dot(weighted, level[...], preferred_element_type=F32)

    def chain_step(t, carry):
        for turn in range(2):
            side = jnp.where(z <= last - z, 1 - turn, turn)
            before = jnp.where(side == 0, last - z, z)
            after = last - before
            c = t - SKEW * before
            head = before == 0
            togo = after - depth_of(c)

            @pl.when((c >= jnp.where(head, ahead, 0)) & (c < chunks) & (togo > 0))
            def _():
                own = part_of(side, c)

                @pl.when(head)
                def _():
                    leaving[side, c] = own.astype(BF16)

                @pl.when(jnp.logical_not(head))
                def _():
                    chain_copy(side, c).wait_recv()
                    leaving[side, c] = (own + arrived[side, c].astype(F32)).astype(BF16)

                pass_on(side, c, togo)

            @pl.when((c == 0) & (after > 0))
            def _():
                @pl.when(head)
                def _():
                    extra_in[side] = jnp.zeros_like(extra_in[side])

                @pl.when(jnp.logical_not(head))
                def _():
                    extra_copy(side).wait_recv()

                extra_out[side, 0:local, :] = extra_in[side, 0:local, :] + factor
                extra_out[side, local:, :] = extra_in[side, local:, :] + edge_part
                extra_copy(side).start()

        return carry

    for hop in hops:
        copies_copy(hop, lax.rem(x + hop, width)).wait_recv()

    def stage_copy(hop, a):
        return remote(
            staged.at[hop, a], pool.at[x, a // 2, o], stage_send.at[a], pool_recv.at[a // 2],
            {"walk": lax.rem(x + hop, width), "orb": a % 2},
        )

    def swap_core():
        return remote(edge.at[o], edge.at[o], edge_sems.at[0], edge_sems.at[1], {"orb": 1 - o})

    def prepare(a):
        @pl.when(at_owner[a])
        def _():
            for hop in range(width):
                source = copies[lax.rem(x + hop, width), base + a]
                held = walkers[source % local]
                if hop > 0:
                    staged[hop, a] = held
                    stage_copy(hop, a).start()
                else:
                    @pl.when(a % 2 == o)
                    def _():
                        pool[x, a // 2, o] = held

                    @pl.when(a % 2 != o)
                    def _():
                        staged[hop, a] = held
                        stage_copy(hop, a).start()

            @pl.when(a % 2 != o)
            def _():
                def give(c, carry):
                    leaving[near, c] = part_of(near, c).astype(BF16)
                    swap_copy(c).start()
                    return carry

                lax.fori_loop(a * each, (a + 1) * each, give, jnp.int32(0))

    def send_back(a):
        @pl.when(at_end)
        def _():
            def back_step(c, carry):
                leaving[near, c] = part_of(near, c).astype(BF16)
                back_copy(c).start()
                return carry

            lax.fori_loop(a * each, (a + 1) * each, back_step, jnp.int32(0))

    for a in range(half):
        if insets[a]:
            prepare(a)

    lax.fori_loop(0, SKEW * (last - 1) + chunks, chain_step, jnp.int32(0))

    for a in range(half):
        if not insets[a]:
            prepare(a)
        else:
            send_back(a)

    for side in range(2):
        @pl.when(at_end & (near == side))
        def _():
            extra_copy(side).wait_recv()

    owning = functools.reduce(jnp.logical_or, at_owner)

    @pl.when(owning)
    def _():
        edge[o] = edge_part + extra_in[0, local:, :] + extra_in[1, local:, :]
        swap_core().start()
        swap_core().wait_recv()

    share = rows // PARTS
    short = last <= REACH
    plans = [
        tuple(n for n in PLANS[min(half - a, len(PLANS)) - 1] if -insets[a] <= n <= last - insets[a])
        if short else (1,) + (-1,) * insets[a] for a in range(half)
    ]

    def passes(a, away):
        if not short:
            return (away > 0) & (away < last - insets[a])
        gaps = [away == n for n in range(1, last - insets[a]) if n + 1 not in plans[a]]
        return functools.reduce(jnp.logical_or, gaps, jnp.bool_(False))

    def place(w, part):
        return gathered.at[w, pl.ds(part * share, share)]

    def away_z(n):
        return jnp.where(near == 0, z + n, z - n)

    def spread_copies(a):
        w = base + a
        targets = []
        for n in plans[a]:
            for core in (1 - a % 2, a % 2):
                targets.append((core, {"vec": away_z(n), "orb": core}))
        targets.append((1 - a % 2, {"orb": 1 - o}))
        return [
            remote(
                result.at[a // 2, core, pl.ds(part * share, share)], place(w, part),
                own_send.at[a // 2], slot_recv.at[w, part], where,
            )
            for n, (core, where) in enumerate(targets)
            for part in range(PARTS)
        ]

    upper = lax.broadcasted_iota(jnp.int32, (block, block), 0) < lax.broadcasted_iota(jnp.int32, (block, block), 1)
    level_mask = lax.broadcasted_iota(jnp.int32, (block, block), 0) == lax.broadcasted_iota(jnp.int32, (block, block), 1)

    def finish(a):
        w = base + a
        i = a // 2

        def put(r, c, value):
            full[columns(r), columns(c)] = value

        come = gathered.at[pl.ds(0, 2 * width - 1)]
        remote(come, come, stage_send.at[0], pool_recv.at[i], {"orb": 1 - o}).wait_recv()
        column = copies[x, w] // local
        for core in range(2):
            start = pool[0, i, core]
            for other in hops:
                start = jnp.where(column == other, pool[other, i, core], start)
            terms[0, :, core * rows:(core + 1) * rows] = start.T
        whole = pl.ds(a * each, each)
        remote(leaving.at[near, whole], given.at[whole], swap_send.at[i], swap_recv.at[i], {"orb": 1 - o}).wait_recv()
        if insets[a]:
            for core in range(2):
                remote(
                    leaving.at[near, whole], back.at[core, whole], chain_send.at[near, a], back_recv.at[core, i],
                    {"vec": inward, "orb": core},
                ).wait_recv()
        for n in range(BLOCKS):
            first_c = a * each + n * SUB
            for c in range(first_c, first_c + SUB):
                remote(
                    leaving.at[near, c], arrived.at[near, c], chain_send.at[near, c // each], chain_recv.at[near, c], {"vec": inward}
                ).wait_recv()
                remote(
                    leaving.at[near, c], crossed.at[c], chain_send.at[near, c // each], cross_recv.at[c // (2 * each) * each + c % each],
                    {"vec": inward, "orb": 1 - o},
                ).wait_recv()
            run = pl.ds(first_c, SUB)
            kept = partial[w, n] + arrived[near, run].reshape(block, block).astype(F32)
            taken = given[run].reshape(block, block).astype(F32) + crossed[run].reshape(block, block).astype(F32)
            if insets[a]:
                kept = kept + back[o, run].reshape(block, block).astype(F32)
                taken = taken + back[1 - o, run].reshape(block, block).astype(F32)
            for core, value in ((o, kept), (1 - o, taken)):
                if n == 0:
                    flipped = value.T
                    line = edge[core, pl.ds(w, 1), :]
                    put(2 * core, 2 * core, jnp.where(upper | level_mask, value, flipped).astype(BF16))
                    low = jnp.where(level_mask, jnp.broadcast_to(line, (block, block)), jnp.where(upper, flipped, value))
                    put(2 * core + 1, 2 * core + 1, low.astype(BF16))
                else:
                    r, k = ((2 * core, 1), (2 * core, 2 + core), (2 * core + 1, 3 * (1 - core)))[n - 1]
                    value = value.astype(BF16)
                    put(r, k, value)
                    put(k, r, value.T)

        for degree in range(1, ORDER + 1):
            fresh = (jnp.dot(terms[degree - 1], full[...], preferred_element_type=F32) * (1.0 / degree)).astype(BF16)
            terms[degree] = fresh
        running = terms[0].astype(F32)
        for degree in range(1, ORDER + 1):
            running = running + terms[degree].astype(F32)
        result[i] = running.astype(BF16).T.reshape(2, rows, electrons)
        for copy in spread_copies(a):
            copy.start()
        settle = pltpu.make_async_copy(result.at[i, o], gathered.at[w], write_sems.at[i])
        settle.start()

    def onward(w, part, hop_to):
        spot = place(w, part)
        return remote(spot, spot, next_send.at[w, part], slot_recv.at[w, part], {"vec": hop_to})

    def route(side, a):
        w = side * half + a
        away = jnp.where(side == 0, z, last - z) - insets[a]
        hop_to = jnp.where(side == 0, z + 1, z - 1)
        return w, away, hop_to

    def forward(slots):
        for a in slots:
            for side in (near, 1 - near):
                w, away, hop_to = route(side, a)

                @pl.when(passes(a, away))
                def _():
                    for part in range(PARTS):
                        onward(w, part, hop_to).wait_recv()
                        onward(w, part, hop_to).start()

    early = [a for a in range(half) if short and a < EARLY]
    forward(early)
    for a in range(half):
        @pl.when(at_owner[a] & (a % 2 == o))
        def _():
            finish(a)

    new_log = old_log + factor + extra_in[0, 0:local, :] + extra_in[1, 0:local, :]
    out_log[...] = new_log

    forward([a for a in range(half) if a not in early])

    for copy in bias_copies:
        copy.wait_send()
    for hop in hops:
        facts_copy(hop, x).wait_send()
        copies_copy(hop, x).wait_send()

    def sent(side, a):
        whole = pl.ds(a * each, each)
        return remote(
            leaving.at[side, whole], arrived.at[side, whole], chain_send.at[side, a], chain_recv.at[side, a], {"orb": 1 - o}
        )

    for side in range(2):
        for a in range(half):
            @pl.when(downstream[side] - insets[a] != 0)
            def _():
                sent(side, a).wait_send()

    for side in range(2):
        @pl.when(downstream[side] > 0)
        def _():
            extra_copy(side).wait_send()

    @pl.when(owning)
    def _():
        swap_core().wait_send()

    for a in range(half):
        @pl.when(at_owner[a])
        def _():
            def moved(n):
                run = gathered.at[pl.ds(0, n)]
                return remote(run, run, stage_send.at[a], slot_recv.at[0, 0], {"orb": 1 - o})

            @pl.when(a % 2 == o)
            def _():
                moved(width - 1).wait_send()

            @pl.when(a % 2 != o)
            def _():
                moved(width).wait_send()

                whole = pl.ds(a * each, each)
                remote(
                    leaving.at[near, whole], given.at[whole], swap_send.at[a // 2], swap_recv.at[a // 2], {"orb": 1 - o}
                ).wait_send()

    for a in range(half):
        for side in (near, 1 - near):
            w, away, hop_to = route(side, a)

            @pl.when(((away != 0) | (o != a % 2)) & jnp.logical_not(passes(a, away)))
            def _():
                for part in range(PARTS):
                    onward(w, part, hop_to).wait_recv()

    for a in range(half):
        @pl.when(at_owner[a] & (a % 2 == o))
        def _():
            run = gathered.at[pl.ds(0, 2 * len(plans[a]) + 1)]
            remote(run, run, own_send.at[a // 2], slot_recv.at[0, 0], {"orb": 1 - o}).wait_send()
            pltpu.make_async_copy(result.at[a // 2, o], gathered.at[base + a], write_sems.at[a // 2]).wait()

    for a in range(half):
        for side in range(2):
            w, away, hop_to = route(side, a)

            @pl.when(passes(a, away))
            def _():
                for part in range(PARTS):
                    onward(w, part, hop_to).wait_send()


def per_device(depth, width, walkers, inv_intersection, trial, vectors, aux_field, log_weight, copy_list):
    local, rows, electrons = walkers.shape
    count, _, orbitals = vectors.shape
    half = local // 2
    block = orbitals // 4
    span = 2 * block // count
    wide = count * span
    piece = block // SUB
    chunks = half * BLOCKS * SUB
    mine = half // 2
    lanes = 128
    dma = pltpu.SemaphoreType.DMA
    anywhere = pl.BlockSpec(memory_space=pl.ANY)
    out, out_log = pl.pallas_call(
        functools.partial(kernel, depth, width),
        out_shape=(
            pltpu.VMEM(walkers.shape, BF16),
            pltpu.VMEM((local, 128), F32),
        ),
        in_specs=[anywhere] * 7,
        out_specs=(anywhere, pl.BlockSpec(memory_space=pltpu.VMEM)),
        scratch_shapes=[
            pltpu.VMEM(walkers.shape, BF16),
            pltpu.VMEM(inv_intersection.shape, BF16),
            pltpu.VMEM(trial.shape, BF16),
            pltpu.VMEM(vectors.shape, BF16),
            pltpu.VMEM(aux_field.shape, F32),
            pltpu.SMEM((local,), F32),
            pltpu.SMEM((width, local), jnp.int32),
            pltpu.VMEM((local, rows, electrons), BF16),
            pltpu.VMEM((count, rows, electrons), BF16),
            pltpu.VMEM((block // span, wide, BLOCKS * block), BF16),
            pltpu.VMEM((wide, block), BF16),
            pltpu.VMEM((2, width, local, lanes), F32),
            pltpu.VMEM((width, local, lanes), F32),
            pltpu.VMEM((local, lanes), F32),
            pltpu.VMEM((local, lanes), F32),
            pltpu.VMEM((local, BLOCKS, block, block), F32),
            pltpu.VMEM((2, chunks, piece, block), BF16),
            pltpu.VMEM((2, chunks, piece, block), BF16),
            pltpu.VMEM((chunks, piece, block), BF16),
            pltpu.VMEM((chunks, piece, block), BF16),
            pltpu.VMEM((2, chunks, piece, block), BF16),
            pltpu.VMEM((2, 2 * local, lanes), F32),
            pltpu.VMEM((2, 2 * local, lanes), F32),
            pltpu.VMEM((2, local, lanes), F32),
            pltpu.VMEM((width, half, rows, electrons), BF16),
            pltpu.VMEM((width, mine, 2, rows, electrons), BF16),
            pltpu.VMEM((orbitals, orbitals), BF16),
            pltpu.VMEM((ORDER + 1, electrons, orbitals), BF16),
            pltpu.VMEM((mine, 2, rows, electrons), BF16),
            dma((6 + LOADS,)),
            dma((width,)),
            dma((width,)),
            dma((width,)),
            dma((width,)),
            dma((2 * width,)),
            dma((2, width)),
            dma((2, half)),
            dma((2, chunks)),
            dma((chunks // 2,)),
            dma((2, mine)),
            dma((mine,)),
            dma((mine,)),
            dma((2,)),
            dma((2,)),
            dma((2,)),
            dma((half,)),
            dma((mine,)),
            dma((mine,)),
            dma((local, PARTS)),
            dma((local, PARTS)),
            dma((mine,)),
        ],
        compiler_params=pltpu.CompilerParams(collective_id=0, has_side_effects=True),
    )(walkers, inv_intersection, trial, vectors, aux_field, log_weight, copy_list)

    def settle(out_ref, log_ref, o1, o2, flat, sems):
        c1 = pltpu.make_async_copy(out_ref, o1, sems.at[0])
        c1.start()
        for s in range(local):
            flat[s] = jnp.max(log_ref[s:s + 1, :])
        c2 = pltpu.make_async_copy(flat, o2, sems.at[1])
        c2.start()
        c1.wait()
        c2.wait()

    return pl.pallas_call(
        settle,
        out_shape=(jax.ShapeDtypeStruct(walkers.shape, BF16), jax.ShapeDtypeStruct((local,), F32)),
        in_specs=[pl.BlockSpec(memory_space=pltpu.VMEM)] * 2,
        out_specs=(anywhere, anywhere),
        scratch_shapes=[pltpu.SMEM((local,), F32), dma((2,))],
    )(pltpu.with_memory_space_constraint(out, pltpu.VMEM), pltpu.with_memory_space_constraint(out_log, pltpu.VMEM))


def solution(mesh):
    depth, width = mesh.shape["vec"], mesh.shape["walk"]
    assert mesh.shape["orb"] == 2 and depth > 1
    return jax.shard_map(
        functools.partial(per_device, depth, width),
        mesh=mesh,
        in_specs=(
            P(("grp", "walk"), "orb", None),
            P(("grp", "walk"), None, None),
            P(),
            P("vec", "orb", None),
            P(("grp", "walk"), "vec"),
            P(("grp", "walk")),
            P(("grp", "walk")),
        ),
        out_specs=(P(("grp", "walk"), "orb", None), P(("grp", "walk"))),
        check_vma=False,
    )
```

```python
import functools
import math

import jax
import jax.numpy as jnp
from jax import lax
from jax.experimental import pallas as pl
from jax.experimental.pallas import tpu as pltpu
from jax.sharding import PartitionSpec as P

ORDER = 6
BLOCKS = 4
SUB = 1
SKEW = 5
EARLY = 1
PARTS = 1
LOADS = 2
REACH = 3
PLANS = ((2, -1, 1), (3, 2, 1), (3, 2, 1), (2, 1))
MESH = pl.DeviceIdType.MESH
F32 = jnp.float32
BF16 = jnp.bfloat16

step_root = math.sqrt(0.08)


def remote(src, dst, send, recv, where):
    return pltpu.make_async_remote_copy(
        src_ref=src, dst_ref=dst, send_sem=send, recv_sem=recv, device_id=where, device_id_type=MESH
    )


def kernel(
    depth, width,
    walkers_in, inverse_in, trial_in, vectors_in, aux_in, log_in, copies_in,
    out, out_log,
    walkers, inverse, trial, vectors, aux, log_weight, copies,
    green, mixed, strips, level, bias_all, facts, known, picked, partial, leaving, arrived, given, crossed,
    back, extra_in, extra_out, edge, staged, pool, full, terms, result,
    load_sems, copies_send, copies_recv, facts_send, facts_recv, bias_send, bias_recv,
    chain_send, chain_recv, cross_recv, back_recv, swap_send, swap_recv, extra_send, extra_recv, edge_sems,
    stage_send, pool_recv, own_send, next_send, slot_recv, write_sems,
):
    gathered = out
    z = lax.axis_index("vec")
    x = lax.axis_index("walk")
    o = lax.axis_index("orb")
    last = depth - 1
    local, rows, electrons = walkers.shape
    count, _, orbitals = vectors.shape
    half = local // 2
    block = orbitals // 4
    span = 2 * block // count
    wide = count * span
    piece = block // SUB
    each = BLOCKS * SUB
    chunks = half * each
    mine = half // 2
    lanes = extra_in.shape[2]
    insets = [1 if a == half - 1 and last >= REACH else 0 for a in range(half)]
    hops = range(1, width)

    barrier = pltpu.get_barrier_semaphore()

    def greet(where):
        pl.semaphore_signal(barrier, inc=1, device_id=where, device_id_type=MESH)

    greet({"orb": 1 - o})
    for hop in hops:
        for core in range(2):
            greet({"walk": lax.rem(x + hop, width), "orb": core})

    @pl.when(z > 0)
    def _():
        for core in range(2):
            greet({"vec": z - 1, "orb": core})

    @pl.when(z < last)
    def _():
        for core in range(2):
            greet({"vec": z + 1, "orb": core})

    batch = count // LOADS
    pairs = [(trial_in, trial)]
    for n in range(LOADS):
        group = pl.ds(n * batch, batch)
        pairs.append((vectors_in.at[group], vectors.at[group]))
    pairs += [
        (inverse_in, inverse), (walkers_in, walkers), (copies_in, copies.at[x]), (log_in, log_weight), (aux_in, aux),
    ]
    loads = [pltpu.make_async_copy(src, dst, load_sems.at[n]) for n, (src, dst) in enumerate(pairs)]
    for load in loads:
        load.start()

    loads[0].wait()
    for n in range(LOADS):
        loads[1 + n].wait()
        for g in range(n * batch, (n + 1) * batch):
            mixed[g] = jnp.dot(vectors[g], trial[...], preferred_element_type=F32).astype(BF16)
    for load in loads[1 + LOADS:]:
        load.wait()
    for w in range(local):
        green[w] = jnp.dot(walkers[w], inverse[w], preferred_element_type=F32).astype(BF16)
    walker_id = lax.broadcasted_iota(jnp.int32, (local, lanes), 0)
    weights = jnp.zeros((local, lanes), F32)
    for w in range(local):
        weights = jnp.where(walker_id == w, log_weight[w], weights)
    facts[x] = weights
    facts[x, :, 0:count] = aux[...]
    left = [green[:, j * span:(j + 1) * span, :].reshape(local * span, electrons) for j in range(rows // span)]
    right = [mixed[:, j * span:(j + 1) * span, :].reshape(wide, electrons) for j in range(rows // span)]
    gram = lax.dot_general(
        jnp.concatenate(left, axis=1), jnp.concatenate(right, axis=1), (((1,), (1,)), ((), ())), preferred_element_type=F32
    )
    row_id = lax.broadcasted_iota(jnp.int32, (local * span, wide), 0)
    col_id = lax.broadcasted_iota(jnp.int32, (local * span, wide), 1)
    same = row_id % span == col_id % span
    folded = jnp.sum(jnp.where(same, gram, 0.0).reshape(local, span, wide), axis=1)
    lane_id = lax.broadcasted_iota(jnp.int32, (local, wide), 1)
    step = 1
    while step < span:
        low = lane_id % (2 * step) < step
        folded = folded + jnp.where(low, pltpu.roll(folded, wide - step, 1), pltpu.roll(folded, step, 1))
        step *= 2
    lane = lax.broadcasted_iota(jnp.int32, (local, lanes), 1) % span
    fold = span // 2
    bias_all[o, x] = jnp.where(lane < fold, folded[:, :lanes], folded[:, lanes:])

    sides = jnp.where(z > 0, 2, 0) + jnp.where(z < last, 2, 0)
    pl.semaphore_wait(barrier, 1 + 2 * (width - 1) + sides)

    bias_peers = [{"walk": lax.rem(x + hop, width), "orb": core} for hop in hops for core in range(2)] + [{"orb": 1 - o}]
    bias_copies = [
        remote(bias_all.at[o, x], bias_all.at[o, x], bias_send.at[0], bias_recv.at[0], where)
        for n, where in enumerate(bias_peers)
    ]
    def facts_copy(hop, owner):
        return remote(
            facts.at[owner], facts.at[owner], facts_send.at[hop], facts_recv.at[owner], {"walk": lax.rem(x + hop, width)}
        )

    def copies_copy(hop, owner):
        return remote(
            copies.at[owner], copies.at[owner], copies_send.at[hop], copies_recv.at[owner],
            {"walk": lax.rem(x + hop, width)},
        )

    for copy in bias_copies:
        copy.start()
    for hop in hops:
        facts_copy(hop, x).start()
        copies_copy(hop, x).start()

    chunk_row = lax.broadcasted_iota(jnp.int32, (count, span, block), 1)
    chunk_col = lax.broadcasted_iota(jnp.int32, (count, span, block), 2)
    crossing = jnp.zeros((count, span, block), F32)

    def columns(n):
        return pl.ds(pl.multiple_of(n * block, block), block)

    for j in range(block // span):
        here = slice(j * span, (j + 1) * span)
        below = slice(block + j * span, block + (j + 1) * span)
        first = vectors[:, here, columns(2 * o)].astype(F32)
        second = vectors[:, below, columns(1 + 2 * o)].astype(F32)
        crossing = crossing + jnp.where(chunk_row + j * span == chunk_col, second, 0.0)
        joined = jnp.where(chunk_row + j * span <= chunk_col, first, second).astype(BF16)
        strips[j, :, 0:block] = joined.reshape(wide, block)
        strips[j, :, block:2 * block] = vectors[:, here, block:2 * block].reshape(wide, block)
        strips[j, :, 2 * block:3 * block] = vectors[:, here, columns(2 + o)].reshape(wide, block)
        strips[j, :, 3 * block:] = vectors[:, below, columns(3 * (1 - o))].reshape(wide, block)
    level[...] = crossing.reshape(wide, block).astype(BF16)

    for hop in hops:
        facts_copy(hop, lax.rem(x + hop, width)).wait_recv()
    sources = [(copies[x, s] // local, pl.ds(copies[x, s] % local, 1)) for s in range(local)]
    for s, (column, row) in enumerate(sources):
        known[s:s + 1, :] = facts[column, row, :]
    pick_row = lax.broadcasted_iota(jnp.int32, (count, wide), 0)
    pick_col = lax.broadcasted_iota(jnp.int32, (count, wide), 1)
    pick = jnp.where(pick_row == pick_col // span, 1.0, 0.0).astype(F32)
    drawn = jnp.dot(known[:, 0:count], pick, precision=lax.Precision.HIGHEST, preferred_element_type=F32)
    old_log = jnp.broadcast_to(known[:, count:count + 1], (local, lanes))

    tables = partial.at[0, 0, pl.ds(0, (2 * width - 1) * local)]
    bias_done = remote(tables, tables, bias_send.at[0], bias_recv.at[0], {"orb": 1 - o})
    bias_done.wait_recv()

    for s, (column, row) in enumerate(sources):
        picked[s:s + 1, :] = bias_all[0, column, row, :] + bias_all[1, column, row, :]
    both = picked[...]
    bias = jnp.concatenate(
        [jnp.where(lane < fold, both, pltpu.roll(both, fold, 1)), jnp.where(lane < fold, pltpu.roll(both, lanes - fold, 1), both)],
        axis=1,
    )
    shift = -step_root * bias
    field = drawn - shift
    factor = jnp.sum(drawn * shift - 0.5 * shift * shift, axis=1, keepdims=True) * (1.0 / span)
    factor = jnp.broadcast_to(factor, (local, lanes))
    weighted = (field * step_root).astype(BF16)
    spread = jnp.broadcast_to(weighted.astype(F32)[:, None, :], (local, span, wide)).reshape(local * span, wide)
    kron = jnp.where(same, spread, 0.0).astype(BF16)

    def to_next(side):
        return jnp.where(side == 0, z - 1, z + 1)

    upstream = [last - z, z]
    downstream = [z, last - z]
    at_end = (z == 0) | (z == last)
    near = jnp.where(z <= last - z, 0, 1)
    base = near * half
    inward = jnp.where(near == 0, z + 1, z - 1)
    at_owner = [(z == n) | (z == last - n) for n in insets]

    def depth_of(c):
        return sum(jnp.where(c // each == a, n, 0) for a, n in enumerate(insets) if n) + jnp.int32(0)

    def chain_copy(side, c):
        return remote(
            leaving.at[side, c], arrived.at[side, c], chain_send.at[side, c // each], chain_recv.at[side, c], {"vec": to_next(side)}
        )

    def cross_copy(side, c):
        return remote(
            leaving.at[side, c], crossed.at[c], chain_send.at[side, c // each], cross_recv.at[c // (2 * each) * each + c % each], {"vec": to_next(side), "orb": 1 - o}
        )

    def swap_copy(c):
        return remote(leaving.at[near, c], given.at[c], swap_send.at[c // (2 * each)], swap_recv.at[c // (2 * each)], {"orb": 1 - o})

    def extra_copy(side):
        return remote(
            extra_out.at[side], extra_in.at[side], extra_send.at[side], extra_recv.at[side], {"vec": to_next(side)}
        )

    def back_copy(c):
        return remote(
            leaving.at[near, c], back.at[o, c], chain_send.at[near, c // each], back_recv.at[o, c // (2 * each)],
            {"vec": inward, "orb": (c // each) % 2},
        )

    def part_of(side, c):
        at = c % each
        return partial[side * half + c // each, at // SUB, pl.ds(pl.multiple_of((at % SUB) * piece, piece), piece), :]

    def pass_on(side, c, togo):
        here = (c // each) % 2 == o

        @pl.when((togo > 1) | here)
        def _():
            chain_copy(side, c).start()

        @pl.when((togo == 1) & jnp.logical_not(here))
        def _():
            cross_copy(side, c).start()

    pair = BLOCKS // 2
    ahead = pair * SUB
    for n0 in range(0, BLOCKS, pair):
        for j in range(block // span):
            summed = jnp.dot(kron, strips[j, :, n0 * block:(n0 + pair) * block], preferred_element_type=F32)
            for n in range(pair):
                partial[:, n0 + n, j * span:(j + 1) * span, :] = summed[:, n * block:(n + 1) * block].reshape(
                    local, span, block
                )
        if n0 == 0:
            @pl.when(at_end)
            def _():
                for c in range(ahead):
                    leaving[1 - near, c] = part_of(1 - near, c).astype(BF16)
                    pass_on(1 - near, c, last - insets[0])
    edge_part = jnp.dot(weighted, level[...], preferred_element_type=F32)

    def chain_step(t, carry):
        for turn in range(2):
            side = jnp.where(z <= last - z, 1 - turn, turn)
            before = jnp.where(side == 0, last - z, z)
            after = last - before
            c = t - SKEW * before
            head = before == 0
            togo = after - depth_of(c)

            @pl.when((c >= jnp.where(head, ahead, 0)) & (c < chunks) & (togo > 0))
            def _():
                own = part_of(side, c)

                @pl.when(head)
                def _():
                    leaving[side, c] = own.astype(BF16)

                @pl.when(jnp.logical_not(head))
                def _():
                    chain_copy(side, c).wait_recv()
                    leaving[side, c] = (own + arrived[side, c].astype(F32)).astype(BF16)

                pass_on(side, c, togo)

            @pl.when((c == 0) & (after > 0))
            def _():
                @pl.when(head)
                def _():
                    extra_in[side] = jnp.zeros_like(extra_in[side])

                @pl.when(jnp.logical_not(head))
                def _():
                    extra_copy(side).wait_recv()

                extra_out[side, 0:local, :] = extra_in[side, 0:local, :] + factor
                extra_out[side, local:, :] = extra_in[side, local:, :] + edge_part
                extra_copy(side).start()

        return carry

    for hop in hops:
        copies_copy(hop, lax.rem(x + hop, width)).wait_recv()

    def stage_copy(hop, a):
        return remote(
            staged.at[hop, a], pool.at[x, a // 2, o], stage_send.at[a], pool_recv.at[a // 2],
            {"walk": lax.rem(x + hop, width), "orb": a % 2},
        )

    def swap_core():
        return remote(edge.at[o], edge.at[o], edge_sems.at[0], edge_sems.at[1], {"orb": 1 - o})

    def prepare(a):
        @pl.when(at_owner[a])
        def _():
            for hop in range(width):
                source = copies[lax.rem(x + hop, width), base + a]
                held = walkers[source % local]
                if hop > 0:
                    staged[hop, a] = held
                    stage_copy(hop, a).start()
                else:
                    @pl.when(a % 2 == o)
                    def _():
                        pool[x, a // 2, o] = held

                    @pl.when(a % 2 != o)
                    def _():
                        staged[hop, a] = held
                        stage_copy(hop, a).start()

            @pl.when(a % 2 != o)
            def _():
                def give(c, carry):
                    leaving[near, c] = part_of(near, c).astype(BF16)
                    swap_copy(c).start()
                    return carry

                lax.fori_loop(a * each, (a + 1) * each, give, jnp.int32(0))

    def send_back(a):
        @pl.when(at_end)
        def _():
            def back_step(c, carry):
                leaving[near, c] = part_of(near, c).astype(BF16)
                back_copy(c).start()
                return carry

            lax.fori_loop(a * each, (a + 1) * each, back_step, jnp.int32(0))

    for a in range(half):
        if insets[a]:
            prepare(a)

    lax.fori_loop(0, SKEW * (last - 1) + chunks, chain_step, jnp.int32(0))

    for a in range(half):
        if not insets[a]:
            prepare(a)
        else:
            send_back(a)

    for side in range(2):
        @pl.when(at_end & (near == side))
        def _():
            extra_copy(side).wait_recv()

    owning = functools.reduce(jnp.logical_or, at_owner)

    @pl.when(owning)
    def _():
        edge[o] = edge_part + extra_in[0, local:, :] + extra_in[1, local:, :]
        swap_core().start()
        swap_core().wait_recv()

    share = rows // PARTS
    short = last <= REACH
    plans = [
        tuple(n for n in PLANS[min(half - a, len(PLANS)) - 1] if -insets[a] <= n <= last - insets[a])
        if short else (1,) + (-1,) * insets[a] for a in range(half)
    ]

    def passes(a, away):
        if not short:
            return (away > 0) & (away < last - insets[a])
        gaps = [away == n for n in range(1, last - insets[a]) if n + 1 not in plans[a]]
        return functools.reduce(jnp.logical_or, gaps, jnp.bool_(False))

    def place(w, part):
        return gathered.at[w, pl.ds(part * share, share)]

    def away_z(n):
        return jnp.where(near == 0, z + n, z - n)

    def spread_copies(a):
        w = base + a
        targets = []
        for n in plans[a]:
            for core in (1 - a % 2, a % 2):
                targets.append((core, {"vec": away_z(n), "orb": core}))
        targets.append((1 - a % 2, {"orb": 1 - o}))
        return [
            remote(
                result.at[a // 2, core, pl.ds(part * share, share)], place(w, part),
                own_send.at[a // 2], slot_recv.at[w, part], where,
            )
            for n, (core, where) in enumerate(targets)
            for part in range(PARTS)
        ]

    upper = lax.broadcasted_iota(jnp.int32, (block, block), 0) < lax.broadcasted_iota(jnp.int32, (block, block), 1)
    level_mask = lax.broadcasted_iota(jnp.int32, (block, block), 0) == lax.broadcasted_iota(jnp.int32, (block, block), 1)

    def finish(a):
        w = base + a
        i = a // 2

        def put(r, c, value):
            full[columns(r), columns(c)] = value

        come = gathered.at[pl.ds(0, 2 * width - 1)]
        remote(come, come, stage_send.at[0], pool_recv.at[i], {"orb": 1 - o}).wait_recv()
        column = copies[x, w] // local
        for core in range(2):
            start = pool[0, i, core]
            for other in hops:
                start = jnp.where(column == other, pool[other, i, core], start)
            terms[0, :, core * rows:(core + 1) * rows] = start.T
        whole = pl.ds(a * each, each)
        remote(leaving.at[near, whole], given.at[whole], swap_send.at[i], swap_recv.at[i], {"orb": 1 - o}).wait_recv()
        if insets[a]:
            for core in range(2):
                remote(
                    leaving.at[near, whole], back.at[core, whole], chain_send.at[near, a], back_recv.at[core, i],
                    {"vec": inward, "orb": core},
                ).wait_recv()
        for n in range(BLOCKS):
            first_c = a * each + n * SUB
            for c in range(first_c, first_c + SUB):
                remote(
                    leaving.at[near, c], arrived.at[near, c], chain_send.at[near, c // each], chain_recv.at[near, c], {"vec": inward}
                ).wait_recv()
                remote(
                    leaving.at[near, c], crossed.at[c], chain_send.at[near, c // each], cross_recv.at[c // (2 * each) * each + c % each],
                    {"vec": inward, "orb": 1 - o},
                ).wait_recv()
            run = pl.ds(first_c, SUB)
            kept = partial[w, n] + arrived[near, run].reshape(block, block).astype(F32)
            taken = given[run].reshape(block, block).astype(F32) + crossed[run].reshape(block, block).astype(F32)
            if insets[a]:
                kept = kept + back[o, run].reshape(block, block).astype(F32)
                taken = taken + back[1 - o, run].reshape(block, block).astype(F32)
            for core, value in ((o, kept), (1 - o, taken)):
                if n == 0:
                    flipped = value.T
                    line = edge[core, pl.ds(w, 1), :]
                    put(2 * core, 2 * core, jnp.where(upper | level_mask, value, flipped).astype(BF16))
                    low = jnp.where(level_mask, jnp.broadcast_to(line, (block, block)), jnp.where(upper, flipped, value))
                    put(2 * core + 1, 2 * core + 1, low.astype(BF16))
                else:
                    r, k = ((2 * core, 1), (2 * core, 2 + core), (2 * core + 1, 3 * (1 - core)))[n - 1]
                    value = value.astype(BF16)
                    put(r, k, value)
                    put(k, r, value.T)

        for degree in range(1, ORDER + 1):
            fresh = (jnp.dot(terms[degree - 1], full[...], preferred_element_type=F32) * (1.0 / degree)).astype(BF16)
            terms[degree] = fresh
        running = terms[0].astype(F32)
        for degree in range(1, ORDER + 1):
            running = running + terms[degree].astype(F32)
        result[i] = running.astype(BF16).T.reshape(2, rows, electrons)
        for copy in spread_copies(a):
            copy.start()
        settle = pltpu.make_async_copy(result.at[i, o], gathered.at[w], write_sems.at[i])
        settle.start()

    def onward(w, part, hop_to):
        spot = place(w, part)
        return remote(spot, spot, next_send.at[w % half if short else w, part], slot_recv.at[w, part], {"vec": hop_to})

    def route(side, a):
        w = side * half + a
        away = jnp.where(side == 0, z, last - z) - insets[a]
        hop_to = jnp.where(side == 0, z + 1, z - 1)
        return w, away, hop_to

    def forward(slots):
        for a in slots:
            for side in (near, 1 - near):
                w, away, hop_to = route(side, a)

                @pl.when(passes(a, away))
                def _():
                    for part in range(PARTS):
                        onward(w, part, hop_to).wait_recv()
                        onward(w, part, hop_to).start()

    early = [a for a in range(half) if short and a < EARLY]
    forward(early)
    for a in range(half):
        @pl.when(at_owner[a] & (a % 2 == o))
        def _():
            finish(a)

    new_log = old_log + factor + extra_in[0, 0:local, :] + extra_in[1, 0:local, :]
    out_log[...] = new_log

    forward([a for a in range(half) if a not in early])

    bias_done.wait_send()
    for hop in hops:
        facts_copy(hop, x).wait_send()
        copies_copy(hop, x).wait_send()

    def sent(side, a):
        whole = pl.ds(a * each, each)
        return remote(
            leaving.at[side, whole], arrived.at[side, whole], chain_send.at[side, a], chain_recv.at[side, a], {"orb": 1 - o}
        )

    for side in range(2):
        for a in range(half):
            @pl.when(downstream[side] - insets[a] != 0)
            def _():
                sent(side, a).wait_send()

    for side in range(2):
        @pl.when(downstream[side] > 0)
        def _():
            extra_copy(side).wait_send()

    @pl.when(owning)
    def _():
        swap_core().wait_send()

    for a in range(half):
        @pl.when(at_owner[a])
        def _():
            def moved(n):
                run = gathered.at[pl.ds(0, n)]
                return remote(run, run, stage_send.at[a], slot_recv.at[0, 0], {"orb": 1 - o})

            @pl.when(a % 2 == o)
            def _():
                moved(width - 1).wait_send()

            @pl.when(a % 2 != o)
            def _():
                moved(width).wait_send()

                whole = pl.ds(a * each, each)
                remote(
                    leaving.at[near, whole], given.at[whole], swap_send.at[a // 2], swap_recv.at[a // 2], {"orb": 1 - o}
                ).wait_send()

    for a in range(half):
        for side in (near, 1 - near):
            w, away, hop_to = route(side, a)

            @pl.when(((away != 0) | (o != a % 2)) & jnp.logical_not(passes(a, away)))
            def _():
                for part in range(PARTS):
                    onward(w, part, hop_to).wait_recv()

    for a in range(half):
        @pl.when(at_owner[a] & (a % 2 == o))
        def _():
            run = gathered.at[pl.ds(0, 2 * len(plans[a]) + 1)]
            remote(run, run, own_send.at[a // 2], slot_recv.at[0, 0], {"orb": 1 - o}).wait_send()
            pltpu.make_async_copy(result.at[a // 2, o], gathered.at[base + a], write_sems.at[a // 2]).wait()

    for a in range(half):
        for side in range(2):
            w, away, hop_to = route(side, a)

            @pl.when(passes(a, away))
            def _():
                for part in range(PARTS):
                    onward(w, part, hop_to).wait_send()


def per_device(depth, width, walkers, inv_intersection, trial, vectors, aux_field, log_weight, copy_list):
    local, rows, electrons = walkers.shape
    count, _, orbitals = vectors.shape
    half = local // 2
    block = orbitals // 4
    span = 2 * block // count
    wide = count * span
    piece = block // SUB
    chunks = half * BLOCKS * SUB
    mine = half // 2
    lanes = 128
    dma = pltpu.SemaphoreType.DMA
    anywhere = pl.BlockSpec(memory_space=pl.ANY)
    out, out_log = pl.pallas_call(
        functools.partial(kernel, depth, width),
        out_shape=(
            pltpu.VMEM(walkers.shape, BF16),
            pltpu.VMEM((local, 128), F32),
        ),
        in_specs=[anywhere] * 7,
        out_specs=(anywhere, pl.BlockSpec(memory_space=pltpu.VMEM)),
        scratch_shapes=[
            pltpu.VMEM(walkers.shape, BF16),
            pltpu.VMEM(inv_intersection.shape, BF16),
            pltpu.VMEM(trial.shape, BF16),
            pltpu.VMEM(vectors.shape, BF16),
            pltpu.VMEM(aux_field.shape, F32),
            pltpu.SMEM((local,), F32),
            pltpu.SMEM((width, local), jnp.int32),
            pltpu.VMEM((local, rows, electrons), BF16),
            pltpu.VMEM((count, rows, electrons), BF16),
            pltpu.VMEM((block // span, wide, BLOCKS * block), BF16),
            pltpu.VMEM((wide, block), BF16),
            pltpu.VMEM((2, width, local, lanes), F32),
            pltpu.VMEM((width, local, lanes), F32),
            pltpu.VMEM((local, lanes), F32),
            pltpu.VMEM((local, lanes), F32),
            pltpu.VMEM((local, BLOCKS, block, block), F32),
            pltpu.VMEM((2, chunks, piece, block), BF16),
            pltpu.VMEM((2, chunks, piece, block), BF16),
            pltpu.VMEM((chunks, piece, block), BF16),
            pltpu.VMEM((chunks, piece, block), BF16),
            pltpu.VMEM((2, chunks, piece, block), BF16),
            pltpu.VMEM((2, 2 * local, lanes), F32),
            pltpu.VMEM((2, 2 * local, lanes), F32),
            pltpu.VMEM((2, local, lanes), F32),
            pltpu.VMEM((width, half, rows, electrons), BF16),
            pltpu.VMEM((width, mine, 2, rows, electrons), BF16),
            pltpu.VMEM((orbitals, orbitals), BF16),
            pltpu.VMEM((ORDER + 1, electrons, orbitals), BF16),
            pltpu.VMEM((mine, 2, rows, electrons), BF16),
            dma((6 + LOADS,)),
            dma((width,)),
            dma((width,)),
            dma((width,)),
            dma((width,)),
            dma((1,)),
            dma((1,)),
            dma((2, half)),
            dma((2, chunks)),
            dma((chunks // 2,)),
            dma((2, mine)),
            dma((mine,)),
            dma((mine,)),
            dma((2,)),
            dma((2,)),
            dma((2,)),
            dma((half,)),
            dma((mine,)),
            dma((mine,)),
            dma((half if depth - 1 <= REACH else local, PARTS)),
            dma((local, PARTS)),
            dma((mine,)),
        ],
        compiler_params=pltpu.CompilerParams(collective_id=0, has_side_effects=True),
    )(walkers, inv_intersection, trial, vectors, aux_field, log_weight, copy_list)

    def settle(out_ref, log_ref, o1, o2, flat, sems):
        c1 = pltpu.make_async_copy(out_ref, o1, sems.at[0])
        c1.start()
        for s in range(local):
            flat[s] = jnp.max(log_ref[s:s + 1, :])
        c2 = pltpu.make_async_copy(flat, o2, sems.at[1])
        c2.start()
        c1.wait()
        c2.wait()

    return pl.pallas_call(
        settle,
        out_shape=(jax.ShapeDtypeStruct(walkers.shape, BF16), jax.ShapeDtypeStruct((local,), F32)),
        in_specs=[pl.BlockSpec(memory_space=pltpu.VMEM)] * 2,
        out_specs=(anywhere, anywhere),
        scratch_shapes=[pltpu.SMEM((local,), F32), dma((2,))],
    )(pltpu.with_memory_space_constraint(out, pltpu.VMEM), pltpu.with_memory_space_constraint(out_log, pltpu.VMEM))


def solution(mesh):
    depth, width = mesh.shape["vec"], mesh.shape["walk"]
    assert mesh.shape["orb"] == 2 and depth > 1
    return jax.shard_map(
        functools.partial(per_device, depth, width),
        mesh=mesh,
        in_specs=(
            P(("grp", "walk"), "orb", None),
            P(("grp", "walk"), None, None),
            P(),
            P("vec", "orb", None),
            P(("grp", "walk"), "vec"),
            P(("grp", "walk")),
            P(("grp", "walk")),
        ),
        out_specs=(P(("grp", "walk"), "orb", None), P(("grp", "walk"))),
        check_vma=False,
    )
```

```python
import functools
import math

import jax
import jax.numpy as jnp
from jax import lax
from jax.experimental import pallas as pl
from jax.experimental.pallas import tpu as pltpu
from jax.sharding import PartitionSpec as P

ORDER = 6
BLOCKS = 4
SUB = 1
SKEW = 5
EARLY = 1
PARTS = 1
LOADS = 2
REACH = 3
PLANS = ((2, -1, 1), (3, 2, 1), (3, 1), (2, 1))
MESH = pl.DeviceIdType.MESH
F32 = jnp.float32
BF16 = jnp.bfloat16

step_root = math.sqrt(0.08)


def remote(src, dst, send, recv, where):
    return pltpu.make_async_remote_copy(
        src_ref=src, dst_ref=dst, send_sem=send, recv_sem=recv, device_id=where, device_id_type=MESH
    )


def kernel(
    depth, width,
    walkers_in, inverse_in, trial_in, vectors_in, aux_in, log_in, copies_in,
    out, out_log,
    walkers, inverse, trial, vectors, aux, log_weight, copies,
    green, mixed, strips, level, bias_all, facts, known, picked, partial, leaving, arrived, given, crossed,
    back, extra_in, extra_out, edge, staged, pool, full, terms, result,
    load_sems, copies_send, copies_recv, facts_send, facts_recv, bias_send, bias_recv,
    chain_send, chain_recv, cross_recv, back_recv, swap_send, swap_recv, extra_send, extra_recv, edge_sems,
    stage_send, pool_recv, own_send, next_send, slot_recv, write_sems,
):
    gathered = out
    z = lax.axis_index("vec")
    x = lax.axis_index("walk")
    o = lax.axis_index("orb")
    last = depth - 1
    local, rows, electrons = walkers.shape
    count, _, orbitals = vectors.shape
    half = local // 2
    block = orbitals // 4
    span = 2 * block // count
    wide = count * span
    piece = block // SUB
    each = BLOCKS * SUB
    chunks = half * each
    mine = half // 2
    lanes = extra_in.shape[2]
    insets = [1 if a == half - 1 and last >= REACH else 0 for a in range(half)]
    hops = range(1, width)

    barrier = pltpu.get_barrier_semaphore()

    def greet(where):
        pl.semaphore_signal(barrier, inc=1, device_id=where, device_id_type=MESH)

    greet({"orb": 1 - o})
    for hop in hops:
        for core in range(2):
            greet({"walk": lax.rem(x + hop, width), "orb": core})

    @pl.when(z > 0)
    def _():
        for core in range(2):
            greet({"vec": z - 1, "orb": core})

    @pl.when(z < last)
    def _():
        for core in range(2):
            greet({"vec": z + 1, "orb": core})

    batch = count // LOADS
    pairs = [(trial_in, trial)]
    for n in range(LOADS):
        group = pl.ds(n * batch, batch)
        pairs.append((vectors_in.at[group], vectors.at[group]))
    pairs += [
        (inverse_in, inverse), (walkers_in, walkers), (copies_in, copies.at[x]), (log_in, log_weight), (aux_in, aux),
    ]
    loads = [pltpu.make_async_copy(src, dst, load_sems.at[n]) for n, (src, dst) in enumerate(pairs)]
    for load in loads:
        load.start()

    loads[0].wait()
    for n in range(LOADS):
        loads[1 + n].wait()
        for g in range(n * batch, (n + 1) * batch):
            mixed[g] = jnp.dot(vectors[g], trial[...], preferred_element_type=F32).astype(BF16)
    for load in loads[1 + LOADS:]:
        load.wait()
    for w in range(local):
        green[w] = jnp.dot(walkers[w], inverse[w], preferred_element_type=F32).astype(BF16)
    walker_id = lax.broadcasted_iota(jnp.int32, (local, lanes), 0)
    weights = jnp.zeros((local, lanes), F32)
    for w in range(local):
        weights = jnp.where(walker_id == w, log_weight[w], weights)
    facts[x] = weights
    facts[x, :, 0:count] = aux[...]
    left = [green[:, j * span:(j + 1) * span, :].reshape(local * span, electrons) for j in range(rows // span)]
    right = [mixed[:, j * span:(j + 1) * span, :].reshape(wide, electrons) for j in range(rows // span)]
    gram = lax.dot_general(
        jnp.concatenate(left, axis=1), jnp.concatenate(right, axis=1), (((1,), (1,)), ((), ())), preferred_element_type=F32
    )
    row_id = lax.broadcasted_iota(jnp.int32, (local * span, wide), 0)
    col_id = lax.broadcasted_iota(jnp.int32, (local * span, wide), 1)
    same = row_id % span == col_id % span
    folded = jnp.sum(jnp.where(same, gram, 0.0).reshape(local, span, wide), axis=1)
    lane_id = lax.broadcasted_iota(jnp.int32, (local, wide), 1)
    step = 1
    while step < span:
        low = lane_id % (2 * step) < step
        folded = folded + jnp.where(low, pltpu.roll(folded, wide - step, 1), pltpu.roll(folded, step, 1))
        step *= 2
    lane = lax.broadcasted_iota(jnp.int32, (local, lanes), 1) % span
    fold = span // 2
    bias_all[o, x] = jnp.where(lane < fold, folded[:, :lanes], folded[:, lanes:])

    sides = jnp.where(z > 0, 2, 0) + jnp.where(z < last, 2, 0)
    pl.semaphore_wait(barrier, 1 + 2 * (width - 1) + sides)

    bias_peers = [{"walk": lax.rem(x + hop, width), "orb": core} for hop in hops for core in range(2)] + [{"orb": 1 - o}]
    bias_copies = [
        remote(bias_all.at[o, x], bias_all.at[o, x], bias_send.at[n], bias_recv.at[o, x], where)
        for n, where in enumerate(bias_peers)
    ]
    def facts_copy(hop, owner):
        return remote(
            facts.at[owner], facts.at[owner], facts_send.at[hop], facts_recv.at[owner], {"walk": lax.rem(x + hop, width)}
        )

    def copies_copy(hop, owner):
        return remote(
            copies.at[owner], copies.at[owner], copies_send.at[hop], copies_recv.at[owner],
            {"walk": lax.rem(x + hop, width)},
        )

    for copy in bias_copies:
        copy.start()
    for hop in hops:
        facts_copy(hop, x).start()
        copies_copy(hop, x).start()

    chunk_row = lax.broadcasted_iota(jnp.int32, (count, span, block), 1)
    chunk_col = lax.broadcasted_iota(jnp.int32, (count, span, block), 2)
    crossing = jnp.zeros((count, span, block), F32)

    def columns(n):
        return pl.ds(pl.multiple_of(n * block, block), block)

    for j in range(block // span):
        here = slice(j * span, (j + 1) * span)
        below = slice(block + j * span, block + (j + 1) * span)
        first = vectors[:, here, columns(2 * o)].astype(F32)
        second = vectors[:, below, columns(1 + 2 * o)].astype(F32)
        crossing = crossing + jnp.where(chunk_row + j * span == chunk_col, second, 0.0)
        joined = jnp.where(chunk_row + j * span <= chunk_col, first, second).astype(BF16)
        strips[j, :, 0:block] = joined.reshape(wide, block)
        strips[j, :, block:2 * block] = vectors[:, here, block:2 * block].reshape(wide, block)
        strips[j, :, 2 * block:3 * block] = vectors[:, here, columns(2 + o)].reshape(wide, block)
        strips[j, :, 3 * block:] = vectors[:, below, columns(3 * (1 - o))].reshape(wide, block)
    level[...] = crossing.reshape(wide, block).astype(BF16)

    for hop in hops:
        facts_copy(hop, lax.rem(x + hop, width)).wait_recv()
    sources = [(copies[x, s] // local, pl.ds(copies[x, s] % local, 1)) for s in range(local)]
    for s, (column, row) in enumerate(sources):
        known[s:s + 1, :] = facts[column, row, :]
    pick_row = lax.broadcasted_iota(jnp.int32, (count, wide), 0)
    pick_col = lax.broadcasted_iota(jnp.int32, (count, wide), 1)
    pick = jnp.where(pick_row == pick_col // span, 1.0, 0.0).astype(F32)
    drawn = jnp.dot(known[:, 0:count], pick, precision=lax.Precision.HIGHEST, preferred_element_type=F32)
    old_log = jnp.broadcast_to(known[:, count:count + 1], (local, lanes))

    for hop in hops:
        other = lax.rem(x + hop, width)
        for core in range(2):
            remote(
                bias_all.at[core, other], bias_all.at[core, other], bias_send.at[0], bias_recv.at[core, other], {"walk": other}
            ).wait_recv()
    remote(bias_all.at[1 - o, x], bias_all.at[1 - o, x], bias_send.at[0], bias_recv.at[1 - o, x], {"orb": 1 - o}).wait_recv()

    for s, (column, row) in enumerate(sources):
        picked[s:s + 1, :] = bias_all[0, column, row, :] + bias_all[1, column, row, :]
    both = picked[...]
    bias = jnp.concatenate(
        [jnp.where(lane < fold, both, pltpu.roll(both, fold, 1)), jnp.where(lane < fold, pltpu.roll(both, lanes - fold, 1), both)],
        axis=1,
    )
    shift = -step_root * bias
    field = drawn - shift
    factor = jnp.sum(drawn * shift - 0.5 * shift * shift, axis=1, keepdims=True) * (1.0 / span)
    factor = jnp.broadcast_to(factor, (local, lanes))
    weighted = (field * step_root).astype(BF16)
    spread = jnp.broadcast_to(weighted.astype(F32)[:, None, :], (local, span, wide)).reshape(local * span, wide)
    kron = jnp.where(same, spread, 0.0).astype(BF16)

    def to_next(side):
        return jnp.where(side == 0, z - 1, z + 1)

    upstream = [last - z, z]
    downstream = [z, last - z]
    at_end = (z == 0) | (z == last)
    near = jnp.where(z <= last - z, 0, 1)
    base = near * half
    inward = jnp.where(near == 0, z + 1, z - 1)
    at_owner = [(z == n) | (z == last - n) for n in insets]

    def depth_of(c):
        return sum(jnp.where(c // each == a, n, 0) for a, n in enumerate(insets) if n) + jnp.int32(0)

    def chain_copy(side, c):
        return remote(
            leaving.at[side, c], arrived.at[side, c], chain_send.at[side, c // each], chain_recv.at[side, c], {"vec": to_next(side)}
        )

    def cross_copy(side, c):
        return remote(
            leaving.at[side, c], crossed.at[c], chain_send.at[side, c // each], cross_recv.at[c // (2 * each) * each + c % each], {"vec": to_next(side), "orb": 1 - o}
        )

    def swap_copy(c):
        return remote(leaving.at[near, c], given.at[c], swap_send.at[c // (2 * each)], swap_recv.at[c // (2 * each)], {"orb": 1 - o})

    def extra_copy(side):
        return remote(
            extra_out.at[side], extra_in.at[side], extra_send.at[side], extra_recv.at[side], {"vec": to_next(side)}
        )

    def back_copy(c):
        return remote(
            leaving.at[near, c], back.at[o, c], chain_send.at[near, c // each], back_recv.at[o, c // (2 * each)],
            {"vec": inward, "orb": (c // each) % 2},
        )

    def part_of(side, c):
        at = c % each
        return partial[side * half + c // each, at // SUB, pl.ds(pl.multiple_of((at % SUB) * piece, piece), piece), :]

    def pass_on(side, c, togo):
        here = (c // each) % 2 == o

        @pl.when((togo > 1) | here)
        def _():
            chain_copy(side, c).start()

        @pl.when((togo == 1) & jnp.logical_not(here))
        def _():
            cross_copy(side, c).start()

    pair = BLOCKS // 2
    ahead = pair * SUB
    for n0 in range(0, BLOCKS, pair):
        for j in range(block // span):
            summed = jnp.dot(kron, strips[j, :, n0 * block:(n0 + pair) * block], preferred_element_type=F32)
            for n in range(pair):
                partial[:, n0 + n, j * span:(j + 1) * span, :] = summed[:, n * block:(n + 1) * block].reshape(
                    local, span, block
                )
        if n0 == 0:
            @pl.when(at_end)
            def _():
                for c in range(ahead):
                    leaving[1 - near, c] = part_of(1 - near, c).astype(BF16)
                    pass_on(1 - near, c, last - insets[0])
    edge_part = jnp.dot(weighted, level[...], preferred_element_type=F32)

    def chain_step(t, carry):
        for turn in range(2):
            side = jnp.where(z <= last - z, 1 - turn, turn)
            before = jnp.where(side == 0, last - z, z)
            after = last - before
            c = t - SKEW * before
            head = before == 0
            togo = after - depth_of(c)

            @pl.when((c >= jnp.where(head, ahead, 0)) & (c < chunks) & (togo > 0))
            def _():
                own = part_of(side, c)

                @pl.when(head)
                def _():
                    leaving[side, c] = own.astype(BF16)

                @pl.when(jnp.logical_not(head))
                def _():
                    chain_copy(side, c).wait_recv()
                    leaving[side, c] = (own + arrived[side, c].astype(F32)).astype(BF16)

                pass_on(side, c, togo)

            @pl.when((c == 0) & (after > 0))
            def _():
                @pl.when(head)
                def _():
                    extra_in[side] = jnp.zeros_like(extra_in[side])

                @pl.when(jnp.logical_not(head))
                def _():
                    extra_copy(side).wait_recv()

                extra_out[side, 0:local, :] = extra_in[side, 0:local, :] + factor
                extra_out[side, local:, :] = extra_in[side, local:, :] + edge_part
                extra_copy(side).start()

        return carry

    for hop in hops:
        copies_copy(hop, lax.rem(x + hop, width)).wait_recv()

    def stage_copy(hop, a):
        return remote(
            staged.at[hop, a], pool.at[x, a // 2, o], stage_send.at[a], pool_recv.at[a // 2],
            {"walk": lax.rem(x + hop, width), "orb": a % 2},
        )

    def swap_core():
        return remote(edge.at[o], edge.at[o], edge_sems.at[0], edge_sems.at[1], {"orb": 1 - o})

    def prepare(a):
        @pl.when(at_owner[a])
        def _():
            for hop in range(width):
                source = copies[lax.rem(x + hop, width), base + a]
                held = walkers[source % local]
                if hop > 0:
                    staged[hop, a] = held
                    stage_copy(hop, a).start()
                else:
                    @pl.when(a % 2 == o)
                    def _():
                        pool[x, a // 2, o] = held

                    @pl.when(a % 2 != o)
                    def _():
                        staged[hop, a] = held
                        stage_copy(hop, a).start()

            @pl.when(a % 2 != o)
            def _():
                def give(c, carry):
                    leaving[near, c] = part_of(near, c).astype(BF16)
                    swap_copy(c).start()
                    return carry

                lax.fori_loop(a * each, (a + 1) * each, give, jnp.int32(0))

    def send_back(a):
        @pl.when(at_end)
        def _():
            def back_step(c, carry):
                leaving[near, c] = part_of(near, c).astype(BF16)
                back_copy(c).start()
                return carry

            lax.fori_loop(a * each, (a + 1) * each, back_step, jnp.int32(0))

    for a in range(half):
        if insets[a]:
            prepare(a)

    lax.fori_loop(0, SKEW * (last - 1) + chunks, chain_step, jnp.int32(0))

    for a in range(half):
        if not insets[a]:
            prepare(a)
        else:
            send_back(a)

    for side in range(2):
        @pl.when(at_end & (near == side))
        def _():
            extra_copy(side).wait_recv()

    owning = functools.reduce(jnp.logical_or, at_owner)

    @pl.when(owning)
    def _():
        edge[o] = edge_part + extra_in[0, local:, :] + extra_in[1, local:, :]
        swap_core().start()
        swap_core().wait_recv()

    share = rows // PARTS
    short = last <= REACH
    plans = [
        tuple(n for n in PLANS[min(half - a, len(PLANS)) - 1] if -insets[a] <= n <= last - insets[a])
        if short else (1,) + (-1,) * insets[a] for a in range(half)
    ]

    def passes(a, away):
        if not short:
            return (away > 0) & (away < last - insets[a])
        gaps = [away == n for n in range(1, last - insets[a]) if n + 1 not in plans[a]]
        return functools.reduce(jnp.logical_or, gaps, jnp.bool_(False))

    def place(w, part):
        return gathered.at[w, pl.ds(part * share, share)]

    def away_z(n):
        return jnp.where(near == 0, z + n, z - n)

    def spread_copies(a):
        w = base + a
        targets = []
        for n in plans[a]:
            for core in (1 - a % 2, a % 2):
                targets.append((core, {"vec": away_z(n), "orb": core}))
        targets.append((1 - a % 2, {"orb": 1 - o}))
        return [
            remote(
                result.at[a // 2, core, pl.ds(part * share, share)], place(w, part),
                own_send.at[a // 2], slot_recv.at[w, part], where,
            )
            for n, (core, where) in enumerate(targets)
            for part in range(PARTS)
        ]

    upper = lax.broadcasted_iota(jnp.int32, (block, block), 0) < lax.broadcasted_iota(jnp.int32, (block, block), 1)
    level_mask = lax.broadcasted_iota(jnp.int32, (block, block), 0) == lax.broadcasted_iota(jnp.int32, (block, block), 1)

    def finish(a):
        w = base + a
        i = a // 2

        def put(r, c, value):
            full[columns(r), columns(c)] = value

        come = gathered.at[pl.ds(0, 2 * width - 1)]
        remote(come, come, stage_send.at[0], pool_recv.at[i], {"orb": 1 - o}).wait_recv()
        column = copies[x, w] // local
        for core in range(2):
            start = pool[0, i, core]
            for other in hops:
                start = jnp.where(column == other, pool[other, i, core], start)
            terms[0, :, core * rows:(core + 1) * rows] = start.T
        whole = pl.ds(a * each, each)
        remote(leaving.at[near, whole], given.at[whole], swap_send.at[i], swap_recv.at[i], {"orb": 1 - o}).wait_recv()
        if insets[a]:
            for core in range(2):
                remote(
                    leaving.at[near, whole], back.at[core, whole], chain_send.at[near, a], back_recv.at[core, i],
                    {"vec": inward, "orb": core},
                ).wait_recv()
        for n in range(BLOCKS):
            first_c = a * each + n * SUB
            for c in range(first_c, first_c + SUB):
                remote(
                    leaving.at[near, c], arrived.at[near, c], chain_send.at[near, c // each], chain_recv.at[near, c], {"vec": inward}
                ).wait_recv()
                remote(
                    leaving.at[near, c], crossed.at[c], chain_send.at[near, c // each], cross_recv.at[c // (2 * each) * each + c % each],
                    {"vec": inward, "orb": 1 - o},
                ).wait_recv()
            run = pl.ds(first_c, SUB)
            kept = partial[w, n] + arrived[near, run].reshape(block, block).astype(F32)
            taken = given[run].reshape(block, block).astype(F32) + crossed[run].reshape(block, block).astype(F32)
            if insets[a]:
                kept = kept + back[o, run].reshape(block, block).astype(F32)
                taken = taken + back[1 - o, run].reshape(block, block).astype(F32)
            for core, value in ((o, kept), (1 - o, taken)):
                if n == 0:
                    flipped = value.T
                    line = edge[core, pl.ds(w, 1), :]
                    put(2 * core, 2 * core, jnp.where(upper | level_mask, value, flipped).astype(BF16))
                    low = jnp.where(level_mask, jnp.broadcast_to(line, (block, block)), jnp.where(upper, flipped, value))
                    put(2 * core + 1, 2 * core + 1, low.astype(BF16))
                else:
                    r, k = ((2 * core, 1), (2 * core, 2 + core), (2 * core + 1, 3 * (1 - core)))[n - 1]
                    value = value.astype(BF16)
                    put(r, k, value)
                    put(k, r, value.T)

        for degree in range(1, ORDER + 1):
            fresh = (jnp.dot(terms[degree - 1], full[...], preferred_element_type=F32) * (1.0 / degree)).astype(BF16)
            terms[degree] = fresh
        running = terms[0].astype(F32)
        for degree in range(1, ORDER + 1):
            running = running + terms[degree].astype(F32)
        result[i] = running.astype(BF16).T.reshape(2, rows, electrons)
        for copy in spread_copies(a):
            copy.start()
        settle = pltpu.make_async_copy(result.at[i, o], gathered.at[w], write_sems.at[i])
        settle.start()

    def onward(w, part, hop_to):
        spot = place(w, part)
        return remote(spot, spot, next_send.at[w, part], slot_recv.at[w, part], {"vec": hop_to})

    def route(side, a):
        w = side * half + a
        away = jnp.where(side == 0, z, last - z) - insets[a]
        hop_to = jnp.where(side == 0, z + 1, z - 1)
        return w, away, hop_to

    def forward(slots):
        for a in slots:
            for side in (near, 1 - near):
                w, away, hop_to = route(side, a)

                @pl.when(passes(a, away))
                def _():
                    for part in range(PARTS):
                        onward(w, part, hop_to).wait_recv()
                        onward(w, part, hop_to).start()

    early = [a for a in range(half) if short and a < EARLY]
    forward(early)
    for a in range(half):
        @pl.when(at_owner[a] & (a % 2 == o))
        def _():
            finish(a)

    new_log = old_log + factor + extra_in[0, 0:local, :] + extra_in[1, 0:local, :]
    out_log[...] = new_log

    forward([a for a in range(half) if a not in early])

    for copy in bias_copies:
        copy.wait_send()
    for hop in hops:
        facts_copy(hop, x).wait_send()
        copies_copy(hop, x).wait_send()

    def sent(side, a):
        whole = pl.ds(a * each, each)
        return remote(
            leaving.at[side, whole], arrived.at[side, whole], chain_send.at[side, a], chain_recv.at[side, a], {"orb": 1 - o}
        )

    for side in range(2):
        for a in range(half):
            @pl.when(downstream[side] - insets[a] != 0)
            def _():
                sent(side, a).wait_send()

    for side in range(2):
        @pl.when(downstream[side] > 0)
        def _():
            extra_copy(side).wait_send()

    @pl.when(owning)
    def _():
        swap_core().wait_send()

    for a in range(half):
        @pl.when(at_owner[a])
        def _():
            def moved(n):
                run = gathered.at[pl.ds(0, n)]
                return remote(run, run, stage_send.at[a], slot_recv.at[0, 0], {"orb": 1 - o})

            @pl.when(a % 2 == o)
            def _():
                moved(width - 1).wait_send()

            @pl.when(a % 2 != o)
            def _():
                moved(width).wait_send()

                whole = pl.ds(a * each, each)
                remote(
                    leaving.at[near, whole], given.at[whole], swap_send.at[a // 2], swap_recv.at[a // 2], {"orb": 1 - o}
                ).wait_send()

    for a in range(half):
        for side in (near, 1 - near):
            w, away, hop_to = route(side, a)

            @pl.when(((away != 0) | (o != a % 2)) & jnp.logical_not(passes(a, away)))
            def _():
                for part in range(PARTS):
                    onward(w, part, hop_to).wait_recv()

    for a in range(half):
        @pl.when(at_owner[a] & (a % 2 == o))
        def _():
            run = gathered.at[pl.ds(0, 2 * len(plans[a]) + 1)]
            remote(run, run, own_send.at[a // 2], slot_recv.at[0, 0], {"orb": 1 - o}).wait_send()
            pltpu.make_async_copy(result.at[a // 2, o], gathered.at[base + a], write_sems.at[a // 2]).wait()

    for a in range(half):
        for side in range(2):
            w, away, hop_to = route(side, a)

            @pl.when(passes(a, away))
            def _():
                for part in range(PARTS):
                    onward(w, part, hop_to).wait_send()


def per_device(depth, width, walkers, inv_intersection, trial, vectors, aux_field, log_weight, copy_list):
    local, rows, electrons = walkers.shape
    count, _, orbitals = vectors.shape
    half = local // 2
    block = orbitals // 4
    span = 2 * block // count
    wide = count * span
    piece = block // SUB
    chunks = half * BLOCKS * SUB
    mine = half // 2
    lanes = 128
    dma = pltpu.SemaphoreType.DMA
    anywhere = pl.BlockSpec(memory_space=pl.ANY)
    out, out_log = pl.pallas_call(
        functools.partial(kernel, depth, width),
        out_shape=(
            pltpu.VMEM(walkers.shape, BF16),
            pltpu.VMEM((local, 128), F32),
        ),
        in_specs=[anywhere] * 7,
        out_specs=(anywhere, pl.BlockSpec(memory_space=pltpu.VMEM)),
        scratch_shapes=[
            pltpu.VMEM(walkers.shape, BF16),
            pltpu.VMEM(inv_intersection.shape, BF16),
            pltpu.VMEM(trial.shape, BF16),
            pltpu.VMEM(vectors.shape, BF16),
            pltpu.VMEM(aux_field.shape, F32),
            pltpu.SMEM((local,), F32),
            pltpu.SMEM((width, local), jnp.int32),
            pltpu.VMEM((local, rows, electrons), BF16),
            pltpu.VMEM((count, rows, electrons), BF16),
            pltpu.VMEM((block // span, wide, BLOCKS * block), BF16),
            pltpu.VMEM((wide, block), BF16),
            pltpu.VMEM((2, width, local, lanes), F32),
            pltpu.VMEM((width, local, lanes), F32),
            pltpu.VMEM((local, lanes), F32),
            pltpu.VMEM((local, lanes), F32),
            pltpu.VMEM((local, BLOCKS, block, block), F32),
            pltpu.VMEM((2, chunks, piece, block), BF16),
            pltpu.VMEM((2, chunks, piece, block), BF16),
            pltpu.VMEM((chunks, piece, block), BF16),
            pltpu.VMEM((chunks, piece, block), BF16),
            pltpu.VMEM((2, chunks, piece, block), BF16),
            pltpu.VMEM((2, 2 * local, lanes), F32),
            pltpu.VMEM((2, 2 * local, lanes), F32),
            pltpu.VMEM((2, local, lanes), F32),
            pltpu.VMEM((width, half, rows, electrons), BF16),
            pltpu.VMEM((width, mine, 2, rows, electrons), BF16),
            pltpu.VMEM((orbitals, orbitals), BF16),
            pltpu.VMEM((ORDER + 1, electrons, orbitals), BF16),
            pltpu.VMEM((mine, 2, rows, electrons), BF16),
            dma((6 + LOADS,)),
            dma((width,)),
            dma((width,)),
            dma((width,)),
            dma((width,)),
            dma((2 * width,)),
            dma((2, width)),
            dma((2, half)),
            dma((2, chunks)),
            dma((chunks // 2,)),
            dma((2, mine)),
            dma((mine,)),
            dma((mine,)),
            dma((2,)),
            dma((2,)),
            dma((2,)),
            dma((half,)),
            dma((mine,)),
            dma((mine,)),
            dma((local, PARTS)),
            dma((local, PARTS)),
            dma((mine,)),
        ],
        compiler_params=pltpu.CompilerParams(collective_id=0, has_side_effects=True),
    )(walkers, inv_intersection, trial, vectors, aux_field, log_weight, copy_list)

    def settle(out_ref, log_ref, o1, o2, flat, sems):
        c1 = pltpu.make_async_copy(out_ref, o1, sems.at[0])
        c1.start()
        for s in range(local):
            flat[s] = jnp.max(log_ref[s:s + 1, :])
        c2 = pltpu.make_async_copy(flat, o2, sems.at[1])
        c2.start()
        c1.wait()
        c2.wait()

    return pl.pallas_call(
        settle,
        out_shape=(jax.ShapeDtypeStruct(walkers.shape, BF16), jax.ShapeDtypeStruct((local,), F32)),
        in_specs=[pl.BlockSpec(memory_space=pltpu.VMEM)] * 2,
        out_specs=(anywhere, anywhere),
        scratch_shapes=[pltpu.SMEM((local,), F32), dma((2,))],
    )(pltpu.with_memory_space_constraint(out, pltpu.VMEM), pltpu.with_memory_space_constraint(out_log, pltpu.VMEM))


def solution(mesh):
    depth, width = mesh.shape["vec"], mesh.shape["walk"]
    assert mesh.shape["orb"] == 2 and depth > 1
    return jax.shard_map(
        functools.partial(per_device, depth, width),
        mesh=mesh,
        in_specs=(
            P(("grp", "walk"), "orb", None),
            P(("grp", "walk"), None, None),
            P(),
            P("vec", "orb", None),
            P(("grp", "walk"), "vec"),
            P(("grp", "walk")),
            P(("grp", "walk")),
        ),
        out_specs=(P(("grp", "walk"), "orb", None), P(("grp", "walk"))),
        check_vma=False,
    )
```
